32 devices in a mesh: seq: 16 (over z, y, x), mp: 2 (over core).
Axes of the slice: x: 2, y: 2, z: 4, core: 2. Of those that a mesh axis runs over, the one named last changes fastest.
Arguments:
- states: bfloat16 [4096, 768], P('seq'), may hold values from -24 to 24
- qkv_weight: bfloat16 [3, 768, 768], P(None, None, 'mp'), may hold values from -0.21875 to 0.21875
- out_weight: bfloat16 [768, 768], P('mp'), may hold values from -0.21875 to 0.21875
- up_weight: bfloat16 [768, 3072], P(None, 'mp'), may hold values from -0.21875 to 0.21875
- down_weight: bfloat16 [3072, 768], P('mp'), may hold values from -0.109375 to 0.109375
- attn_gain: float32 [768], replicated, may hold values from 0.5 to 1.5
- mlp_gain: float32 [768], replicated, may hold values from 0.5 to 1.5
- global_ids: int32 [2], replicated, may hold values from 0 to 63, as said below
- random_owner: int32 [2, 64, 6, 3], P('mp', 'seq'), may hold values from 0 to 15, all different within a row; in each aligned block of 24 rows (0 to 23, 24 to 47, ..., all dimensions but the last counted through in order) at most 5 rows name the same one
- random_local: int32 [2, 64, 6, 3], P('mp', 'seq'), may hold values from 0 to 3
Outputs:
- layer_out: bfloat16 [4096, 768], P('seq')
The draws below stay inside these ranges and needn't reach their ends.
Inputs may be any that keep to these rules, and one draw needn't show every extreme that they name: `global_ids`: 2 different block numbers; the second is 63. The random key block is random_owner * 4 + random_local. For one query block and head the 3 owners differ. Within the rows of one device (aligned blocks of 4 * K rows over the first three dimensions, K the third dimension) no owner is named more than 5 times, a bound that some block reaches.
All inputs are finite; a program needn't handle non-finite values.
Results may differ from the reference program's by a relative error of at most 0.008.
The reference program's roundings to bfloat16 on the way count: a program that leaves them out, or rounds other values in their place, can miss the bound.
Values may be sent and summed in bfloat16 or wider, within the bound.
A program may use at most 192 MiB of HBM per device.

```python
import math
import jax
import jax.numpy as jnp
import numpy as np
from jax import lax

D = 768
H = 12
HD = 64
FF = 3072
BS = 64
R = 3
G = 2
QB_DEV = 4
TOKENS = 4096
NB = 64
MOST = 5
N_SEQ = 16
N_MP = 2


def chosen_blocks(key):
    first = jax.random.randint(jax.random.fold_in(key, 11), (1,), 0, NB - 1)
    return jnp.concatenate([first, jnp.full((1,), NB - 1)]).astype(jnp.int32)


def draw_global_ids(key, part):
    return chosen_blocks(key)


def draw_states(key, part):
    split_keys = jax.random.split(jax.random.fold_in(key, 23), 5)
    starts = chosen_blocks(key) * BS + 3
    picked = jax.random.randint(split_keys[3], (8,), BS // 2, TOKENS - BS)
    anchors = jnp.concatenate([starts, picked])
    direction = jax.random.uniform(split_keys[2], (D,), jnp.float32, -1.7, 1.7)
    jitter = jax.random.normal(split_keys[4], (2, anchors.shape[0], D), jnp.float32) * 0.05
    sample = jax.random.normal(split_keys[1], (TOKENS, D), jnp.float32)
    strength = jnp.linspace(2.5, 3.5, anchors.shape[0]).astype(jnp.float32)
    first_rows = strength[:, None] * direction[None, :] + jitter[0]
    second_rows = strength[:, None] * direction[None, :] * 1.01 + jitter[1]
    sample = sample.at[anchors].set(first_rows).at[anchors + 1].set(second_rows)
    return jnp.clip(sample, -6.0, 6.0).astype(jnp.bfloat16)


def place_ends(array, rng, low, largest):
    place = [jax.random.randint(jax.random.fold_in(rng, axis), (), 0, length) for axis, length in enumerate(array.shape)]
    longest = array.shape.index(max(array.shape))
    neighbour = place[:longest] + [(place[longest] + 1) % array.shape[longest]] + place[longest + 1:]
    return array.at[tuple(place)].set(low).at[tuple(neighbour)].set(largest)


def levels(key, extent, shards, low, high):
    loudness, own = 1.0, jax.random.fold_in(key, 6)
    for dim, shards_of in shards:
        steps = jnp.exp(jax.random.uniform(jax.random.fold_in(own, dim), (shards_of,), jnp.float32, low / len(shards), high / len(shards)))
        loudness = loudness * jnp.repeat(steps, extent[dim] // shards_of).reshape([-1 if axis == dim else 1 for axis in range(len(extent))])
    return loudness


def shared_out(stream_key, own, number, rows, count, top, most, lean):
    ranking = jax.random.permutation(stream_key, count)
    crowded, usual = shares(count, rows * top, most, lean, True), shares(count, rows * top, most, lean, False)
    places = jnp.arange(count)

    def named(tallies, rotation):
        used = int((tallies > 0).sum())
        fixed = max(1, used // 4)
        moved = fixed + (places - fixed + rotation * (used - fixed)) % max(1, count - fixed)
        return jnp.zeros((count,), jnp.int32).at[ranking[jnp.where(places < fixed, places, moved)]].set(jnp.asarray(tallies, jnp.int32))

    tallies = jnp.where(number % 4 == 0, named(crowded, number // 4), named(usual, number - number // 4 - 1))
    mixed = jax.random.permutation(jax.random.fold_in(own, 3), count)
    donor, sink = mixed[0:count // 2 * 2:2], mixed[1:count // 2 * 2:2]
    room = jnp.minimum(tallies[donor] - 1, most - tallies[sink]) // 2
    room = jnp.where((donor == ranking[0]) | (sink == ranking[0]) | (tallies[sink] == 0), 0, jnp.maximum(room, 0))
    moved = jax.random.randint(jax.random.fold_in(own, 4), (count // 2,), 0, 1 << 20) % (room + 1)
    tallies = tallies.at[donor].add(-moved).at[sink].add(moved)
    items = jnp.searchsorted(jnp.cumsum(tallies), jnp.arange(rows * top), side="right").astype(jnp.int32)
    grid = items.reshape(top, rows).T
    grid = grid[jax.random.permutation(jax.random.fold_in(own, 1), rows)]
    rotation = jax.random.randint(jax.random.fold_in(own, 2), (rows, 1), 0, top)
    return jnp.take_along_axis(grid, (jnp.arange(top)[None, :] + rotation) % top, axis=1)


def shares(number_of, total, reach, skew, full):
    weights = [(1 << 20) // math.isqrt(rank ** skew) + 1 for rank in range(1, number_of + 1)]
    largest = reach if full else min(reach, max(-(-total // number_of), total * weights[0] // sum(weights)))
    least = 1 if total - largest >= number_of - 1 else 0
    holding, spare = [largest] + [least] * (number_of - 1), total - largest - least * (number_of - 1)
    while spare > 0:
        free = [i for i in range(1, number_of) if holding[i] < largest] or [i for i in range(1, number_of) if holding[i] < reach]
        mass, left = sum([weights[i] for i in free]), spare
        for i in free:
            addition = min(reach - holding[i], max(1, left * weights[i] // mass), spare)
            holding[i] = holding[i] + addition
            spare = spare - addition
    return np.array(holding)


def noise(own_key, extent, scale, bound, pieces=(), held_as=jnp.bfloat16):
    array = scale * jax.random.normal(own_key, extent, jnp.float32)
    if pieces:
        array = array * levels(own_key, extent, pieces, -0.22, 0.18)
    return jnp.clip(array, -bound, bound).astype(held_as)


def setup_inputs(seed: int = 0) -> dict:
    seeds = jax.random.split(jax.random.key(seed), 11)
    states = draw_states(jax.random.fold_in(seeds[10], 71), 0)
    qkv_weight = noise(seeds[1], (3, D, D), D ** -0.5, 0.21875, ((2, 2),))
    out_weight = noise(seeds[2], (D, D), D ** -0.5, 0.21875, ((0, 2),))
    up_weight = noise(seeds[3], (D, FF), D ** -0.5, 0.21875, ((1, 2),))
    down_weight = noise(seeds[4], (FF, D), FF ** -0.5, 0.109375, ((0, 2),))
    attn_gain = jnp.clip(1.0 + 0.1 * jax.random.normal(seeds[5], (D,), jnp.float32), 0.5, 1.5)
    mlp_gain = jnp.clip(1.0 + 0.1 * jax.random.normal(seeds[6], (D,), jnp.float32), 0.5, 1.5)
    global_ids = draw_global_ids(jax.random.fold_in(seeds[10], 71), 0)
    random_owner_keys = jax.random.split(jax.random.fold_in(seeds[8], 1), N_MP * NB * (H // N_MP) // (QB_DEV * (H // N_MP)))
    random_owner_turns = jax.random.permutation(jax.random.fold_in(seeds[8], 3), N_MP * NB * (H // N_MP) // (QB_DEV * (H // N_MP)))
    random_owner = jax.vmap(lambda own, number: shared_out(jax.random.fold_in(seeds[8], 2), own, number, QB_DEV * (H // N_MP), N_SEQ, R, MOST, 2))(random_owner_keys, random_owner_turns).reshape((N_MP, NB, H // N_MP, R))
    random_local = place_ends(jax.random.randint(seeds[9], (N_MP, NB, H // N_MP, R), 0, QB_DEV), jax.random.fold_in(seeds[9], 1), 0, QB_DEV - 1).astype(jnp.int32)
    return dict(states=states, qkv_weight=qkv_weight, out_weight=out_weight, up_weight=up_weight, down_weight=down_weight, attn_gain=attn_gain, mlp_gain=mlp_gain, global_ids=global_ids, random_owner=random_owner, random_local=random_local)


EPSILON = 1e-05
NEGATIVE = -1e+30

def layer_norm(inputs, scales):
    center = lax.optimization_barrier(jnp.mean(inputs, axis=-1, keepdims=True))
    shifted = inputs - center
    spread = lax.optimization_barrier(jnp.mean(shifted * shifted, axis=-1, keepdims=True))
    return shifted * lax.rsqrt(spread + EPSILON) * scales.astype(jnp.float32)

def softmax_rows(scores):
    highest = lax.optimization_barrier(jnp.max(scores, axis=-1, keepdims=True))
    raised = jnp.exp(scores - highest)
    return raised / lax.optimization_barrier(jnp.sum(raised, axis=-1, keepdims=True))

def reference(states, qkv_weight, out_weight, up_weight, down_weight, attn_gain, mlp_gain, global_ids, random_owner, random_local):
    block_count = TOKENS // BS
    scaling = HD ** (-0.5)
    highest = lax.Precision.HIGHEST
    query_all = jnp.dot(states, qkv_weight[0], preferred_element_type=jnp.float32).astype(jnp.bfloat16)
    key_all = jnp.dot(states, qkv_weight[1], preferred_element_type=jnp.float32).astype(jnp.bfloat16)
    value_all = jnp.dot(states, qkv_weight[2], preferred_element_type=jnp.float32).astype(jnp.bfloat16)
    query_heads = query_all.reshape(block_count, BS, H, HD)
    key_heads = key_all.reshape(block_count, BS, H, HD).transpose(0, 2, 1, 3)
    value_heads = value_all.reshape(block_count, BS, H, HD).transpose(0, 2, 1, 3)
    random_ids = (random_owner * QB_DEV + random_local).transpose(1, 0, 2, 3).reshape(block_count, H, R)
    head_range = jnp.arange(H, dtype=jnp.int32)
    global_keys = key_heads[global_ids].astype(jnp.float32)
    global_values = value_heads[global_ids].astype(jnp.float32)

    def sparse_group(first_block):
        block_ids = first_block + jnp.arange(QB_DEV, dtype=jnp.int32)
        query_part = lax.dynamic_slice_in_dim(query_heads, first_block, QB_DEV, 0).astype(jnp.float32)
        offsets = block_ids[:, None] + jnp.arange(-1, 2, dtype=jnp.int32)[None, :]
        inside = (offsets >= 0) & (offsets < block_count)
        clipped = jnp.clip(offsets, 0, block_count - 1)
        window_keys = key_heads[clipped].astype(jnp.float32)
        window_values = value_heads[clipped].astype(jnp.float32)
        chosen = random_ids[block_ids]
        random_keys = key_heads[chosen, head_range[None, :, None]].astype(jnp.float32)
        random_values = value_heads[chosen, head_range[None, :, None]].astype(jnp.float32)
        score_window = jnp.einsum('bqhd,bwhkd->bhqwk', query_part, window_keys, precision=highest) * scaling
        score_window = jnp.where(inside[:, None, None, :, None], score_window, NEGATIVE)
        score_random = jnp.einsum('bqhd,bhrkd->bhqrk', query_part, random_keys, precision=highest) * scaling
        score_global = jnp.einsum('bqhd,ghkd->bhqgk', query_part, global_keys, precision=highest) * scaling
        joined = jnp.concatenate([score_window, score_random, score_global], axis=3)
        joined_shape = joined.shape
        flat_weights = softmax_rows(joined.reshape(joined_shape[0], joined_shape[1], joined_shape[2], -1))
        weights = lax.optimization_barrier(flat_weights.astype(jnp.bfloat16)).astype(jnp.float32).reshape(joined_shape)
        result = jnp.einsum('bhqwk,bwhkd->bqhd', weights[:, :, :, :3], window_values, precision=highest)
        result = result + jnp.einsum('bhqrk,bhrkd->bqhd', weights[:, :, :, 3:3 + R], random_values, precision=highest)
        result = result + jnp.einsum('bhqgk,ghkd->bqhd', weights[:, :, :, 3 + R:], global_values, precision=highest)
        return result
    sparse = lax.map(sparse_group, jnp.arange(N_SEQ, dtype=jnp.int32) * QB_DEV)
    sparse = sparse.reshape(block_count, BS, H, HD)
    global_queries = query_heads[global_ids].astype(jnp.float32).transpose(2, 0, 1, 3).reshape(H, G * BS, HD)
    every_key = key_heads.transpose(1, 0, 2, 3).reshape(H, TOKENS, HD)
    every_value = value_heads.transpose(1, 0, 2, 3).reshape(H, TOKENS, HD)

    def global_head(inputs):
        query_rows, key_rows, value_rows = inputs
        scores = jnp.dot(query_rows, key_rows.astype(jnp.float32).T, precision=highest) * scaling
        return jnp.dot(softmax_rows(scores), value_rows.astype(jnp.float32), precision=highest)
    global_out = lax.map(global_head, (global_queries, every_key, every_value))
    global_out = global_out.reshape(H, G, BS, HD).transpose(1, 2, 0, 3)
    sparse = sparse.at[global_ids].set(global_out)
    attended = sparse.astype(jnp.bfloat16).reshape(TOKENS, D)
    projected = jnp.dot(attended, out_weight, preferred_element_type=jnp.float32)
    normed = layer_norm(states.astype(jnp.float32) + projected, attn_gain).astype(jnp.bfloat16)
    hidden = jax.nn.gelu(jnp.dot(normed, up_weight, preferred_element_type=jnp.float32), approximate=False).astype(jnp.bfloat16)
    expanded = jnp.dot(hidden, down_weight, preferred_element_type=jnp.float32)
    return layer_norm(normed.astype(jnp.float32) + expanded, mlp_gain).astype(jnp.bfloat16)
```

```python
import functools

import jax
import jax.numpy as jnp
from jax import lax
from jax.experimental import pallas as pl
from jax.experimental.pallas import tpu as pltpu
from jax.sharding import PartitionSpec as P

HD = 64
BS = 64
R = 3
LANES = 128
MESH = pl.DeviceIdType.MESH

EPSILON = 1e-05
NEGATIVE = -1e30


def layer_norm(inputs, scales):
    center = jnp.mean(inputs, axis=-1, keepdims=True)
    shifted = inputs - center
    spread = jnp.mean(shifted * shifted, axis=-1, keepdims=True)
    return shifted * lax.rsqrt(spread + EPSILON) * scales


def dot_t(a, b):
    return lax.dot_general(a, b, (((1,), (1,)), ((), ())), preferred_element_type=jnp.float32)


def dot(a, b):
    return jnp.dot(a, b, preferred_element_type=jnp.float32)


def swap_halves(x):
    return pltpu.roll(x, HD, 1)


def attend_kernel(
    n,
    cap,
    heads,
    blocks,
    g_count,
    states_hbm,
    weight_hbm,
    wanted,
    slot,
    gids,
    att,
    states,
    weight,
    tab,
    tab_s,
    cand,
    cand_in,
    pick,
    gath,
    gstates,
    kvb,
    qpad,
    stage,
    rr,
    halo_l,
    halo_r,
    win,
    gq,
    gkv,
    part,
    part_in,
    gmine,
    gout,
    scores,
    s_tab,
    r_tab,
    s_cand,
    r_cand,
    s_gath,
    r_gath,
    s_rand,
    r_rand,
    s_halo,
    r_halo,
    s_part,
    r_part,
    s_gout,
    r_gout,
    s_mp,
    r_mp,
    l_sem,
    w_sem,
):
    me = lax.axis_index("seq")
    mine = lax.axis_index("mp")
    pairs = heads // 2
    width = states.shape[1]
    cols = width // LANES
    quarters = BS // 16
    half = gath.shape[0]
    gper = gath.shape[1] // (cols * quarters)
    units = gper * cols * quarters
    per = cand_in.shape[1]
    cand_parts = units // per
    rows_per = part_in.shape[2]
    part_parts = part.shape[0]
    left = lax.rem(me + n - 1, n)
    right = lax.rem(me + 1, n)

    def peer(k):
        return lax.rem(me + k, n)

    def each_peer(body):
        def step(k, carry):
            body(peer(k))
            return carry

        lax.fori_loop(1, n, step, 0)

    def guarded(limit, who, body):
        if limit < n:
            pl.when(who < limit)(body)
        else:
            body()

    def remote(src, dst, ssem, rsem, d):
        return pltpu.make_async_remote_copy(
            src_ref=src,
            dst_ref=dst,
            send_sem=ssem,
            recv_sem=rsem,
            device_id={"seq": d},
            device_id_type=MESH,
        )

    def tab_copy(d, owner):
        return remote(wanted.at[d], tab.at[owner], s_tab.at[d], r_tab.at[owner], d)

    def cand_copy(d, owner, at):
        return remote(
            cand.at[pl.ds(at * per, per)], cand_in.at[owner], s_cand.at[d], r_cand.at[owner], d
        )

    def gath_copy(d, owner):
        return remote(
            pick, gath.at[mine, pl.ds(owner * per, per)], s_gath.at[d], r_gath.at[owner], d
        )

    def rand_copy(d, owner):
        return remote(
            stage.at[pl.ds(d * cap, cap)],
            rr.at[pl.ds(owner * cap, cap)],
            s_rand.at[d],
            r_rand.at[owner],
            d,
        )

    def part_copy(d, owner, at):
        return remote(part.at[at], part_in.at[owner], s_part.at[d], r_part.at[owner], d)

    def gout_copy(d, owner):
        return remote(gmine, gout.at[owner], s_gout.at[d], r_gout.at[owner], d)

    def mp_copy(k, owner):
        other = lax.rem(mine + k, half)
        return pltpu.make_async_remote_copy(
            src_ref=gath.at[mine],
            dst_ref=gath.at[owner],
            send_sem=s_mp.at[k],
            recv_sem=r_mp.at[owner],
            device_id={"mp": other},
            device_id_type=MESH,
        )

    to_right = remote(
        kvb.at[pl.ds((blocks - 1) * heads, heads)], halo_l, s_halo.at[0], r_halo.at[0], right
    )
    to_left = remote(kvb.at[pl.ds(0, heads)], halo_r, s_halo.at[1], r_halo.at[1], left)

    loads = [pltpu.make_async_copy(states_hbm, states, w_sem.at[3])] + [
        pltpu.make_async_copy(weight_hbm.at[i], weight.at[i], w_sem.at[i]) for i in (1, 2, 0)
    ]
    for load in loads:
        load.start()

    barrier = pltpu.get_barrier_semaphore()
    each_peer(
        lambda d: pl.semaphore_signal(barrier, inc=1, device_id={"seq": d}, device_id_type=MESH)
    )
    for k in range(1, half):
        pl.semaphore_signal(
            barrier, inc=1, device_id={"mp": lax.rem(mine + k, half)}, device_id_type=MESH
        )

    loads[0].wait()
    for i in range(gper):
        local = lax.rem(gids[mine * gper + i], blocks)
        for j in range(cols):
            cut = slice(j * LANES, (j + 1) * LANES)
            piece = states[0:BS, cut]
            for b in range(1, blocks):
                piece = jnp.where(local == b, states[b * BS : (b + 1) * BS, cut], piece)
            for q in range(quarters):
                cand[(i * cols + j) * quarters + q] = piece[q * 16 : (q + 1) * 16]
    tab[me] = wanted[me]

    def own_cand():
        cand_in[me] = cand[pl.ds(me * per, per)]

    guarded(cand_parts, me, own_cand)
    loads[1].wait()
    loads[2].wait()

    lane = lax.broadcasted_iota(jnp.int32, (BS, LANES), 1)
    low = lane < HD
    x = states[...]
    for j in range(pairs):
        cut = slice(j * LANES, (j + 1) * LANES)
        k = dot(x, weight[1, :, cut])
        v = dot(x, weight[2, :, cut])
        for b in range(blocks):
            kb, vb = k[b * BS : (b + 1) * BS], v[b * BS : (b + 1) * BS]
            kvb[b * heads + 2 * j] = jnp.where(low, kb, swap_halves(vb)).astype(jnp.bfloat16)
            kvb[b * heads + 2 * j + 1] = jnp.where(low, swap_halves(kb), vb).astype(jnp.bfloat16)

    pl.semaphore_wait(barrier, n - 1 + half - 1)
    each_peer(lambda d: tab_copy(d, me).start())
    each_peer(lambda d: guarded(cand_parts, d, lambda: cand_copy(d, me, d).start()))
    to_right.start()
    to_left.start()

    loads[3].wait()
    scaling = HD ** (-0.5)
    for j in range(pairs):
        cut = slice(j * LANES, (j + 1) * LANES)
        q = dot(x, weight[0, :, cut]).astype(jnp.bfloat16).astype(jnp.float32) * scaling
        for b in range(blocks):
            qb = q[b * BS : (b + 1) * BS]
            qpad[b * heads + 2 * j] = jnp.where(low, qb, 0.0).astype(jnp.bfloat16)
            qpad[b * heads + 2 * j + 1] = jnp.where(low, swap_halves(qb), 0.0).astype(jnp.bfloat16)

    def relay():
        each_peer(lambda d: cand_copy(d, d, me).wait_recv())
        for u in range(per):
            g = (me * per + u) // (cols * quarters)
            wanted_id = gids[mine * gper + g]

            def choose(d, so_far):
                here = (wanted_id >= d * blocks) & (wanted_id < (d + 1) * blocks)
                return jnp.where(here, cand_in[d, u], so_far)

            pick[u] = lax.fori_loop(1, n, choose, cand_in[0, u])
        gath[mine, pl.ds(me * per, per)] = pick[...]
        each_peer(lambda d: gath_copy(d, me).start())

    guarded(cand_parts, me, relay)

    each_peer(lambda d: tab_copy(d, d).wait_recv())
    table = pltpu.make_async_copy(tab, tab_s, l_sem)
    table.start()
    table.wait()

    def serve(d):
        for c in range(cap):
            stage[d * cap + c] = kvb[tab_s[d, 0, c]]
        rand_copy(d, me).start()

    def serve_some(start, stop):
        def step(k, carry):
            serve(peer(k))
            return carry

        lax.fori_loop(start, stop, step, 0)

    for c in range(cap):
        rr[me * cap + c] = kvb[tab_s[me, 0, c]]

    each_peer(lambda d: guarded(cand_parts, d, lambda: gath_copy(d, d).wait_recv()))
    for k in range(1, half):
        mp_copy(k, mine).start()
    for k in range(1, half):
        mp_copy(k, lax.rem(mine + k, half)).wait_recv()
    for g in range(g_count):
        for j in range(cols):
            for q in range(quarters):
                gstates[g * BS + q * 16 : g * BS + (q + 1) * 16, j * LANES : (j + 1) * LANES] = (
                    gath[g // gper, ((g % gper) * cols + j) * quarters + q]
                )
    gx = gstates[...]
    rows = g_count * BS
    glane = lax.broadcasted_iota(jnp.int32, (rows, LANES), 1)
    glow = glane < HD
    for j in range(pairs):
        cut = slice(j * LANES, (j + 1) * LANES)
        q = dot(gx, weight[0, :, cut]).astype(jnp.bfloat16).astype(jnp.float32) * scaling
        k = dot(gx, weight[1, :, cut])
        v = dot(gx, weight[2, :, cut])
        gq[2 * j] = jnp.where(glow, q, 0.0).astype(jnp.bfloat16)
        gq[2 * j + 1] = jnp.where(glow, swap_halves(q), 0.0).astype(jnp.bfloat16)
        gkv[2 * j] = jnp.where(glow, k, swap_halves(v)).astype(jnp.bfloat16)
        gkv[2 * j + 1] = jnp.where(glow, swap_halves(k), v).astype(jnp.bfloat16)

    for h in range(heads):
        keys = jnp.concatenate([kvb[b * heads + h] for b in range(blocks)], axis=0)
        s = dot_t(gq[h], keys)
        high = jnp.max(s, axis=-1, keepdims=True)
        e = jnp.exp(s - high)
        total = jnp.sum(e, axis=-1, keepdims=True)
        e_high = e.astype(jnp.bfloat16)
        e_low = (e - e_high.astype(jnp.float32)).astype(jnp.bfloat16)
        acc = (dot(e_high, keys) + dot(e_low, keys)) * (1.0 / total)
        level = high + jnp.log(total)
        first = level.astype(jnp.bfloat16).astype(jnp.float32)
        second = (level - first).astype(jnp.bfloat16).astype(jnp.float32)
        third = level - first - second
        packed = jnp.where(
            glane < 16,
            first,
            jnp.where(glane < 32, second, jnp.where(glow, third, acc)),
        ).astype(jnp.bfloat16)
        cuts = rows // rows_per
        for c in range(cuts):
            part[(h // 2) * cuts + c, h % 2] = packed[c * rows_per : (c + 1) * rows_per]
    each_peer(lambda d: guarded(part_parts, d, lambda: part_copy(d, me, d).start()))
    serve_some(1, n)

    to_right.wait_recv()
    to_left.wait_recv()
    win[0:heads] = halo_l[...]
    win[heads : heads + blocks * heads] = kvb[...]
    win[heads + blocks * heads :] = halo_r[...]

    near = 3 + g_count
    slot_lane = lax.broadcasted_iota(jnp.int32, (BS, near * BS), 1)

    def near_keys(at, h):
        return jnp.concatenate([win[at + t * heads] for t in range(3)] + [gkv[h]], axis=0)

    def near_step(b, carry):
        first = me * blocks + b
        start = jnp.where(first == 0, BS, 0)
        stop = jnp.where(first == n * blocks - 1, 2 * BS, 3 * BS)
        outside = (slot_lane < start) | ((slot_lane >= stop) & (slot_lane < 3 * BS))
        for h in range(heads):
            at = b * heads + h
            scores[at] = jnp.where(outside, NEGATIVE, dot_t(qpad[at], near_keys(at, h)))
        return carry

    lax.fori_loop(0, blocks, near_step, 0)

    def combine():
        part_in[me] = part[me]
        each_peer(lambda d: part_copy(d, d, me).wait_recv())
        outs = []
        for parity in range(2):

            def level(d):
                piece = part_in[d, parity].astype(jnp.float32)
                return piece, piece[:, 0:1] + piece[:, 16:17] + piece[:, 32:33]

            def top(d, best):
                return jnp.maximum(best, level(d)[1])

            best = lax.fori_loop(1, n, top, level(0)[1])

            def add(d, so_far):
                piece, high = level(d)
                factor = jnp.exp(high - best)
                return so_far[0] + piece * factor, so_far[1] + factor

            zero = (jnp.zeros((rows_per, LANES), jnp.float32), jnp.zeros((rows_per, 1), jnp.float32))
            summed, total = lax.fori_loop(0, n, add, zero)
            outs.append(summed / total)
        plow = lax.broadcasted_iota(jnp.int32, (rows_per, LANES), 1) < HD
        done = jnp.where(plow, swap_halves(outs[0]), outs[1]).astype(jnp.bfloat16)
        gmine[...] = done
        gout[me] = done
        each_peer(lambda d: gout_copy(d, me).start())

    guarded(part_parts, me, combine)

    each_peer(lambda d: rand_copy(d, d).wait_recv())

    def block_step(b, carry):
        for j in range(pairs):
            halves = []
            for h in (2 * j, 2 * j + 1):
                at = b * heads + h
                early_keys = near_keys(at, h)
                keys = jnp.concatenate([rr[slot[at * R + r]] for r in range(R)], axis=0)
                s = dot_t(qpad[at], keys)
                early_s = scores[at]
                high = jnp.maximum(
                    jnp.max(s, axis=-1, keepdims=True), jnp.max(early_s, axis=-1, keepdims=True)
                )
                e = jnp.exp(s - high)
                early_e = jnp.exp(early_s - high)
                total = jnp.sum(e, axis=-1, keepdims=True) + jnp.sum(
                    early_e, axis=-1, keepdims=True
                )
                share = 1.0 / total
                w = (e * share).astype(jnp.bfloat16)
                early_w = (early_e * share).astype(jnp.bfloat16)
                halves.append(dot(w, keys) + dot(early_w, early_keys))
            att[j, pl.ds(pl.multiple_of(b * BS, BS), BS), :] = jnp.where(
                low, swap_halves(halves[0]), halves[1]
            ).astype(jnp.bfloat16)
        return carry

    lax.fori_loop(0, blocks, block_step, 0)

    each_peer(lambda d: guarded(part_parts, d, lambda: gout_copy(d, d).wait_recv()))
    for j in range(pairs):
        for g in range(g_count):
            cuts = BS // rows_per
            at = (j * g_count + g) * cuts
            row = jnp.concatenate([gout[at + c] for c in range(cuts)], axis=0).astype(jnp.float32)
            for b in range(blocks):
                here = gids[g] == me * blocks + b
                old = att[j, b * BS : (b + 1) * BS, :].astype(jnp.float32)
                att[j, b * BS : (b + 1) * BS, :] = jnp.where(here, row, old).astype(jnp.bfloat16)

    def drain(d):
        tab_copy(d, me).wait_send()
        guarded(cand_parts, d, lambda: cand_copy(d, me, d).wait_send())
        guarded(cand_parts, me, lambda: gath_copy(d, me).wait_send())
        rand_copy(d, me).wait_send()
        guarded(part_parts, d, lambda: part_copy(d, me, d).wait_send())
        guarded(part_parts, me, lambda: gout_copy(d, me).wait_send())

    each_peer(drain)
    for k in range(1, half):
        mp_copy(k, mine).wait_send()
    to_right.wait_send()
    to_left.wait_send()


TREES = ("zxy", "zyx", "yzx", "xzy")
PLACES = ((0, 0), (1, 0), (0, 1), (1, 1))
TURNS = (
    (-8.5, -3.0, -1.5, 10.5),
    (-5.5, 3.0, 0.0, 8.0),
    (-2.0, 5.0, 3.5, 13.5),
    (-1.5, 2.0, 7.5, 11.0),
)
LAG = 3


def arrivals(depth):
    pieces = [
        (3.5 * slot + TURNS[t][p], t, slot, *PLACES[p])
        for t in range(len(TREES))
        for slot in range(depth)
        for p in range(len(PLACES))
        if slot or p
    ]
    return [piece[1:] for piece in sorted(pieces)]


def hops(tree, slot, dx, dy):
    moved = {"x": dx, "y": dy, "z": slot}
    last = max((i for i in range(3) if moved[tree[i]]), default=-1)
    onward = tree[last + 1 :]
    via = tree[last] if last >= 0 else ""
    return via, ("z" if via == "z" else "") + onward


def slots(z, depth):
    inward = 1 if 2 * z < depth else -1
    return sorted(range(depth), key=lambda q: (abs(q - z), (z - q) * inward))


def gather_kernel(
    n,
    heads,
    blocks,
    g_count,
    states_hbm,
    weight_hbm,
    owner,
    local,
    gids,
    att,
    xs,
    wq,
    wkv,
    kv,
    q_all,
    wide,
    gmine,
    gout,
    scores,
    s_x,
    s_y,
    s_up,
    s_down,
    s_mp,
    r_ici,
    r_mp,
    s_gout,
    r_gout,
    l_sem,
):
    me = lax.axis_index("seq")
    mine = lax.axis_index("mp")
    pairs = heads // 2
    inner = heads * HD
    trees = len(TREES)
    per = 2 * trees
    piece = xs.shape[1]
    width = xs.shape[2]
    tokens = per * piece
    depth = n // 4
    units = pairs * g_count
    x_at, y_at, z_at = lax.rem(me, 2), lax.rem(me // 2, 2), me // 4

    def remote(src, dst, ssem, rsem, where):
        return pltpu.make_async_remote_copy(
            src_ref=src,
            dst_ref=dst,
            send_sem=ssem,
            recv_sem=rsem,
            device_id=where,
            device_id_type=MESH,
        )

    def peer(k):
        return lax.rem(me + k, n)

    def each_peer(body):
        def step(k, carry):
            body(peer(k))
            return carry

        lax.fori_loop(1, n, step, 0)

    def plane(slot):
        if slot == 0:
            return z_at
        found = slots(0, depth)[slot]
        for z in range(1, depth):
            found = jnp.where(z_at == z, slots(z, depth)[slot], found)
        return found

    def shard_of(slot, dx, dy):
        x = 1 - x_at if dx else x_at
        y = 1 - y_at if dy else y_at
        return plane(slot) * 4 + y * 2 + x

    def ici(shard, t, ssem, d):
        at = xs.at[(shard * 2 + mine) * trees + t]
        return remote(at, at, ssem.at[shard * trees + t], r_ici.at[shard * trees + t], {"seq": d})

    def across(shard, t, core):
        at = xs.at[(shard * 2 + core) * trees + t]
        return remote(
            at, at, s_mp.at[shard * trees + t], r_mp.at[shard * trees + t], {"mp": 1 - mine}
        )

    x_peer = me + 1 - 2 * x_at
    y_peer = me + 2 - 4 * y_at
    up, down = lax.rem(me + 4, n), lax.rem(me + n - 4, n)

    def onward(t, slot, dx, dy, act):
        shard = shard_of(slot, dx, dy)
        via, axes = hops(TREES[t], slot, dx, dy)
        for axis in axes:
            if axis == "x":
                act(ici(shard, t, s_x, x_peer))
            elif axis == "y":
                act(ici(shard, t, s_y, y_peer))
            else:
                source = plane(slot)
                go_up = z_at < depth - 1
                go_down = z_at > 0
                if via == "z":
                    go_up = go_up & (source < z_at)
                    go_down = go_down & (source > z_at)
                pl.when(go_up)(lambda: act(ici(shard, t, s_up, up)))
                pl.when(go_down)(lambda: act(ici(shard, t, s_down, down)))
        if slot or dx or dy:
            act(across(shard, t, mine))

    order = arrivals(depth)

    loads = [
        pltpu.make_async_copy(states_hbm, xs.at[pl.ds(me * per, per)], l_sem.at[0]),
        pltpu.make_async_copy(weight_hbm.at[1], wkv.at[:, 0:inner], l_sem.at[1]),
        pltpu.make_async_copy(weight_hbm.at[2], wkv.at[:, inner : 2 * inner], l_sem.at[2]),
        pltpu.make_async_copy(weight_hbm.at[0], wq, l_sem.at[3]),
    ]
    for load in loads:
        load.start()
    barrier = pltpu.get_barrier_semaphore()
    each_peer(
        lambda d: pl.semaphore_signal(barrier, inc=1, device_id={"seq": d}, device_id_type=MESH)
    )
    pl.semaphore_signal(barrier, inc=1, device_id={"mp": 1 - mine}, device_id_type=MESH)
    loads[0].wait()
    pl.semaphore_wait(barrier, n)
    for t in range(trees):
        onward(t, 0, 0, 0, lambda copy: copy.start())
    for load in loads[1:]:
        load.wait()

    def project(shard):
        def step(c, carry):
            x = xs[pl.ds(shard * per, per)].reshape(tokens, width)
            cut = pl.ds(pl.multiple_of(c * 256, 256), 256)
            y = dot(x, wkv[:, cut]).astype(jnp.bfloat16)
            kv[pl.ds(shard * blocks, blocks), :, cut] = y.reshape(blocks, BS, 256)
            return carry

        lax.fori_loop(0, 2 * inner // 256, step, 0)

    x = xs[pl.ds(me * per, per)].reshape(tokens, width)
    scaling = HD ** (-0.5)
    q_all[...] = (
        dot(x, wq[...]).astype(jnp.bfloat16).astype(jnp.float32) * scaling
    ).astype(jnp.bfloat16)
    project(me)

    waiting = []
    left = dict()

    def finish(place):
        shard = shard_of(*place)
        for t in range(trees):
            across(shard, t, 1 - mine).wait_recv()
        project(shard)

    for t, slot, dx, dy in order:
        shard = shard_of(slot, dx, dy)
        ici(shard, t, s_x, x_peer).wait_recv()
        onward(t, slot, dx, dy, lambda copy: copy.start())
        waiting = [(count - 1, place) for count, place in waiting]
        while waiting and waiting[0][0] <= 0:
            finish(waiting.pop(0)[1])
        place = (slot, dx, dy)
        left[place] = left.get(place, trees) - 1
        if left[place] == 0:
            waiting.append((LAG, place))
    for _, place in waiting:
        finish(place)

    lane = lax.broadcasted_iota(jnp.int32, (BS, LANES), 1)
    low = lane < HD

    def split(q):
        zero = jnp.zeros_like(q)
        return jnp.concatenate([jnp.where(low, q, zero), jnp.where(low, zero, q)], axis=0)

    def together(out):
        return jnp.where(low, out[0:BS], out[BS : 2 * BS]).astype(jnp.bfloat16)

    chunk = wide.shape[2]
    per_chunk = chunk // BS
    chunks = wide.shape[0]

    def share():
        j, g = me // g_count, lax.rem(me, g_count)
        k_cut = pl.ds(pl.multiple_of(j * LANES, LANES), LANES)
        v_cut = pl.ds(pl.multiple_of(inner + j * LANES, LANES), LANES)
        rows = BS // piece
        x = xs[pl.ds(gids[g] * rows, rows)].reshape(BS, width)
        q = dot(x, wq[:, k_cut]).astype(jnp.bfloat16).astype(jnp.float32) * scaling
        q2 = split(q.astype(jnp.bfloat16))

        def score(c, best):
            keys = kv[pl.ds(c * per_chunk, per_chunk), :, k_cut].reshape(chunk, LANES)
            s = dot_t(q2, keys)
            wide[c] = s
            return jnp.maximum(best, jnp.max(s, axis=-1, keepdims=True))

        high = lax.fori_loop(0, chunks, score, jnp.full((2 * BS, 1), NEGATIVE, jnp.float32))

        def add(c, so_far):
            values = kv[pl.ds(c * per_chunk, per_chunk), :, v_cut].reshape(chunk, LANES)
            e = jnp.exp(wide[c] - high)
            e_high = e.astype(jnp.bfloat16)
            e_low = (e - e_high.astype(jnp.float32)).astype(jnp.bfloat16)
            return (
                so_far[0] + dot(e_high, values) + dot(e_low, values),
                so_far[1] + jnp.sum(e, axis=-1, keepdims=True),
            )

        zero = (jnp.zeros((2 * BS, LANES), jnp.float32), jnp.zeros((2 * BS, 1), jnp.float32))
        summed, total = lax.fori_loop(0, chunks, add, zero)
        done = together(summed / total)
        gmine[...] = done
        gout[me] = done
        each_peer(lambda d: gout_copy(d, me).start())

    def gout_copy(d, unit):
        return remote(gmine, gout.at[unit], s_gout.at[d], r_gout.at[unit], {"seq": d})

    def guarded(who, body):
        if units < n:
            pl.when(who < units)(body)
        else:
            body()

    guarded(me, share)

    slot_lane = lax.broadcasted_iota(jnp.int32, (1, 3 * BS), 1)
    last = n * blocks - 1

    def block_step(b, carry):
        first = me * blocks + b
        start = jnp.where(first == 0, BS, 0)
        stop = jnp.where(first == last, 2 * BS, 3 * BS)
        bias = jnp.where((slot_lane < start) | (slot_lane >= stop), NEGATIVE, 0.0)
        near = [jnp.maximum(first - 1, 0), first, jnp.minimum(first + 1, last)]
        ends = [gids[g] for g in range(g_count)]
        for j in range(pairs):
            one = [
                owner[0, b, 2 * j, r] * blocks + local[0, b, 2 * j, r] for r in range(R)
            ]
            two = [
                owner[0, b, 2 * j + 1, r] * blocks + local[0, b, 2 * j + 1, r] for r in range(R)
            ]

            def rows(base):
                cut = slice(base + j * LANES, base + (j + 1) * LANES)
                return jnp.concatenate(
                    [kv[at, :, cut] for at in near]
                    + [jnp.where(low, kv[a, :, cut], kv[c, :, cut]) for a, c in zip(one, two)]
                    + [kv[at, :, cut] for at in ends],
                    axis=0,
                )

            q = q_all[pl.ds(pl.multiple_of(b * BS, BS), BS), j * LANES : (j + 1) * LANES]
            s = dot_t(split(q), rows(0))
            s = jnp.concatenate([s[:, 0 : 3 * BS] + bias, s[:, 3 * BS :]], axis=1)
            e = jnp.exp(s - jnp.max(s, axis=-1, keepdims=True))
            w = (e * (1.0 / jnp.sum(e, axis=-1, keepdims=True))).astype(jnp.bfloat16)
            att[j, pl.ds(pl.multiple_of(b * BS, BS), BS), :] = together(dot(w, rows(inner)))
        return carry

    lax.fori_loop(0, blocks, block_step, 0)

    each_peer(lambda d: guarded(d, lambda: gout_copy(d, d).wait_recv()))
    for j in range(pairs):
        for g in range(g_count):
            row = gout[j * g_count + g].astype(jnp.float32)
            for b in range(blocks):
                here = gids[g] == me * blocks + b
                old = att[j, b * BS : (b + 1) * BS, :].astype(jnp.float32)
                att[j, b * BS : (b + 1) * BS, :] = jnp.where(here, row, old).astype(jnp.bfloat16)

    for t in range(trees):
        onward(t, 0, 0, 0, lambda copy: copy.wait_send())
    for t, slot, dx, dy in order:
        onward(t, slot, dx, dy, lambda copy: copy.wait_send())
    each_peer(lambda d: guarded(me, lambda: gout_copy(d, me).wait_send()))


def tail_kernel(
    chunks,
    att,
    states,
    out_w,
    up_w,
    down_w,
    gain1,
    gain2,
    out,
    mine1,
    theirs1,
    mine2,
    theirs2,
    s1,
    r1,
    s2,
    r2,
    normed,
):
    other = 1 - lax.axis_index("mp")
    barrier = pltpu.get_barrier_semaphore()
    pl.semaphore_signal(barrier, inc=1, device_id={"mp": other}, device_id_type=MESH)
    pl.semaphore_wait(barrier, 1)
    rows = states.shape[0] // chunks

    def swap(mine, theirs, ssem, rsem, c):
        return pltpu.make_async_remote_copy(
            src_ref=mine.at[c],
            dst_ref=theirs.at[c],
            send_sem=ssem.at[c],
            recv_sem=rsem.at[c],
            device_id={"mp": other},
            device_id_type=MESH,
        )

    for c in range(chunks):
        cut = slice(c * rows, (c + 1) * rows)
        acc = dot(att[0, cut, :], out_w[0:LANES, :])
        for j in range(1, att.shape[0]):
            acc = acc + dot(att[j, cut, :], out_w[j * LANES : (j + 1) * LANES, :])
        mine1[c] = acc.astype(mine1.dtype)
        swap(mine1, theirs1, s1, r1, c).start()
    for c in range(chunks):
        cut = slice(c * rows, (c + 1) * rows)
        swap(mine1, theirs1, s1, r1, c).wait_recv()
        summed = mine1[c].astype(jnp.float32) + theirs1[c].astype(jnp.float32)
        norm = layer_norm(states[cut, :].astype(jnp.float32) + summed, gain1[...])
        norm = norm.astype(jnp.bfloat16)
        normed[c] = norm
        v = dot(norm, up_w[...])
        hidden = (v * (1.0 + lax.erf(v * (0.5**0.5))) * 0.5).astype(jnp.bfloat16)
        mine2[c] = dot(hidden, down_w[...]).astype(mine2.dtype)
        swap(mine2, theirs2, s2, r2, c).start()
    for c in range(chunks):
        cut = slice(c * rows, (c + 1) * rows)
        swap(mine2, theirs2, s2, r2, c).wait_recv()
        summed = mine2[c].astype(jnp.float32) + theirs2[c].astype(jnp.float32)
        out[cut, :] = layer_norm(normed[c].astype(jnp.float32) + summed, gain2[...]).astype(
            jnp.bfloat16
        )
    for c in range(chunks):
        swap(mine1, theirs1, s1, r1, c).wait_send()
        swap(mine2, theirs2, s2, r2, c).wait_send()


def vmem_specs(count):
    return [pl.BlockSpec(memory_space=pltpu.VMEM)] * count


def attend_requested(states, qkv_weight, global_ids, random_owner, random_local):
    tokens, width = states.shape
    heads = qkv_weight.shape[2] // HD
    pairs = heads // 2
    blocks = tokens // BS
    g_count = global_ids.shape[0]
    n = lax.axis_size("seq")

    owner = random_owner.reshape(-1)
    items = owner.shape[0]
    cap = max(2, items // n + 1)
    head_list = jnp.broadcast_to(
        jnp.arange(heads, dtype=jnp.int32)[None, :, None], (blocks, heads, R)
    ).reshape(-1)
    code = random_local.reshape(-1) * heads + head_list
    earlier = jnp.arange(items)[:, None] > jnp.arange(items)[None, :]
    rank = jnp.sum(((owner[:, None] == owner[None, :]) & earlier).astype(jnp.int32), axis=1)
    slot = owner * cap + rank
    place = owner * LANES + rank
    wanted = jnp.sum(
        jnp.where(
            place[None, None, :]
            == (jnp.arange(n)[:, None] * LANES + jnp.arange(LANES)[None, :])[:, :, None],
            code[None, None, :],
            0,
        ),
        axis=2,
    ).reshape(n, 1, LANES)

    half = lax.axis_size("mp")
    units = (g_count // half) * (width // LANES) * (BS // 16)
    per = -(-units // n)
    part_rows = pairs * g_count * BS
    rows_per = -(-part_rows // n // 16) * 16
    parts = part_rows // rows_per
    bf = jnp.bfloat16
    own = blocks * heads
    dma = pltpu.SemaphoreType.DMA
    return pl.pallas_call(
        functools.partial(attend_kernel, n, cap, heads, blocks, g_count),
        out_shape=jax.ShapeDtypeStruct((pairs, tokens, LANES), bf),
        in_specs=[pl.BlockSpec(memory_space=pltpu.HBM)] * 2
        + vmem_specs(1)
        + [pl.BlockSpec(memory_space=pltpu.SMEM)] * 2,
        out_specs=pl.BlockSpec(memory_space=pltpu.VMEM),
        scratch_shapes=[
            pltpu.VMEM((tokens, width), bf),
            pltpu.VMEM(qkv_weight.shape, bf),
            pltpu.VMEM((n, 1, LANES), jnp.int32),
            pltpu.SMEM((n, 1, LANES), jnp.int32),
            pltpu.VMEM((units, 16, LANES), bf),
            pltpu.VMEM((n, per, 16, LANES), bf),
            pltpu.VMEM((per, 16, LANES), bf),
            pltpu.VMEM((half, units, 16, LANES), bf),
            pltpu.VMEM((g_count * BS, width), bf),
            pltpu.VMEM((own, BS, LANES), bf),
            pltpu.VMEM((own, BS, LANES), bf),
            pltpu.VMEM((n * cap, BS, LANES), bf),
            pltpu.VMEM((n * cap, BS, LANES), bf),
            pltpu.VMEM((heads, BS, LANES), bf),
            pltpu.VMEM((heads, BS, LANES), bf),
            pltpu.VMEM((own + 2 * heads, BS, LANES), bf),
            pltpu.VMEM((heads, g_count * BS, LANES), bf),
            pltpu.VMEM((heads, g_count * BS, LANES), bf),
            pltpu.VMEM((parts, 2, rows_per, LANES), bf),
            pltpu.VMEM((n, 2, rows_per, LANES), bf),
            pltpu.VMEM((rows_per, LANES), bf),
            pltpu.VMEM((parts, rows_per, LANES), bf),
            pltpu.VMEM((own, BS, (3 + g_count) * BS), jnp.float32),
        ]
        + [dma((n,))] * 8
        + [dma((2,))] * 2
        + [dma((n,))] * 4
        + [dma((half,))] * 2
        + [dma(()), dma((4,))],
        cost_estimate=pl.CostEstimate(
            flops=30_000_000_000, bytes_accessed=20_000_000, transcendentals=0
        ),
        compiler_params=pltpu.CompilerParams(
            collective_id=0, has_side_effects=True, vmem_limit_bytes=32 * 1024 * 1024
        ),
    )(
        pltpu.with_memory_space_constraint(states, pltpu.HBM),
        pltpu.with_memory_space_constraint(qkv_weight, pltpu.HBM),
        wanted,
        slot,
        global_ids,
    )


def attend_gathered(states, qkv_weight, global_ids, random_owner, random_local):
    tokens, width = states.shape
    inner = qkv_weight.shape[2]
    heads = inner // HD
    pairs = heads // 2
    blocks = tokens // BS
    g_count = global_ids.shape[0]
    n = lax.axis_size("seq")
    trees = len(TREES)
    piece = tokens // (2 * trees)
    chunk = 8 * BS
    bf = jnp.bfloat16
    dma = pltpu.SemaphoreType.DMA
    return pl.pallas_call(
        functools.partial(gather_kernel, n, heads, blocks, g_count),
        out_shape=jax.ShapeDtypeStruct((pairs, tokens, LANES), bf),
        in_specs=[pl.BlockSpec(memory_space=pltpu.HBM)] * 2
        + [pl.BlockSpec(memory_space=pltpu.SMEM)] * 3,
        out_specs=pl.BlockSpec(memory_space=pltpu.VMEM),
        scratch_shapes=[
            pltpu.VMEM((n * 2 * trees, piece, width), bf),
            pltpu.VMEM((width, inner), bf),
            pltpu.VMEM((width, 2 * inner), bf),
            pltpu.VMEM((n * blocks, BS, 2 * inner), bf),
            pltpu.VMEM((tokens, inner), bf),
            pltpu.VMEM((n * tokens // chunk, 2 * BS, chunk), jnp.float32),
            pltpu.VMEM((BS, LANES), bf),
            pltpu.VMEM((pairs * g_count, BS, LANES), bf),
            pltpu.VMEM((8, LANES), jnp.float32),
        ]
        + [dma((n * trees,))] * 7
        + [dma((n,)), dma((pairs * g_count,)), dma((4,))],
        cost_estimate=pl.CostEstimate(
            flops=30_000_000_000, bytes_accessed=20_000_000, transcendentals=0
        ),
        compiler_params=pltpu.CompilerParams(
            collective_id=0, has_side_effects=True, vmem_limit_bytes=40 * 1024 * 1024
        ),
    )(
        pltpu.with_memory_space_constraint(
            states.reshape(2 * trees, piece, width), pltpu.HBM
        ),
        pltpu.with_memory_space_constraint(qkv_weight, pltpu.HBM),
        random_owner,
        random_local,
        global_ids,
    )


def gathers(states, qkv_weight, global_ids):
    tokens, width = states.shape
    n = lax.axis_size("seq")
    inner = qkv_weight.shape[2]
    held = n * tokens * (width + 2 * inner) * 2
    units = inner // LANES * global_ids.shape[0]
    return (
        n % 4 == 0
        and lax.axis_size("mp") == 2
        and held <= 24 * 1024 * 1024
        and units <= n
        and tokens % (2 * len(TREES) * 16) == 0
        and 2 * inner % 256 == 0
    )


def shards(
    states,
    qkv_weight,
    out_weight,
    up_weight,
    down_weight,
    attn_gain,
    mlp_gain,
    global_ids,
    random_owner,
    random_local,
):
    tokens, width = states.shape
    bf = jnp.bfloat16
    dma = pltpu.SemaphoreType.DMA
    attend = attend_gathered if gathers(states, qkv_weight, global_ids) else attend_requested
    att = attend(states, qkv_weight, global_ids, random_owner, random_local)

    chunks = 4
    rows = tokens // chunks
    link = jnp.bfloat16
    return pl.pallas_call(
        functools.partial(tail_kernel, chunks),
        out_shape=jax.ShapeDtypeStruct((tokens, width), bf),
        in_specs=vmem_specs(7),
        out_specs=pl.BlockSpec(memory_space=pltpu.VMEM),
        scratch_shapes=[pltpu.VMEM((chunks, rows, width), link)] * 4
        + [dma((chunks,))] * 4
        + [pltpu.VMEM((chunks, rows, width), bf)],
        compiler_params=pltpu.CompilerParams(
            collective_id=1, has_side_effects=True, vmem_limit_bytes=32 * 1024 * 1024
        ),
    )(
        att,
        states,
        out_weight,
        up_weight,
        down_weight,
        attn_gain.reshape(1, width),
        mlp_gain.reshape(1, width),
    )


def solution(mesh):
    in_specs = (
        P("seq", None),
        P(None, None, "mp"),
        P("mp", None),
        P(None, "mp"),
        P("mp", None),
        P(),
        P(),
        P(),
        P("mp", "seq", None, None),
        P("mp", "seq", None, None),
    )
    out_specs = P("seq", None)
    return jax.shard_map(shards, mesh=mesh, in_specs=in_specs, out_specs=out_specs, check_vma=False)
```

```python
import functools

import jax
import jax.numpy as jnp
from jax import lax
from jax.experimental import pallas as pl
from jax.experimental.pallas import tpu as pltpu
from jax.sharding import PartitionSpec as P

HD = 64
BS = 64
R = 3
LANES = 128
MESH = pl.DeviceIdType.MESH

EPSILON = 1e-05
NEGATIVE = -1e30


def layer_norm(inputs, scales):
    center = jnp.mean(inputs, axis=-1, keepdims=True)
    shifted = inputs - center
    spread = jnp.mean(shifted * shifted, axis=-1, keepdims=True)
    return shifted * lax.rsqrt(spread + EPSILON) * scales


def dot_t(a, b):
    return lax.dot_general(a, b, (((1,), (1,)), ((), ())), preferred_element_type=jnp.float32)


def dot(a, b):
    return jnp.dot(a, b, preferred_element_type=jnp.float32)


def swap_halves(x):
    return pltpu.roll(x, HD, 1)


def attend_kernel(
    n,
    cap,
    heads,
    blocks,
    g_count,
    states_hbm,
    weight_hbm,
    wanted,
    slot,
    gids,
    att,
    states,
    weight,
    tab,
    tab_s,
    cand,
    cand_in,
    pick,
    gath,
    gstates,
    kvb,
    qpad,
    stage,
    rr,
    halo_l,
    halo_r,
    win,
    gq,
    gkv,
    part,
    part_in,
    gmine,
    gout,
    scores,
    s_tab,
    r_tab,
    s_cand,
    r_cand,
    s_gath,
    r_gath,
    s_rand,
    r_rand,
    s_halo,
    r_halo,
    s_part,
    r_part,
    s_gout,
    r_gout,
    s_mp,
    r_mp,
    l_sem,
    w_sem,
):
    me = lax.axis_index("seq")
    mine = lax.axis_index("mp")
    pairs = heads // 2
    width = states.shape[1]
    cols = width // LANES
    quarters = BS // 16
    half = gath.shape[0]
    gper = gath.shape[1] // (cols * quarters)
    units = gper * cols * quarters
    per = cand_in.shape[1]
    cand_parts = units // per
    rows_per = part_in.shape[2]
    part_parts = part.shape[0]
    left = lax.rem(me + n - 1, n)
    right = lax.rem(me + 1, n)

    def peer(k):
        return lax.rem(me + k, n)

    def each_peer(body):
        def step(k, carry):
            body(peer(k))
            return carry

        lax.fori_loop(1, n, step, 0)

    def guarded(limit, who, body):
        if limit < n:
            pl.when(who < limit)(body)
        else:
            body()

    def remote(src, dst, ssem, rsem, d):
        return pltpu.make_async_remote_copy(
            src_ref=src,
            dst_ref=dst,
            send_sem=ssem,
            recv_sem=rsem,
            device_id={"seq": d},
            device_id_type=MESH,
        )

    def tab_copy(d, owner):
        return remote(wanted.at[d], tab.at[owner], s_tab.at[d], r_tab.at[owner], d)

    def cand_copy(d, owner, at):
        return remote(
            cand.at[pl.ds(at * per, per)], cand_in.at[owner], s_cand.at[d], r_cand.at[owner], d
        )

    def gath_copy(d, owner):
        return remote(
            pick, gath.at[mine, pl.ds(owner * per, per)], s_gath.at[d], r_gath.at[owner], d
        )

    def rand_copy(d, owner):
        return remote(
            stage.at[pl.ds(d * cap, cap)],
            rr.at[pl.ds(owner * cap, cap)],
            s_rand.at[d],
            r_rand.at[owner],
            d,
        )

    def part_copy(d, owner, at):
        return remote(part.at[at], part_in.at[owner], s_part.at[d], r_part.at[owner], d)

    def gout_copy(d, owner):
        return remote(gmine, gout.at[owner], s_gout.at[d], r_gout.at[owner], d)

    def mp_copy(k, owner):
        other = lax.rem(mine + k, half)
        return pltpu.make_async_remote_copy(
            src_ref=gath.at[mine],
            dst_ref=gath.at[owner],
            send_sem=s_mp.at[k],
            recv_sem=r_mp.at[owner],
            device_id={"mp": other},
            device_id_type=MESH,
        )

    to_right = remote(
        kvb.at[pl.ds((blocks - 1) * heads, heads)], halo_l, s_halo.at[0], r_halo.at[0], right
    )
    to_left = remote(kvb.at[pl.ds(0, heads)], halo_r, s_halo.at[1], r_halo.at[1], left)

    loads = [pltpu.make_async_copy(states_hbm, states, w_sem.at[3])] + [
        pltpu.make_async_copy(weight_hbm.at[i], weight.at[i], w_sem.at[i]) for i in (1, 2, 0)
    ]
    for load in loads:
        load.start()

    barrier = pltpu.get_barrier_semaphore()
    each_peer(
        lambda d: pl.semaphore_signal(barrier, inc=1, device_id={"seq": d}, device_id_type=MESH)
    )
    for k in range(1, half):
        pl.semaphore_signal(
            barrier, inc=1, device_id={"mp": lax.rem(mine + k, half)}, device_id_type=MESH
        )

    loads[0].wait()
    for i in range(gper):
        local = lax.rem(gids[mine * gper + i], blocks)
        for j in range(cols):
            cut = slice(j * LANES, (j + 1) * LANES)
            piece = states[0:BS, cut]
            for b in range(1, blocks):
                piece = jnp.where(local == b, states[b * BS : (b + 1) * BS, cut], piece)
            for q in range(quarters):
                cand[(i * cols + j) * quarters + q] = piece[q * 16 : (q + 1) * 16]
    tab[me] = wanted[me]

    def own_cand():
        cand_in[me] = cand[pl.ds(me * per, per)]

    guarded(cand_parts, me, own_cand)
    loads[1].wait()
    loads[2].wait()

    lane = lax.broadcasted_iota(jnp.int32, (BS, LANES), 1)
    low = lane < HD
    x = states[...]
    for j in range(pairs):
        cut = slice(j * LANES, (j + 1) * LANES)
        k = dot(x, weight[1, :, cut])
        v = dot(x, weight[2, :, cut])
        for b in range(blocks):
            kb, vb = k[b * BS : (b + 1) * BS], v[b * BS : (b + 1) * BS]
            kvb[b * heads + 2 * j] = jnp.where(low, kb, swap_halves(vb)).astype(jnp.bfloat16)
            kvb[b * heads + 2 * j + 1] = jnp.where(low, swap_halves(kb), vb).astype(jnp.bfloat16)

    pl.semaphore_wait(barrier, n - 1 + half - 1)
    each_peer(lambda d: tab_copy(d, me).start())
    each_peer(lambda d: guarded(cand_parts, d, lambda: cand_copy(d, me, d).start()))
    to_right.start()
    to_left.start()

    loads[3].wait()
    scaling = HD ** (-0.5)
    for j in range(pairs):
        cut = slice(j * LANES, (j + 1) * LANES)
        q = dot(x, weight[0, :, cut]).astype(jnp.bfloat16).astype(jnp.float32) * scaling
        for b in range(blocks):
            qb = q[b * BS : (b + 1) * BS]
            qpad[b * heads + 2 * j] = jnp.where(low, qb, 0.0).astype(jnp.bfloat16)
            qpad[b * heads + 2 * j + 1] = jnp.where(low, swap_halves(qb), 0.0).astype(jnp.bfloat16)

    def relay():
        each_peer(lambda d: cand_copy(d, d, me).wait_recv())
        for u in range(per):
            g = (me * per + u) // (cols * quarters)
            wanted_id = gids[mine * gper + g]

            def choose(d, so_far):
                here = (wanted_id >= d * blocks) & (wanted_id < (d + 1) * blocks)
                return jnp.where(here, cand_in[d, u], so_far)

            pick[u] = lax.fori_loop(1, n, choose, cand_in[0, u])
        gath[mine, pl.ds(me * per, per)] = pick[...]
        each_peer(lambda d: gath_copy(d, me).start())

    guarded(cand_parts, me, relay)

    each_peer(lambda d: tab_copy(d, d).wait_recv())
    table = pltpu.make_async_copy(tab, tab_s, l_sem)
    table.start()
    table.wait()

    def serve(d):
        for c in range(cap):
            stage[d * cap + c] = kvb[tab_s[d, 0, c]]
        rand_copy(d, me).start()

    def serve_some(start, stop):
        def step(k, carry):
            serve(peer(k))
            return carry

        lax.fori_loop(start, stop, step, 0)

    for c in range(cap):
        rr[me * cap + c] = kvb[tab_s[me, 0, c]]

    each_peer(lambda d: guarded(cand_parts, d, lambda: gath_copy(d, d).wait_recv()))
    for k in range(1, half):
        mp_copy(k, mine).start()
    for k in range(1, half):
        mp_copy(k, lax.rem(mine + k, half)).wait_recv()
    for g in range(g_count):
        for j in range(cols):
            for q in range(quarters):
                gstates[g * BS + q * 16 : g * BS + (q + 1) * 16, j * LANES : (j + 1) * LANES] = (
                    gath[g // gper, ((g % gper) * cols + j) * quarters + q]
                )
    gx = gstates[...]
    rows = g_count * BS
    glane = lax.broadcasted_iota(jnp.int32, (rows, LANES), 1)
    glow = glane < HD
    for j in range(pairs):
        cut = slice(j * LANES, (j + 1) * LANES)
        q = dot(gx, weight[0, :, cut]).astype(jnp.bfloat16).astype(jnp.float32) * scaling
        k = dot(gx, weight[1, :, cut])
        v = dot(gx, weight[2, :, cut])
        gq[2 * j] = jnp.where(glow, q, 0.0).astype(jnp.bfloat16)
        gq[2 * j + 1] = jnp.where(glow, swap_halves(q), 0.0).astype(jnp.bfloat16)
        gkv[2 * j] = jnp.where(glow, k, swap_halves(v)).astype(jnp.bfloat16)
        gkv[2 * j + 1] = jnp.where(glow, swap_halves(k), v).astype(jnp.bfloat16)

    for h in range(heads):
        keys = jnp.concatenate([kvb[b * heads + h] for b in range(blocks)], axis=0)
        s = dot_t(gq[h], keys)
        high = jnp.max(s, axis=-1, keepdims=True)
        e = jnp.exp(s - high)
        total = jnp.sum(e, axis=-1, keepdims=True)
        e_high = e.astype(jnp.bfloat16)
        e_low = (e - e_high.astype(jnp.float32)).astype(jnp.bfloat16)
        acc = (dot(e_high, keys) + dot(e_low, keys)) * (1.0 / total)
        level = high + jnp.log(total)
        first = level.astype(jnp.bfloat16).astype(jnp.float32)
        second = (level - first).astype(jnp.bfloat16).astype(jnp.float32)
        third = level - first - second
        packed = jnp.where(
            glane < 16,
            first,
            jnp.where(glane < 32, second, jnp.where(glow, third, acc)),
        ).astype(jnp.bfloat16)
        cuts = rows // rows_per
        for c in range(cuts):
            part[(h // 2) * cuts + c, h % 2] = packed[c * rows_per : (c + 1) * rows_per]
    each_peer(lambda d: guarded(part_parts, d, lambda: part_copy(d, me, d).start()))
    serve_some(1, n)

    to_right.wait_recv()
    to_left.wait_recv()
    win[0:heads] = halo_l[...]
    win[heads : heads + blocks * heads] = kvb[...]
    win[heads + blocks * heads :] = halo_r[...]

    near = 3 + g_count
    slot_lane = lax.broadcasted_iota(jnp.int32, (BS, near * BS), 1)

    def near_keys(at, h):
        return jnp.concatenate([win[at + t * heads] for t in range(3)] + [gkv[h]], axis=0)

    def near_step(b, carry):
        first = me * blocks + b
        start = jnp.where(first == 0, BS, 0)
        stop = jnp.where(first == n * blocks - 1, 2 * BS, 3 * BS)
        outside = (slot_lane < start) | ((slot_lane >= stop) & (slot_lane < 3 * BS))
        for h in range(heads):
            at = b * heads + h
            scores[at] = jnp.where(outside, NEGATIVE, dot_t(qpad[at], near_keys(at, h)))
        return carry

    lax.fori_loop(0, blocks, near_step, 0)

    def combine():
        part_in[me] = part[me]
        each_peer(lambda d: part_copy(d, d, me).wait_recv())
        outs = []
        for parity in range(2):

            def level(d):
                piece = part_in[d, parity].astype(jnp.float32)
                return piece, piece[:, 0:1] + piece[:, 16:17] + piece[:, 32:33]

            def top(d, best):
                return jnp.maximum(best, level(d)[1])

            best = lax.fori_loop(1, n, top, level(0)[1])

            def add(d, so_far):
                piece, high = level(d)
                factor = jnp.exp(high - best)
                return so_far[0] + piece * factor, so_far[1] + factor

            zero = (jnp.zeros((rows_per, LANES), jnp.float32), jnp.zeros((rows_per, 1), jnp.float32))
            summed, total = lax.fori_loop(0, n, add, zero)
            outs.append(summed / total)
        plow = lax.broadcasted_iota(jnp.int32, (rows_per, LANES), 1) < HD
        done = jnp.where(plow, swap_halves(outs[0]), outs[1]).astype(jnp.bfloat16)
        gmine[...] = done
        gout[me] = done
        each_peer(lambda d: gout_copy(d, me).start())

    guarded(part_parts, me, combine)

    each_peer(lambda d: rand_copy(d, d).wait_recv())

    def block_step(b, carry):
        for j in range(pairs):
            halves = []
            for h in (2 * j, 2 * j + 1):
                at = b * heads + h
                early_keys = near_keys(at, h)
                keys = jnp.concatenate([rr[slot[at * R + r]] for r in range(R)], axis=0)
                s = dot_t(qpad[at], keys)
                early_s = scores[at]
                high = jnp.maximum(
                    jnp.max(s, axis=-1, keepdims=True), jnp.max(early_s, axis=-1, keepdims=True)
                )
                e = jnp.exp(s - high)
                early_e = jnp.exp(early_s - high)
                total = jnp.sum(e, axis=-1, keepdims=True) + jnp.sum(
                    early_e, axis=-1, keepdims=True
                )
                share = 1.0 / total
                w = (e * share).astype(jnp.bfloat16)
                early_w = (early_e * share).astype(jnp.bfloat16)
                halves.append(dot(w, keys) + dot(early_w, early_keys))
            att[j, pl.ds(pl.multiple_of(b * BS, BS), BS), :] = jnp.where(
                low, swap_halves(halves[0]), halves[1]
            ).astype(jnp.bfloat16)
        return carry

    lax.fori_loop(0, blocks, block_step, 0)

    each_peer(lambda d: guarded(part_parts, d, lambda: gout_copy(d, d).wait_recv()))
    for j in range(pairs):
        for g in range(g_count):
            cuts = BS // rows_per
            at = (j * g_count + g) * cuts
            row = jnp.concatenate([gout[at + c] for c in range(cuts)], axis=0).astype(jnp.float32)
            for b in range(blocks):
                here = gids[g] == me * blocks + b
                old = att[j, b * BS : (b + 1) * BS, :].astype(jnp.float32)
                att[j, b * BS : (b + 1) * BS, :] = jnp.where(here, row, old).astype(jnp.bfloat16)

    def drain(d):
        tab_copy(d, me).wait_send()
        guarded(cand_parts, d, lambda: cand_copy(d, me, d).wait_send())
        guarded(cand_parts, me, lambda: gath_copy(d, me).wait_send())
        rand_copy(d, me).wait_send()
        guarded(part_parts, d, lambda: part_copy(d, me, d).wait_send())
        guarded(part_parts, me, lambda: gout_copy(d, me).wait_send())

    each_peer(drain)
    for k in range(1, half):
        mp_copy(k, mine).wait_send()
    to_right.wait_send()
    to_left.wait_send()


TREES = ("zxy", "zyx", "yzx", "xzy")
PLACES = ((0, 0), (1, 0), (0, 1), (1, 1))
TURNS = (
    (-8.5, -3.0, -1.5, 10.5),
    (-5.5, 3.0, 0.0, 8.0),
    (-2.0, 5.0, 3.5, 13.5),
    (-1.5, 2.0, 7.5, 11.0),
)
LAG = 3
CHUNKS = 2


def arrivals(depth):
    pieces = [
        (3.5 * slot + TURNS[t][p], t, slot, *PLACES[p])
        for t in range(len(TREES))
        for slot in range(depth)
        for p in range(len(PLACES))
        if slot or p
    ]
    return [piece[1:] for piece in sorted(pieces)]


def hops(tree, slot, dx, dy):
    moved = {"x": dx, "y": dy, "z": slot}
    last = max((i for i in range(3) if moved[tree[i]]), default=-1)
    onward = tree[last + 1 :]
    via = tree[last] if last >= 0 else ""
    return via, ("z" if via == "z" else "") + onward


def slots(z, depth):
    inward = 1 if 2 * z < depth else -1
    return sorted(range(depth), key=lambda q: (abs(q - z), (z - q) * inward))


def gather_kernel(
    n,
    heads,
    blocks,
    g_count,
    chunks,
    states_hbm,
    weight_hbm,
    owner_hbm,
    local_hbm,
    gids_hbm,
    out_hbm,
    up_hbm,
    down_hbm,
    gain1_hbm,
    gain2_hbm,
    out,
    xs,
    wq,
    wkv,
    kv,
    q_all,
    wide,
    gmine,
    gout,
    owner,
    local,
    gids,
    att,
    out_w,
    up_w,
    down_w,
    gain1,
    gain2,
    mine1,
    theirs1,
    mine2,
    theirs2,
    normed,
    s_x,
    s_y,
    s_up,
    s_down,
    s_mp,
    r_ici,
    r_mp,
    s_gout,
    r_gout,
    s1,
    r1,
    s2,
    r2,
    l_sem,
):
    me = lax.axis_index("seq")
    mine = lax.axis_index("mp")
    pairs = heads // 2
    inner = heads * HD
    trees = len(TREES)
    per = 2 * trees
    piece = xs.shape[1]
    width = xs.shape[2]
    tokens = per * piece
    depth = n // 4
    units = pairs * g_count
    x_at, y_at, z_at = lax.rem(me, 2), lax.rem(me // 2, 2), me // 4

    def remote(src, dst, ssem, rsem, where):
        return pltpu.make_async_remote_copy(
            src_ref=src,
            dst_ref=dst,
            send_sem=ssem,
            recv_sem=rsem,
            device_id=where,
            device_id_type=MESH,
        )

    def peer(k):
        return lax.rem(me + k, n)

    def each_peer(body):
        def step(k, carry):
            body(peer(k))
            return carry

        lax.fori_loop(1, n, step, 0)

    def plane(slot):
        if slot == 0:
            return z_at
        found = slots(0, depth)[slot]
        for z in range(1, depth):
            found = jnp.where(z_at == z, slots(z, depth)[slot], found)
        return found

    def shard_of(slot, dx, dy):
        x = 1 - x_at if dx else x_at
        y = 1 - y_at if dy else y_at
        return plane(slot) * 4 + y * 2 + x

    def ici(shard, t, ssem, d):
        at = xs.at[(shard * 2 + mine) * trees + t]
        return remote(at, at, ssem.at[shard * trees + t], r_ici.at[shard * trees + t], {"seq": d})

    def across(shard, t, core):
        at = xs.at[(shard * 2 + core) * trees + t]
        return remote(
            at, at, s_mp.at[shard * trees + t], r_mp.at[shard * trees + t], {"mp": 1 - mine}
        )

    x_peer = me + 1 - 2 * x_at
    y_peer = me + 2 - 4 * y_at
    up, down = lax.rem(me + 4, n), lax.rem(me + n - 4, n)

    def onward(t, slot, dx, dy, act):
        shard = shard_of(slot, dx, dy)
        via, axes = hops(TREES[t], slot, dx, dy)
        for axis in axes:
            if axis == "x":
                act(ici(shard, t, s_x, x_peer))
            elif axis == "y":
                act(ici(shard, t, s_y, y_peer))
            else:
                source = plane(slot)
                go_up = z_at < depth - 1
                go_down = z_at > 0
                if via == "z":
                    go_up = go_up & (source < z_at)
                    go_down = go_down & (source > z_at)
                pl.when(go_up)(lambda: act(ici(shard, t, s_up, up)))
                pl.when(go_down)(lambda: act(ici(shard, t, s_down, down)))
        if slot or dx or dy:
            act(across(shard, t, mine))

    order = arrivals(depth)

    pairs_of = [
        (states_hbm, xs.at[pl.ds(me * per, per)]),
        (weight_hbm.at[1], wkv.at[:, 0:inner]),
        (weight_hbm.at[2], wkv.at[:, inner : 2 * inner]),
        (weight_hbm.at[0], wq),
        (owner_hbm, owner),
        (local_hbm, local),
        (gids_hbm, gids),
        (gain1_hbm, gain1),
        (gain2_hbm, gain2),
        (out_hbm, out_w),
        (up_hbm, up_w),
        (down_hbm, down_w),
    ]
    loads = [pltpu.make_async_copy(a, b, l_sem.at[i]) for i, (a, b) in enumerate(pairs_of)]
    loads[0].start()
    barrier = pltpu.get_barrier_semaphore()
    for d in (x_peer, y_peer):
        pl.semaphore_signal(barrier, inc=1, device_id={"seq": d}, device_id_type=MESH)
    pl.semaphore_signal(barrier, inc=1, device_id={"mp": 1 - mine}, device_id_type=MESH)
    for there, d in ((z_at < depth - 1, up), (z_at > 0, down)):
        pl.when(there)(
            lambda d=d: pl.semaphore_signal(
                barrier, inc=1, device_id={"seq": d}, device_id_type=MESH
            )
        )
    for load in loads[1:]:
        load.start()
    column = jnp.where(z_at < depth - 1, 1, 0) + jnp.where(z_at > 0, 1, 0)
    loads[0].wait()
    pl.semaphore_wait(barrier, 3 + column)
    for t in range(trees):
        onward(t, 0, 0, 0, lambda copy: copy.start())
    for load in loads[1:4]:
        load.wait()

    def project(shard):
        x = xs[pl.ds(shard * per, per)].reshape(tokens, width)
        y = dot(x, wkv[...]).astype(jnp.bfloat16)
        kv[pl.ds(shard * blocks, blocks)] = y.reshape(blocks, BS, 2 * inner)

    x = xs[pl.ds(me * per, per)].reshape(tokens, width)
    scaling = HD ** (-0.5)
    q_all[...] = (
        dot(x, wq[...]).astype(jnp.bfloat16).astype(jnp.float32) * scaling
    ).astype(jnp.bfloat16)
    project(me)

    waiting = []
    left = dict()

    def finish(place):
        shard = shard_of(*place)
        for t in range(trees):
            across(shard, t, 1 - mine).wait_recv()
        project(shard)

    for t, slot, dx, dy in order:
        shard = shard_of(slot, dx, dy)
        ici(shard, t, s_x, x_peer).wait_recv()
        onward(t, slot, dx, dy, lambda copy: copy.start())
        waiting = [(count - 1, place) for count, place in waiting]
        while waiting and waiting[0][0] <= 0:
            finish(waiting.pop(0)[1])
        place = (slot, dx, dy)
        left[place] = left.get(place, trees) - 1
        if left[place] == 0:
            waiting.append((LAG, place))
    for _, place in waiting:
        finish(place)
    for load in loads[4:]:
        load.wait()

    lane = lax.broadcasted_iota(jnp.int32, (BS, LANES), 1)
    low = lane < HD

    def split(q):
        zero = jnp.zeros_like(q)
        return jnp.concatenate([jnp.where(low, q, zero), jnp.where(low, zero, q)], axis=0)

    def together(out):
        return jnp.where(low, out[0:BS], out[BS : 2 * BS]).astype(jnp.bfloat16)

    chunk = wide.shape[2]
    per_chunk = chunk // BS
    steps = wide.shape[0]

    def share():
        j, g = me // g_count, lax.rem(me, g_count)
        k_cut = pl.ds(pl.multiple_of(j * LANES, LANES), LANES)
        v_cut = pl.ds(pl.multiple_of(inner + j * LANES, LANES), LANES)
        rows = BS // piece
        x = xs[pl.ds(gids[g] * rows, rows)].reshape(BS, width)
        q = dot(x, wq[:, k_cut]).astype(jnp.bfloat16).astype(jnp.float32) * scaling
        q2 = split(q.astype(jnp.bfloat16))

        def score(c, best):
            keys = kv[pl.ds(c * per_chunk, per_chunk), :, k_cut].reshape(chunk, LANES)
            s = dot_t(q2, keys)
            wide[c] = s
            return jnp.maximum(best, jnp.max(s, axis=-1, keepdims=True))

        high = lax.fori_loop(0, steps, score, jnp.full((2 * BS, 1), NEGATIVE, jnp.float32))

        def add(c, so_far):
            values = kv[pl.ds(c * per_chunk, per_chunk), :, v_cut].reshape(chunk, LANES)
            e = jnp.exp(wide[c] - high)
            e_high = e.astype(jnp.bfloat16)
            e_low = (e - e_high.astype(jnp.float32)).astype(jnp.bfloat16)
            return (
                so_far[0] + dot(e_high, values) + dot(e_low, values),
                so_far[1] + jnp.sum(e, axis=-1, keepdims=True),
            )

        zero = (jnp.zeros((2 * BS, LANES), jnp.float32), jnp.zeros((2 * BS, 1), jnp.float32))
        summed, total = lax.fori_loop(0, steps, add, zero)
        done = together(summed / total)
        gmine[...] = done
        gout[me] = done
        each_peer(lambda d: gout_copy(d, me).start())

    def gout_copy(d, unit):
        return remote(gmine, gout.at[unit], s_gout.at[d], r_gout.at[unit], {"seq": d})

    def guarded(who, body):
        if units < n:
            pl.when(who < units)(body)
        else:
            body()

    guarded(me, share)

    slot_lane = lax.broadcasted_iota(jnp.int32, (1, 3 * BS), 1)
    last = n * blocks - 1

    def block_step(b, carry):
        first = me * blocks + b
        start = jnp.where(first == 0, BS, 0)
        stop = jnp.where(first == last, 2 * BS, 3 * BS)
        bias = jnp.where((slot_lane < start) | (slot_lane >= stop), NEGATIVE, 0.0)
        near = [jnp.maximum(first - 1, 0), first, jnp.minimum(first + 1, last)]
        ends = [gids[g] for g in range(g_count)]
        for j in range(pairs):
            one = [
                owner[0, r, b, 2 * j] * blocks + local[0, r, b, 2 * j] for r in range(R)
            ]
            two = [
                owner[0, r, b, 2 * j + 1] * blocks + local[0, r, b, 2 * j + 1] for r in range(R)
            ]

            def rows(base):
                cut = slice(base + j * LANES, base + (j + 1) * LANES)
                return jnp.concatenate(
                    [kv[at, :, cut] for at in near]
                    + [jnp.where(low, kv[a, :, cut], kv[c, :, cut]) for a, c in zip(one, two)]
                    + [kv[at, :, cut] for at in ends],
                    axis=0,
                )

            q = q_all[pl.ds(pl.multiple_of(b * BS, BS), BS), j * LANES : (j + 1) * LANES]
            s = dot_t(split(q), rows(0))
            s = jnp.concatenate([s[:, 0 : 3 * BS] + bias, s[:, 3 * BS :]], axis=1)
            e = jnp.exp(s - jnp.max(s, axis=-1, keepdims=True))
            w = (e * (1.0 / jnp.sum(e, axis=-1, keepdims=True))).astype(jnp.bfloat16)
            att[j, pl.ds(pl.multiple_of(b * BS, BS), BS), :] = together(dot(w, rows(inner)))
        return carry

    lax.fori_loop(0, blocks, block_step, 0)

    each_peer(lambda d: guarded(d, lambda: gout_copy(d, d).wait_recv()))
    for j in range(pairs):
        for g in range(g_count):
            row = gout[j * g_count + g].astype(jnp.float32)
            for b in range(blocks):
                here = gids[g] == me * blocks + b
                old = att[j, b * BS : (b + 1) * BS, :].astype(jnp.float32)
                att[j, b * BS : (b + 1) * BS, :] = jnp.where(here, row, old).astype(jnp.bfloat16)

    rows = tokens // chunks

    def swap(sent, got, ssem, rsem, c):
        return remote(sent.at[c], got.at[c], ssem.at[c], rsem.at[c], {"mp": 1 - mine})

    for c in range(chunks):
        cut = slice(c * rows, (c + 1) * rows)
        acc = dot(att[0, cut, :], out_w[0:LANES, :])
        for j in range(1, pairs):
            acc = acc + dot(att[j, cut, :], out_w[j * LANES : (j + 1) * LANES, :])
        mine1[c] = acc.astype(mine1.dtype)
        swap(mine1, theirs1, s1, r1, c).start()
    x = xs[pl.ds(me * per, per)].reshape(chunks, rows, width)
    for c in range(chunks):
        swap(mine1, theirs1, s1, r1, c).wait_recv()
        summed = mine1[c].astype(jnp.float32) + theirs1[c].astype(jnp.float32)
        norm = layer_norm(x[c].astype(jnp.float32) + summed, gain1[...])
        norm = norm.astype(jnp.bfloat16)
        normed[c] = norm
        v = dot(norm, up_w[...])
        hidden = (v * (1.0 + lax.erf(v * (0.5**0.5))) * 0.5).astype(jnp.bfloat16)
        mine2[c] = dot(hidden, down_w[...]).astype(mine2.dtype)
        swap(mine2, theirs2, s2, r2, c).start()
    for c in range(chunks):
        cut = slice(c * rows, (c + 1) * rows)
        swap(mine2, theirs2, s2, r2, c).wait_recv()
        summed = mine2[c].astype(jnp.float32) + theirs2[c].astype(jnp.float32)
        out[cut, :] = layer_norm(normed[c].astype(jnp.float32) + summed, gain2[...]).astype(
            jnp.bfloat16
        )
    for c in range(chunks):
        swap(mine1, theirs1, s1, r1, c).wait_send()
        swap(mine2, theirs2, s2, r2, c).wait_send()
    for t in range(trees):
        onward(t, 0, 0, 0, lambda copy: copy.wait_send())
    for t, slot, dx, dy in order:
        onward(t, slot, dx, dy, lambda copy: copy.wait_send())
    each_peer(lambda d: guarded(me, lambda: gout_copy(d, me).wait_send()))


def tail_kernel(
    chunks,
    att,
    states,
    out_w,
    up_w,
    down_w,
    gain1,
    gain2,
    out,
    mine1,
    theirs1,
    mine2,
    theirs2,
    s1,
    r1,
    s2,
    r2,
    normed,
):
    other = 1 - lax.axis_index("mp")
    barrier = pltpu.get_barrier_semaphore()
    pl.semaphore_signal(barrier, inc=1, device_id={"mp": other}, device_id_type=MESH)
    pl.semaphore_wait(barrier, 1)
    rows = states.shape[0] // chunks

    def swap(mine, theirs, ssem, rsem, c):
        return pltpu.make_async_remote_copy(
            src_ref=mine.at[c],
            dst_ref=theirs.at[c],
            send_sem=ssem.at[c],
            recv_sem=rsem.at[c],
            device_id={"mp": other},
            device_id_type=MESH,
        )

    for c in range(chunks):
        cut = slice(c * rows, (c + 1) * rows)
        acc = dot(att[0, cut, :], out_w[0:LANES, :])
        for j in range(1, att.shape[0]):
            acc = acc + dot(att[j, cut, :], out_w[j * LANES : (j + 1) * LANES, :])
        mine1[c] = acc.astype(mine1.dtype)
        swap(mine1, theirs1, s1, r1, c).start()
    for c in range(chunks):
        cut = slice(c * rows, (c + 1) * rows)
        swap(mine1, theirs1, s1, r1, c).wait_recv()
        summed = mine1[c].astype(jnp.float32) + theirs1[c].astype(jnp.float32)
        norm = layer_norm(states[cut, :].astype(jnp.float32) + summed, gain1[...])
        norm = norm.astype(jnp.bfloat16)
        normed[c] = norm
        v = dot(norm, up_w[...])
        hidden = (v * (1.0 + lax.erf(v * (0.5**0.5))) * 0.5).astype(jnp.bfloat16)
        mine2[c] = dot(hidden, down_w[...]).astype(mine2.dtype)
        swap(mine2, theirs2, s2, r2, c).start()
    for c in range(chunks):
        cut = slice(c * rows, (c + 1) * rows)
        swap(mine2, theirs2, s2, r2, c).wait_recv()
        summed = mine2[c].astype(jnp.float32) + theirs2[c].astype(jnp.float32)
        out[cut, :] = layer_norm(normed[c].astype(jnp.float32) + summed, gain2[...]).astype(
            jnp.bfloat16
        )
    for c in range(chunks):
        swap(mine1, theirs1, s1, r1, c).wait_send()
        swap(mine2, theirs2, s2, r2, c).wait_send()


def vmem_specs(count):
    return [pl.BlockSpec(memory_space=pltpu.VMEM)] * count


def attend_requested(states, qkv_weight, global_ids, random_owner, random_local):
    tokens, width = states.shape
    heads = qkv_weight.shape[2] // HD
    pairs = heads // 2
    blocks = tokens // BS
    g_count = global_ids.shape[0]
    n = lax.axis_size("seq")

    owner = random_owner.reshape(-1)
    items = owner.shape[0]
    cap = max(2, items // n + 1)
    head_list = jnp.broadcast_to(
        jnp.arange(heads, dtype=jnp.int32)[None, :, None], (blocks, heads, R)
    ).reshape(-1)
    code = random_local.reshape(-1) * heads + head_list
    earlier = jnp.arange(items)[:, None] > jnp.arange(items)[None, :]
    rank = jnp.sum(((owner[:, None] == owner[None, :]) & earlier).astype(jnp.int32), axis=1)
    slot = owner * cap + rank
    place = owner * LANES + rank
    wanted = jnp.sum(
        jnp.where(
            place[None, None, :]
            == (jnp.arange(n)[:, None] * LANES + jnp.arange(LANES)[None, :])[:, :, None],
            code[None, None, :],
            0,
        ),
        axis=2,
    ).reshape(n, 1, LANES)

    half = lax.axis_size("mp")
    units = (g_count // half) * (width // LANES) * (BS // 16)
    per = -(-units // n)
    part_rows = pairs * g_count * BS
    rows_per = -(-part_rows // n // 16) * 16
    parts = part_rows // rows_per
    bf = jnp.bfloat16
    own = blocks * heads
    dma = pltpu.SemaphoreType.DMA
    return pl.pallas_call(
        functools.partial(attend_kernel, n, cap, heads, blocks, g_count),
        out_shape=jax.ShapeDtypeStruct((pairs, tokens, LANES), bf),
        in_specs=[pl.BlockSpec(memory_space=pltpu.HBM)] * 2
        + vmem_specs(1)
        + [pl.BlockSpec(memory_space=pltpu.SMEM)] * 2,
        out_specs=pl.BlockSpec(memory_space=pltpu.VMEM),
        scratch_shapes=[
            pltpu.VMEM((tokens, width), bf),
            pltpu.VMEM(qkv_weight.shape, bf),
            pltpu.VMEM((n, 1, LANES), jnp.int32),
            pltpu.SMEM((n, 1, LANES), jnp.int32),
            pltpu.VMEM((units, 16, LANES), bf),
            pltpu.VMEM((n, per, 16, LANES), bf),
            pltpu.VMEM((per, 16, LANES), bf),
            pltpu.VMEM((half, units, 16, LANES), bf),
            pltpu.VMEM((g_count * BS, width), bf),
            pltpu.VMEM((own, BS, LANES), bf),
            pltpu.VMEM((own, BS, LANES), bf),
            pltpu.VMEM((n * cap, BS, LANES), bf),
            pltpu.VMEM((n * cap, BS, LANES), bf),
            pltpu.VMEM((heads, BS, LANES), bf),
            pltpu.VMEM((heads, BS, LANES), bf),
            pltpu.VMEM((own + 2 * heads, BS, LANES), bf),
            pltpu.VMEM((heads, g_count * BS, LANES), bf),
            pltpu.VMEM((heads, g_count * BS, LANES), bf),
            pltpu.VMEM((parts, 2, rows_per, LANES), bf),
            pltpu.VMEM((n, 2, rows_per, LANES), bf),
            pltpu.VMEM((rows_per, LANES), bf),
            pltpu.VMEM((parts, rows_per, LANES), bf),
            pltpu.VMEM((own, BS, (3 + g_count) * BS), jnp.float32),
        ]
        + [dma((n,))] * 8
        + [dma((2,))] * 2
        + [dma((n,))] * 4
        + [dma((half,))] * 2
        + [dma(()), dma((4,))],
        cost_estimate=pl.CostEstimate(
            flops=30_000_000_000, bytes_accessed=20_000_000, transcendentals=0
        ),
        compiler_params=pltpu.CompilerParams(
            collective_id=0, has_side_effects=True, vmem_limit_bytes=32 * 1024 * 1024
        ),
    )(
        pltpu.with_memory_space_constraint(states, pltpu.HBM),
        pltpu.with_memory_space_constraint(qkv_weight, pltpu.HBM),
        wanted,
        slot,
        global_ids,
    )


def layer_gathered(
    states,
    qkv_weight,
    out_weight,
    up_weight,
    down_weight,
    attn_gain,
    mlp_gain,
    global_ids,
    random_owner,
    random_local,
):
    tokens, width = states.shape
    inner = qkv_weight.shape[2]
    heads = inner // HD
    pairs = heads // 2
    blocks = tokens // BS
    g_count = global_ids.shape[0]
    n = lax.axis_size("seq")
    trees = len(TREES)
    piece = tokens // (2 * trees)
    chunk = 8 * BS
    chunks = CHUNKS
    rows = tokens // chunks
    bf = jnp.bfloat16
    dma = pltpu.SemaphoreType.DMA
    operands = (
        states.reshape(2 * trees, piece, width),
        qkv_weight,
        random_owner.transpose(0, 3, 1, 2),
        random_local.transpose(0, 3, 1, 2),
        global_ids,
        out_weight,
        up_weight,
        down_weight,
        attn_gain.reshape(1, width),
        mlp_gain.reshape(1, width),
    )
    return pl.pallas_call(
        functools.partial(gather_kernel, n, heads, blocks, g_count, chunks),
        out_shape=jax.ShapeDtypeStruct((tokens, width), bf),
        in_specs=[pl.BlockSpec(memory_space=pltpu.HBM)] * len(operands),
        out_specs=pl.BlockSpec(memory_space=pltpu.VMEM),
        scratch_shapes=[
            pltpu.VMEM((n * 2 * trees, piece, width), bf),
            pltpu.VMEM((width, inner), bf),
            pltpu.VMEM((width, 2 * inner), bf),
            pltpu.VMEM((n * blocks, BS, 2 * inner), bf),
            pltpu.VMEM((tokens, inner), bf),
            pltpu.VMEM((n * tokens // chunk, 2 * BS, chunk), jnp.float32),
            pltpu.VMEM((BS, LANES), bf),
            pltpu.VMEM((pairs * g_count, BS, LANES), bf),
            pltpu.SMEM((1, R, blocks, heads), jnp.int32),
            pltpu.SMEM((1, R, blocks, heads), jnp.int32),
            pltpu.SMEM(global_ids.shape, jnp.int32),
            pltpu.VMEM((pairs, tokens, LANES), bf),
            pltpu.VMEM(out_weight.shape, bf),
            pltpu.VMEM(up_weight.shape, bf),
            pltpu.VMEM(down_weight.shape, bf),
            pltpu.VMEM((1, width), jnp.float32),
            pltpu.VMEM((1, width), jnp.float32),
        ]
        + [pltpu.VMEM((chunks, rows, width), bf)] * 5
        + [dma((n * trees,))] * 7
        + [dma((n,)), dma((pairs * g_count,))]
        + [dma((chunks,))] * 4
        + [dma((len(operands) + 2,))],
        compiler_params=pltpu.CompilerParams(
            collective_id=0, has_side_effects=True, vmem_limit_bytes=48 * 1024 * 1024
        ),
    )(*[pltpu.with_memory_space_constraint(a, pltpu.HBM) for a in operands])


def gathers(states, qkv_weight, global_ids):
    tokens, width = states.shape
    n = lax.axis_size("seq")
    inner = qkv_weight.shape[2]
    held = n * tokens * (width + 2 * inner) * 2
    units = inner // LANES * global_ids.shape[0]
    return (
        n % 4 == 0
        and lax.axis_size("mp") == 2
        and held <= 24 * 1024 * 1024
        and units <= n
        and tokens % (2 * len(TREES) * 16) == 0
        and 2 * inner % 256 == 0
    )


def shards(
    states,
    qkv_weight,
    out_weight,
    up_weight,
    down_weight,
    attn_gain,
    mlp_gain,
    global_ids,
    random_owner,
    random_local,
):
    tokens, width = states.shape
    if gathers(states, qkv_weight, global_ids):
        return layer_gathered(
            states,
            qkv_weight,
            out_weight,
            up_weight,
            down_weight,
            attn_gain,
            mlp_gain,
            global_ids,
            random_owner,
            random_local,
        )
    bf = jnp.bfloat16
    dma = pltpu.SemaphoreType.DMA
    att = attend_requested(states, qkv_weight, global_ids, random_owner, random_local)

    chunks = 4
    rows = tokens // chunks
    link = jnp.bfloat16
    return pl.pallas_call(
        functools.partial(tail_kernel, chunks),
        out_shape=jax.ShapeDtypeStruct((tokens, width), bf),
        in_specs=vmem_specs(7),
        out_specs=pl.BlockSpec(memory_space=pltpu.VMEM),
        scratch_shapes=[pltpu.VMEM((chunks, rows, width), link)] * 4
        + [dma((chunks,))] * 4
        + [pltpu.VMEM((chunks, rows, width), bf)],
        compiler_params=pltpu.CompilerParams(
            collective_id=1, has_side_effects=True, vmem_limit_bytes=32 * 1024 * 1024
        ),
    )(
        att,
        states,
        out_weight,
        up_weight,
        down_weight,
        attn_gain.reshape(1, width),
        mlp_gain.reshape(1, width),
    )


def solution(mesh):
    in_specs = (
        P("seq", None),
        P(None, None, "mp"),
        P("mp", None),
        P(None, "mp"),
        P("mp", None),
        P(),
        P(),
        P(),
        P("mp", "seq", None, None),
        P("mp", "seq", None, None),
    )
    out_specs = P("seq", None)
    return jax.shard_map(shards, mesh=mesh, in_specs=in_specs, out_specs=out_specs, check_vma=False)
```

```python
import functools

import jax
import jax.numpy as jnp
from jax import lax
from jax.experimental import pallas as pl
from jax.experimental.pallas import tpu as pltpu
from jax.sharding import PartitionSpec as P

HD = 64
BS = 64
R = 3
LANES = 128
MESH = pl.DeviceIdType.MESH

EPSILON = 1e-05
NEGATIVE = -1e30


def layer_norm(inputs, scales):
    center = jnp.mean(inputs, axis=-1, keepdims=True)
    shifted = inputs - center
    spread = jnp.mean(shifted * shifted, axis=-1, keepdims=True)
    return shifted * lax.rsqrt(spread + EPSILON) * scales


def dot_t(a, b):
    return lax.dot_general(a, b, (((1,), (1,)), ((), ())), preferred_element_type=jnp.float32)


def dot(a, b):
    return jnp.dot(a, b, preferred_element_type=jnp.float32)


def swap_halves(x):
    return pltpu.roll(x, HD, 1)


def attend_kernel(
    n,
    cap,
    heads,
    blocks,
    g_count,
    states_hbm,
    weight_hbm,
    wanted,
    slot,
    gids,
    att,
    states,
    weight,
    tab,
    tab_s,
    cand,
    cand_in,
    pick,
    gath,
    gstates,
    kvb,
    qpad,
    stage,
    rr,
    halo_l,
    halo_r,
    win,
    gq,
    gkv,
    part,
    part_in,
    gmine,
    gout,
    scores,
    s_tab,
    r_tab,
    s_cand,
    r_cand,
    s_gath,
    r_gath,
    s_rand,
    r_rand,
    s_halo,
    r_halo,
    s_part,
    r_part,
    s_gout,
    r_gout,
    s_mp,
    r_mp,
    l_sem,
    w_sem,
):
    me = lax.axis_index("seq")
    mine = lax.axis_index("mp")
    pairs = heads // 2
    width = states.shape[1]
    cols = width // LANES
    quarters = BS // 16
    half = gath.shape[0]
    gper = gath.shape[1] // (cols * quarters)
    units = gper * cols * quarters
    per = cand_in.shape[1]
    cand_parts = units // per
    rows_per = part_in.shape[2]
    part_parts = part.shape[0]
    left = lax.rem(me + n - 1, n)
    right = lax.rem(me + 1, n)

    def peer(k):
        return lax.rem(me + k, n)

    def each_peer(body):
        def step(k, carry):
            body(peer(k))
            return carry

        lax.fori_loop(1, n, step, 0)

    def guarded(limit, who, body):
        if limit < n:
            pl.when(who < limit)(body)
        else:
            body()

    def remote(src, dst, ssem, rsem, d):
        return pltpu.make_async_remote_copy(
            src_ref=src,
            dst_ref=dst,
            send_sem=ssem,
            recv_sem=rsem,
            device_id={"seq": d},
            device_id_type=MESH,
        )

    def tab_copy(d, owner):
        return remote(wanted.at[d], tab.at[owner], s_tab.at[d], r_tab.at[owner], d)

    def cand_copy(d, owner, at):
        return remote(
            cand.at[pl.ds(at * per, per)], cand_in.at[owner], s_cand.at[d], r_cand.at[owner], d
        )

    def gath_copy(d, owner):
        return remote(
            pick, gath.at[mine, pl.ds(owner * per, per)], s_gath.at[d], r_gath.at[owner], d
        )

    def rand_copy(d, owner):
        return remote(
            stage.at[pl.ds(d * cap, cap)],
            rr.at[pl.ds(owner * cap, cap)],
            s_rand.at[d],
            r_rand.at[owner],
            d,
        )

    def part_copy(d, owner, at):
        return remote(part.at[at], part_in.at[owner], s_part.at[d], r_part.at[owner], d)

    def gout_copy(d, owner):
        return remote(gmine, gout.at[owner], s_gout.at[d], r_gout.at[owner], d)

    def mp_copy(k, owner):
        other = lax.rem(mine + k, half)
        return pltpu.make_async_remote_copy(
            src_ref=gath.at[mine],
            dst_ref=gath.at[owner],
            send_sem=s_mp.at[k],
            recv_sem=r_mp.at[owner],
            device_id={"mp": other},
            device_id_type=MESH,
        )

    to_right = remote(
        kvb.at[pl.ds((blocks - 1) * heads, heads)], halo_l, s_halo.at[0], r_halo.at[0], right
    )
    to_left = remote(kvb.at[pl.ds(0, heads)], halo_r, s_halo.at[1], r_halo.at[1], left)

    loads = [pltpu.make_async_copy(states_hbm, states, w_sem.at[3])] + [
        pltpu.make_async_copy(weight_hbm.at[i], weight.at[i], w_sem.at[i]) for i in (1, 2, 0)
    ]
    for load in loads:
        load.start()

    barrier = pltpu.get_barrier_semaphore()
    each_peer(
        lambda d: pl.semaphore_signal(barrier, inc=1, device_id={"seq": d}, device_id_type=MESH)
    )
    for k in range(1, half):
        pl.semaphore_signal(
            barrier, inc=1, device_id={"mp": lax.rem(mine + k, half)}, device_id_type=MESH
        )

    loads[0].wait()
    for i in range(gper):
        local = lax.rem(gids[mine * gper + i], blocks)
        for j in range(cols):
            cut = slice(j * LANES, (j + 1) * LANES)
            piece = states[0:BS, cut]
            for b in range(1, blocks):
                piece = jnp.where(local == b, states[b * BS : (b + 1) * BS, cut], piece)
            for q in range(quarters):
                cand[(i * cols + j) * quarters + q] = piece[q * 16 : (q + 1) * 16]
    tab[me] = wanted[me]

    def own_cand():
        cand_in[me] = cand[pl.ds(me * per, per)]

    guarded(cand_parts, me, own_cand)
    loads[1].wait()
    loads[2].wait()

    lane = lax.broadcasted_iota(jnp.int32, (BS, LANES), 1)
    low = lane < HD
    x = states[...]
    for j in range(pairs):
        cut = slice(j * LANES, (j + 1) * LANES)
        k = dot(x, weight[1, :, cut])
        v = dot(x, weight[2, :, cut])
        for b in range(blocks):
            kb, vb = k[b * BS : (b + 1) * BS], v[b * BS : (b + 1) * BS]
            kvb[b * heads + 2 * j] = jnp.where(low, kb, swap_halves(vb)).astype(jnp.bfloat16)
            kvb[b * heads + 2 * j + 1] = jnp.where(low, swap_halves(kb), vb).astype(jnp.bfloat16)

    pl.semaphore_wait(barrier, n - 1 + half - 1)
    each_peer(lambda d: tab_copy(d, me).start())
    each_peer(lambda d: guarded(cand_parts, d, lambda: cand_copy(d, me, d).start()))
    to_right.start()
    to_left.start()

    loads[3].wait()
    scaling = HD ** (-0.5)
    for j in range(pairs):
        cut = slice(j * LANES, (j + 1) * LANES)
        q = dot(x, weight[0, :, cut]).astype(jnp.bfloat16).astype(jnp.float32) * scaling
        for b in range(blocks):
            qb = q[b * BS : (b + 1) * BS]
            qpad[b * heads + 2 * j] = jnp.where(low, qb, 0.0).astype(jnp.bfloat16)
            qpad[b * heads + 2 * j + 1] = jnp.where(low, swap_halves(qb), 0.0).astype(jnp.bfloat16)

    def relay():
        each_peer(lambda d: cand_copy(d, d, me).wait_recv())
        for u in range(per):
            g = (me * per + u) // (cols * quarters)
            wanted_id = gids[mine * gper + g]

            def choose(d, so_far):
                here = (wanted_id >= d * blocks) & (wanted_id < (d + 1) * blocks)
                return jnp.where(here, cand_in[d, u], so_far)

            pick[u] = lax.fori_loop(1, n, choose, cand_in[0, u])
        gath[mine, pl.ds(me * per, per)] = pick[...]
        each_peer(lambda d: gath_copy(d, me).start())

    guarded(cand_parts, me, relay)

    each_peer(lambda d: tab_copy(d, d).wait_recv())
    table = pltpu.make_async_copy(tab, tab_s, l_sem)
    table.start()
    table.wait()

    def serve(d):
        for c in range(cap):
            stage[d * cap + c] = kvb[tab_s[d, 0, c]]
        rand_copy(d, me).start()

    def serve_some(start, stop):
        def step(k, carry):
            serve(peer(k))
            return carry

        lax.fori_loop(start, stop, step, 0)

    for c in range(cap):
        rr[me * cap + c] = kvb[tab_s[me, 0, c]]

    each_peer(lambda d: guarded(cand_parts, d, lambda: gath_copy(d, d).wait_recv()))
    for k in range(1, half):
        mp_copy(k, mine).start()
    for k in range(1, half):
        mp_copy(k, lax.rem(mine + k, half)).wait_recv()
    for g in range(g_count):
        for j in range(cols):
            for q in range(quarters):
                gstates[g * BS + q * 16 : g * BS + (q + 1) * 16, j * LANES : (j + 1) * LANES] = (
                    gath[g // gper, ((g % gper) * cols + j) * quarters + q]
                )
    gx = gstates[...]
    rows = g_count * BS
    glane = lax.broadcasted_iota(jnp.int32, (rows, LANES), 1)
    glow = glane < HD
    for j in range(pairs):
        cut = slice(j * LANES, (j + 1) * LANES)
        q = dot(gx, weight[0, :, cut]).astype(jnp.bfloat16).astype(jnp.float32) * scaling
        k = dot(gx, weight[1, :, cut])
        v = dot(gx, weight[2, :, cut])
        gq[2 * j] = jnp.where(glow, q, 0.0).astype(jnp.bfloat16)
        gq[2 * j + 1] = jnp.where(glow, swap_halves(q), 0.0).astype(jnp.bfloat16)
        gkv[2 * j] = jnp.where(glow, k, swap_halves(v)).astype(jnp.bfloat16)
        gkv[2 * j + 1] = jnp.where(glow, swap_halves(k), v).astype(jnp.bfloat16)

    for h in range(heads):
        keys = jnp.concatenate([kvb[b * heads + h] for b in range(blocks)], axis=0)
        s = dot_t(gq[h], keys)
        high = jnp.max(s, axis=-1, keepdims=True)
        e = jnp.exp(s - high)
        total = jnp.sum(e, axis=-1, keepdims=True)
        e_high = e.astype(jnp.bfloat16)
        e_low = (e - e_high.astype(jnp.float32)).astype(jnp.bfloat16)
        acc = (dot(e_high, keys) + dot(e_low, keys)) * (1.0 / total)
        level = high + jnp.log(total)
        first = level.astype(jnp.bfloat16).astype(jnp.float32)
        second = (level - first).astype(jnp.bfloat16).astype(jnp.float32)
        third = level - first - second
        packed = jnp.where(
            glane < 16,
            first,
            jnp.where(glane < 32, second, jnp.where(glow, third, acc)),
        ).astype(jnp.bfloat16)
        cuts = rows // rows_per
        for c in range(cuts):
            part[(h // 2) * cuts + c, h % 2] = packed[c * rows_per : (c + 1) * rows_per]
    each_peer(lambda d: guarded(part_parts, d, lambda: part_copy(d, me, d).start()))
    serve_some(1, n)

    to_right.wait_recv()
    to_left.wait_recv()
    win[0:heads] = halo_l[...]
    win[heads : heads + blocks * heads] = kvb[...]
    win[heads + blocks * heads :] = halo_r[...]

    near = 3 + g_count
    slot_lane = lax.broadcasted_iota(jnp.int32, (BS, near * BS), 1)

    def near_keys(at, h):
        return jnp.concatenate([win[at + t * heads] for t in range(3)] + [gkv[h]], axis=0)

    def near_step(b, carry):
        first = me * blocks + b
        start = jnp.where(first == 0, BS, 0)
        stop = jnp.where(first == n * blocks - 1, 2 * BS, 3 * BS)
        outside = (slot_lane < start) | ((slot_lane >= stop) & (slot_lane < 3 * BS))
        for h in range(heads):
            at = b * heads + h
            scores[at] = jnp.where(outside, NEGATIVE, dot_t(qpad[at], near_keys(at, h)))
        return carry

    lax.fori_loop(0, blocks, near_step, 0)

    def combine():
        part_in[me] = part[me]
        each_peer(lambda d: part_copy(d, d, me).wait_recv())
        outs = []
        for parity in range(2):

            def level(d):
                piece = part_in[d, parity].astype(jnp.float32)
                return piece, piece[:, 0:1] + piece[:, 16:17] + piece[:, 32:33]

            def top(d, best):
                return jnp.maximum(best, level(d)[1])

            best = lax.fori_loop(1, n, top, level(0)[1])

            def add(d, so_far):
                piece, high = level(d)
                factor = jnp.exp(high - best)
                return so_far[0] + piece * factor, so_far[1] + factor

            zero = (jnp.zeros((rows_per, LANES), jnp.float32), jnp.zeros((rows_per, 1), jnp.float32))
            summed, total = lax.fori_loop(0, n, add, zero)
            outs.append(summed / total)
        plow = lax.broadcasted_iota(jnp.int32, (rows_per, LANES), 1) < HD
        done = jnp.where(plow, swap_halves(outs[0]), outs[1]).astype(jnp.bfloat16)
        gmine[...] = done
        gout[me] = done
        each_peer(lambda d: gout_copy(d, me).start())

    guarded(part_parts, me, combine)

    each_peer(lambda d: rand_copy(d, d).wait_recv())

    def block_step(b, carry):
        for j in range(pairs):
            halves = []
            for h in (2 * j, 2 * j + 1):
                at = b * heads + h
                early_keys = near_keys(at, h)
                keys = jnp.concatenate([rr[slot[at * R + r]] for r in range(R)], axis=0)
                s = dot_t(qpad[at], keys)
                early_s = scores[at]
                high = jnp.maximum(
                    jnp.max(s, axis=-1, keepdims=True), jnp.max(early_s, axis=-1, keepdims=True)
                )
                e = jnp.exp(s - high)
                early_e = jnp.exp(early_s - high)
                total = jnp.sum(e, axis=-1, keepdims=True) + jnp.sum(
                    early_e, axis=-1, keepdims=True
                )
                share = 1.0 / total
                w = (e * share).astype(jnp.bfloat16)
                early_w = (early_e * share).astype(jnp.bfloat16)
                halves.append(dot(w, keys) + dot(early_w, early_keys))
            att[j, pl.ds(pl.multiple_of(b * BS, BS), BS), :] = jnp.where(
                low, swap_halves(halves[0]), halves[1]
            ).astype(jnp.bfloat16)
        return carry

    lax.fori_loop(0, blocks, block_step, 0)

    each_peer(lambda d: guarded(part_parts, d, lambda: gout_copy(d, d).wait_recv()))
    for j in range(pairs):
        for g in range(g_count):
            cuts = BS // rows_per
            at = (j * g_count + g) * cuts
            row = jnp.concatenate([gout[at + c] for c in range(cuts)], axis=0).astype(jnp.float32)
            for b in range(blocks):
                here = gids[g] == me * blocks + b
                old = att[j, b * BS : (b + 1) * BS, :].astype(jnp.float32)
                att[j, b * BS : (b + 1) * BS, :] = jnp.where(here, row, old).astype(jnp.bfloat16)

    def drain(d):
        tab_copy(d, me).wait_send()
        guarded(cand_parts, d, lambda: cand_copy(d, me, d).wait_send())
        guarded(cand_parts, me, lambda: gath_copy(d, me).wait_send())
        rand_copy(d, me).wait_send()
        guarded(part_parts, d, lambda: part_copy(d, me, d).wait_send())
        guarded(part_parts, me, lambda: gout_copy(d, me).wait_send())

    each_peer(drain)
    for k in range(1, half):
        mp_copy(k, mine).wait_send()
    to_right.wait_send()
    to_left.wait_send()


TREES = ("zxy", "zyx", "yzx", "xzy")
PLACES = ((0, 0), (1, 0), (0, 1), (1, 1))
TURNS = (
    (-8.5, -3.0, -1.5, 10.5),
    (-5.5, 3.0, 0.0, 8.0),
    (-2.0, 5.0, 3.5, 13.5),
    (-1.5, 2.0, 7.5, 11.0),
)
LAG = 6
CHUNKS = 2


def arrivals(depth):
    pieces = [
        (3.5 * slot + TURNS[t][p], t, slot, *PLACES[p])
        for t in range(len(TREES))
        for slot in range(depth)
        for p in range(len(PLACES))
        if slot or p
    ]
    return [piece[1:] for piece in sorted(pieces)]


def hops(tree, slot, dx, dy):
    moved = {"x": dx, "y": dy, "z": slot}
    last = max((i for i in range(3) if moved[tree[i]]), default=-1)
    onward = tree[last + 1 :]
    via = tree[last] if last >= 0 else ""
    return via, ("z" if via == "z" else "") + onward


def slots(z, depth):
    inward = 1 if 2 * z < depth else -1
    return sorted(range(depth), key=lambda q: (abs(q - z), (z - q) * inward))


def gather_kernel(
    n,
    heads,
    blocks,
    g_count,
    chunks,
    states_hbm,
    weight_hbm,
    owner_hbm,
    local_hbm,
    gids_hbm,
    out_hbm,
    up_hbm,
    down_hbm,
    gain1_hbm,
    gain2_hbm,
    out,
    xs,
    wq,
    wkv,
    kv,
    q_all,
    wide,
    scores,
    weights,
    gmine,
    gout,
    owner,
    local,
    gids,
    att,
    out_w,
    up_w,
    down_w,
    gain1,
    gain2,
    mine1,
    theirs1,
    mine2,
    theirs2,
    normed,
    s_x,
    s_y,
    s_up,
    s_down,
    s_mp,
    r_ici,
    r_mp,
    s_gout,
    r_gout,
    s1,
    r1,
    s2,
    r2,
    l_sem,
):
    me = lax.axis_index("seq")
    mine = lax.axis_index("mp")
    pairs = heads // 2
    inner = heads * HD
    trees = len(TREES)
    per = 2 * trees
    piece = xs.shape[1]
    width = xs.shape[2]
    tokens = per * piece
    depth = n // 4
    x_at, y_at, z_at = lax.rem(me, 2), lax.rem(me // 2, 2), me // 4

    def remote(src, dst, ssem, rsem, where):
        return pltpu.make_async_remote_copy(
            src_ref=src,
            dst_ref=dst,
            send_sem=ssem,
            recv_sem=rsem,
            device_id=where,
            device_id_type=MESH,
        )

    def plane(slot):
        if slot == 0:
            return z_at
        found = slots(0, depth)[slot]
        for z in range(1, depth):
            found = jnp.where(z_at == z, slots(z, depth)[slot], found)
        return found

    def shard_of(slot, dx, dy):
        x = 1 - x_at if dx else x_at
        y = 1 - y_at if dy else y_at
        return plane(slot) * 4 + y * 2 + x

    def ici(shard, t, ssem, d):
        at = xs.at[(shard * 2 + mine) * trees + t]
        return remote(at, at, ssem.at[shard * trees + t], r_ici.at[shard * trees + t], {"seq": d})

    def across(shard, core):
        at = xs.at[pl.ds((shard * 2 + core) * trees, trees)]
        return remote(at, at, s_mp.at[shard], r_mp.at[shard], {"mp": 1 - mine})

    x_peer = me + 1 - 2 * x_at
    y_peer = me + 2 - 4 * y_at
    up, down = lax.rem(me + 4, n), lax.rem(me + n - 4, n)

    def onward(t, slot, dx, dy, act):
        shard = shard_of(slot, dx, dy)
        via, axes = hops(TREES[t], slot, dx, dy)
        for axis in axes:
            if axis == "x":
                act(ici(shard, t, s_x, x_peer))
            elif axis == "y":
                act(ici(shard, t, s_y, y_peer))
            else:
                source = plane(slot)
                go_up = z_at < depth - 1
                go_down = z_at > 0
                if via == "z":
                    go_up = go_up & (source < z_at)
                    go_down = go_down & (source > z_at)
                pl.when(go_up)(lambda: act(ici(shard, t, s_up, up)))
                pl.when(go_down)(lambda: act(ici(shard, t, s_down, down)))

    order = arrivals(depth)

    pairs_of = [
        (states_hbm, xs.at[pl.ds(me * per, per)]),
        (weight_hbm.at[1], wkv.at[:, 0:inner]),
        (weight_hbm.at[2], wkv.at[:, inner : 2 * inner]),
        (weight_hbm.at[0], wq),
        (owner_hbm, owner),
        (local_hbm, local),
        (gids_hbm, gids),
        (gain1_hbm, gain1),
        (gain2_hbm, gain2),
        (out_hbm, out_w),
        (up_hbm, up_w),
        (down_hbm, down_w),
    ]
    loads = [pltpu.make_async_copy(a, b, l_sem.at[i]) for i, (a, b) in enumerate(pairs_of)]
    loads[0].start()
    barrier = pltpu.get_barrier_semaphore()
    for d in (x_peer, y_peer):
        pl.semaphore_signal(barrier, inc=1, device_id={"seq": d}, device_id_type=MESH)
    pl.semaphore_signal(barrier, inc=1, device_id={"mp": 1 - mine}, device_id_type=MESH)
    for there, d in ((z_at < depth - 1, up), (z_at > 0, down)):
        pl.when(there)(
            lambda d=d: pl.semaphore_signal(
                barrier, inc=1, device_id={"seq": d}, device_id_type=MESH
            )
        )
    for load in loads[1:]:
        load.start()
    column = jnp.where(z_at < depth - 1, 1, 0) + jnp.where(z_at > 0, 1, 0)
    loads[0].wait()
    pl.semaphore_wait(barrier, 3 + column)
    for t in range(trees):
        onward(t, 0, 0, 0, lambda copy: copy.start())
    for load in loads[1:4]:
        load.wait()

    def project(shard):
        x = xs[pl.ds(shard * per, per)].reshape(tokens, width)
        y = dot(x, wkv[...]).astype(jnp.bfloat16)
        kv[pl.ds(shard * blocks, blocks)] = y.reshape(blocks, BS, 2 * inner)

    x = xs[pl.ds(me * per, per)].reshape(tokens, width)
    scaling = HD ** (-0.5)
    q_all[...] = (
        dot(x, wq[...]).astype(jnp.bfloat16).astype(jnp.float32) * scaling
    ).astype(jnp.bfloat16)
    project(me)

    waiting = []
    left = dict()

    def finish(place):
        shard = shard_of(*place)
        across(shard, 1 - mine).wait_recv()
        project(shard)

    for t, slot, dx, dy in order:
        shard = shard_of(slot, dx, dy)
        ici(shard, t, s_x, x_peer).wait_recv()
        onward(t, slot, dx, dy, lambda copy: copy.start())
        waiting = [(count - 1, place) for count, place in waiting]
        while waiting and waiting[0][0] <= 0:
            finish(waiting.pop(0)[1])
        place = (slot, dx, dy)
        left[place] = left.get(place, trees) - 1
        if left[place] == 0:
            across(shard, mine).start()
            waiting.append((LAG, place))
    for _, place in waiting:
        finish(place)
    for load in loads[4:]:
        load.wait()

    lane = lax.broadcasted_iota(jnp.int32, (BS, LANES), 1)
    low = lane < HD

    def split(q):
        zero = jnp.zeros_like(q)
        return jnp.concatenate([jnp.where(low, q, zero), jnp.where(low, zero, q)], axis=0)

    def together(out):
        return jnp.where(low, out[0:BS], out[BS : 2 * BS]).astype(jnp.bfloat16)

    spot = lax.rem(me, 4)
    final = n - 1
    steps, _, chunk = wide.shape
    per_chunk = chunk // BS

    def fold(best, s, join):
        for c in range(0, s.shape[1], LANES):
            best = join(best, s[:, c : c + LANES])
        return best

    def share():
        first_block = spot < pairs
        j = jnp.where(first_block, spot, z_at)
        block = jnp.where(first_block, gids[0], gids[1])
        k_cut = pl.ds(pl.multiple_of(j * LANES, LANES), LANES)
        v_cut = pl.ds(pl.multiple_of(inner + j * LANES, LANES), LANES)
        rows = BS // piece
        x = xs[pl.ds(block * rows, rows)].reshape(BS, width)
        q = dot(x, wq[:, k_cut]).astype(jnp.bfloat16).astype(jnp.float32) * scaling
        q2 = split(q.astype(jnp.bfloat16))

        def score(c, best):
            keys = kv[pl.ds(c * per_chunk, per_chunk), :, k_cut].reshape(chunk, LANES)
            s = dot_t(q2, keys)
            wide[c] = s
            return fold(best, s, jnp.maximum)

        best = jnp.full((2 * BS, LANES), NEGATIVE, jnp.float32)
        best = lax.fori_loop(0, steps, score, best, unroll=True)
        high = jnp.max(best, axis=-1, keepdims=True)

        def add(c, so_far):
            values = kv[pl.ds(c * per_chunk, per_chunk), :, v_cut].reshape(chunk, LANES)
            e = jnp.exp(wide[c] - high)
            e_high = e.astype(jnp.bfloat16)
            e_low = (e - e_high.astype(jnp.float32)).astype(jnp.bfloat16)
            return (
                so_far[0] + dot(e_high, values) + dot(e_low, values),
                fold(so_far[1], e, jnp.add),
            )

        zero = jnp.zeros((2 * BS, LANES), jnp.float32)
        summed, total = lax.fori_loop(0, steps, add, (zero, zero), unroll=True)
        gmine[...] = together(summed / jnp.sum(total, axis=-1, keepdims=True))

        def to_plane():
            for k in range(1, 4):
                gout_copy(spot, k).start()

        pl.when(first_block)(to_plane)
        pl.when(spot >= pairs)(lambda: last_copy(z_at).start())

    def gout_copy(unit, k):
        d = z_at * 4 + lax.rem(spot + k, 4)
        return remote(gmine, gout.at[unit], s_gout.at[k], r_gout.at[unit], {"seq": d})

    def last_copy(unit):
        at = pairs + unit
        return remote(gmine, gout.at[at], s_gout.at[0], r_gout.at[at], {"seq": final})

    shares = (spot < pairs) | ((spot == 3) & (z_at < pairs))
    pl.when(shares)(share)

    slot_lane = lax.broadcasted_iota(jnp.int32, (1, 3 * BS), 1)
    last = n * blocks - 1

    def rows_of(b, j, base):
        first = me * blocks + b
        near = [jnp.maximum(first - 1, 0), first, jnp.minimum(first + 1, last)]
        one = [owner[0, r, b, 2 * j] * blocks + local[0, r, b, 2 * j] for r in range(R)]
        two = [owner[0, r, b, 2 * j + 1] * blocks + local[0, r, b, 2 * j + 1] for r in range(R)]
        cut = slice(base + j * LANES, base + (j + 1) * LANES)
        return jnp.concatenate(
            [kv[at, :, cut] for at in near]
            + [jnp.where(low, kv[a, :, cut], kv[c, :, cut]) for a, c in zip(one, two)]
            + [kv[gids[g], :, cut] for g in range(g_count)],
            axis=0,
        )

    for b in range(blocks):
        first = me * blocks + b
        start = jnp.where(first == 0, BS, 0)
        stop = jnp.where(first == last, 2 * BS, 3 * BS)
        bias = jnp.where((slot_lane < start) | (slot_lane >= stop), NEGATIVE, 0.0)
        for j in range(pairs):
            q = q_all[b * BS : (b + 1) * BS, j * LANES : (j + 1) * LANES]
            s = dot_t(split(q), rows_of(b, j, 0))
            scores[b * pairs + j, :, 0 : 3 * BS] = s[:, 0 : 3 * BS] + bias
            scores[b * pairs + j, :, 3 * BS :] = s[:, 3 * BS :]

    def weigh(i, carry):
        for part in range(2):
            cut = slice(part * BS, (part + 1) * BS)
            s = scores[i, cut]
            e = jnp.exp(s - jnp.max(s, axis=-1, keepdims=True))
            share_of = 1.0 / jnp.sum(e, axis=-1, keepdims=True)
            weights[i, cut] = (e * share_of).astype(jnp.bfloat16)
        return carry

    lax.fori_loop(0, blocks * pairs, weigh, 0, unroll=6)

    for b in range(blocks):
        for j in range(pairs):
            mixed = dot(weights[b * pairs + j], rows_of(b, j, inner))
            att[j, b * BS : (b + 1) * BS, :] = together(mixed)

    for unit in range(pairs):
        pl.when(spot != unit)(lambda unit=unit: gout_copy(unit, 1).wait_recv())
    for j in range(pairs):
        row = jnp.where(spot == j, gmine[...], gout[j])
        for b in range(blocks):
            cut = slice(b * BS, (b + 1) * BS)
            here = gids[0] == me * blocks + b
            att[j, cut, :] = jnp.where(here, row, att[j, cut, :])

    def take_last():
        for unit in range(pairs):
            last_copy(unit).wait_recv()
            att[unit, (blocks - 1) * BS : blocks * BS, :] = gout[pairs + unit]

    pl.when(me == final)(take_last)

    rows = tokens // chunks

    def swap(sent, got, ssem, rsem, c):
        return remote(sent.at[c], got.at[c], ssem.at[c], rsem.at[c], {"mp": 1 - mine})

    for c in range(chunks):
        cut = slice(c * rows, (c + 1) * rows)
        acc = dot(att[0, cut, :], out_w[0:LANES, :])
        for j in range(1, pairs):
            acc = acc + dot(att[j, cut, :], out_w[j * LANES : (j + 1) * LANES, :])
        mine1[c] = acc.astype(mine1.dtype)
        swap(mine1, theirs1, s1, r1, c).start()
    x = xs[pl.ds(me * per, per)].reshape(chunks, rows, width)
    for c in range(chunks):
        swap(mine1, theirs1, s1, r1, c).wait_recv()
        summed = mine1[c].astype(jnp.float32) + theirs1[c].astype(jnp.float32)
        norm = layer_norm(x[c].astype(jnp.float32) + summed, gain1[...])
        norm = norm.astype(jnp.bfloat16)
        normed[c] = norm
        v = dot(norm, up_w[...])
        hidden = (v * (1.0 + lax.erf(v * (0.5**0.5))) * 0.5).astype(jnp.bfloat16)
        mine2[c] = dot(hidden, down_w[...]).astype(mine2.dtype)
        swap(mine2, theirs2, s2, r2, c).start()
    for c in range(chunks):
        cut = slice(c * rows, (c + 1) * rows)
        swap(mine2, theirs2, s2, r2, c).wait_recv()
        summed = mine2[c].astype(jnp.float32) + theirs2[c].astype(jnp.float32)
        out[cut, :] = layer_norm(normed[c].astype(jnp.float32) + summed, gain2[...]).astype(
            jnp.bfloat16
        )
    for c in range(chunks):
        swap(mine1, theirs1, s1, r1, c).wait_send()
        swap(mine2, theirs2, s2, r2, c).wait_send()
    for t in range(trees):
        onward(t, 0, 0, 0, lambda copy: copy.wait_send())
    for t, slot, dx, dy in order:
        onward(t, slot, dx, dy, lambda copy: copy.wait_send())
    for place in left:
        across(shard_of(*place), mine).wait_send()

    def drain():
        for k in range(1, 4):
            gout_copy(spot, k).wait_send()

    pl.when(spot < pairs)(drain)
    pl.when((spot == 3) & (z_at < pairs))(lambda: last_copy(z_at).wait_send())


def tail_kernel(
    chunks,
    att,
    states,
    out_w,
    up_w,
    down_w,
    gain1,
    gain2,
    out,
    mine1,
    theirs1,
    mine2,
    theirs2,
    s1,
    r1,
    s2,
    r2,
    normed,
):
    other = 1 - lax.axis_index("mp")
    barrier = pltpu.get_barrier_semaphore()
    pl.semaphore_signal(barrier, inc=1, device_id={"mp": other}, device_id_type=MESH)
    pl.semaphore_wait(barrier, 1)
    rows = states.shape[0] // chunks

    def swap(mine, theirs, ssem, rsem, c):
        return pltpu.make_async_remote_copy(
            src_ref=mine.at[c],
            dst_ref=theirs.at[c],
            send_sem=ssem.at[c],
            recv_sem=rsem.at[c],
            device_id={"mp": other},
            device_id_type=MESH,
        )

    for c in range(chunks):
        cut = slice(c * rows, (c + 1) * rows)
        acc = dot(att[0, cut, :], out_w[0:LANES, :])
        for j in range(1, att.shape[0]):
            acc = acc + dot(att[j, cut, :], out_w[j * LANES : (j + 1) * LANES, :])
        mine1[c] = acc.astype(mine1.dtype)
        swap(mine1, theirs1, s1, r1, c).start()
    for c in range(chunks):
        cut = slice(c * rows, (c + 1) * rows)
        swap(mine1, theirs1, s1, r1, c).wait_recv()
        summed = mine1[c].astype(jnp.float32) + theirs1[c].astype(jnp.float32)
        norm = layer_norm(states[cut, :].astype(jnp.float32) + summed, gain1[...])
        norm = norm.astype(jnp.bfloat16)
        normed[c] = norm
        v = dot(norm, up_w[...])
        hidden = (v * (1.0 + lax.erf(v * (0.5**0.5))) * 0.5).astype(jnp.bfloat16)
        mine2[c] = dot(hidden, down_w[...]).astype(mine2.dtype)
        swap(mine2, theirs2, s2, r2, c).start()
    for c in range(chunks):
        cut = slice(c * rows, (c + 1) * rows)
        swap(mine2, theirs2, s2, r2, c).wait_recv()
        summed = mine2[c].astype(jnp.float32) + theirs2[c].astype(jnp.float32)
        out[cut, :] = layer_norm(normed[c].astype(jnp.float32) + summed, gain2[...]).astype(
            jnp.bfloat16
        )
    for c in range(chunks):
        swap(mine1, theirs1, s1, r1, c).wait_send()
        swap(mine2, theirs2, s2, r2, c).wait_send()


def vmem_specs(count):
    return [pl.BlockSpec(memory_space=pltpu.VMEM)] * count


def attend_requested(states, qkv_weight, global_ids, random_owner, random_local):
    tokens, width = states.shape
    heads = qkv_weight.shape[2] // HD
    pairs = heads // 2
    blocks = tokens // BS
    g_count = global_ids.shape[0]
    n = lax.axis_size("seq")

    owner = random_owner.reshape(-1)
    items = owner.shape[0]
    cap = max(2, items // n + 1)
    head_list = jnp.broadcast_to(
        jnp.arange(heads, dtype=jnp.int32)[None, :, None], (blocks, heads, R)
    ).reshape(-1)
    code = random_local.reshape(-1) * heads + head_list
    earlier = jnp.arange(items)[:, None] > jnp.arange(items)[None, :]
    rank = jnp.sum(((owner[:, None] == owner[None, :]) & earlier).astype(jnp.int32), axis=1)
    slot = owner * cap + rank
    place = owner * LANES + rank
    wanted = jnp.sum(
        jnp.where(
            place[None, None, :]
            == (jnp.arange(n)[:, None] * LANES + jnp.arange(LANES)[None, :])[:, :, None],
            code[None, None, :],
            0,
        ),
        axis=2,
    ).reshape(n, 1, LANES)

    half = lax.axis_size("mp")
    units = (g_count // half) * (width // LANES) * (BS // 16)
    per = -(-units // n)
    part_rows = pairs * g_count * BS
    rows_per = -(-part_rows // n // 16) * 16
    parts = part_rows // rows_per
    bf = jnp.bfloat16
    own = blocks * heads
    dma = pltpu.SemaphoreType.DMA
    return pl.pallas_call(
        functools.partial(attend_kernel, n, cap, heads, blocks, g_count),
        out_shape=jax.ShapeDtypeStruct((pairs, tokens, LANES), bf),
        in_specs=[pl.BlockSpec(memory_space=pltpu.HBM)] * 2
        + vmem_specs(1)
        + [pl.BlockSpec(memory_space=pltpu.SMEM)] * 2,
        out_specs=pl.BlockSpec(memory_space=pltpu.VMEM),
        scratch_shapes=[
            pltpu.VMEM((tokens, width), bf),
            pltpu.VMEM(qkv_weight.shape, bf),
            pltpu.VMEM((n, 1, LANES), jnp.int32),
            pltpu.SMEM((n, 1, LANES), jnp.int32),
            pltpu.VMEM((units, 16, LANES), bf),
            pltpu.VMEM((n, per, 16, LANES), bf),
            pltpu.VMEM((per, 16, LANES), bf),
            pltpu.VMEM((half, units, 16, LANES), bf),
            pltpu.VMEM((g_count * BS, width), bf),
            pltpu.VMEM((own, BS, LANES), bf),
            pltpu.VMEM((own, BS, LANES), bf),
            pltpu.VMEM((n * cap, BS, LANES), bf),
            pltpu.VMEM((n * cap, BS, LANES), bf),
            pltpu.VMEM((heads, BS, LANES), bf),
            pltpu.VMEM((heads, BS, LANES), bf),
            pltpu.VMEM((own + 2 * heads, BS, LANES), bf),
            pltpu.VMEM((heads, g_count * BS, LANES), bf),
            pltpu.VMEM((heads, g_count * BS, LANES), bf),
            pltpu.VMEM((parts, 2, rows_per, LANES), bf),
            pltpu.VMEM((n, 2, rows_per, LANES), bf),
            pltpu.VMEM((rows_per, LANES), bf),
            pltpu.VMEM((parts, rows_per, LANES), bf),
            pltpu.VMEM((own, BS, (3 + g_count) * BS), jnp.float32),
        ]
        + [dma((n,))] * 8
        + [dma((2,))] * 2
        + [dma((n,))] * 4
        + [dma((half,))] * 2
        + [dma(()), dma((4,))],
        cost_estimate=pl.CostEstimate(
            flops=30_000_000_000, bytes_accessed=20_000_000, transcendentals=0
        ),
        compiler_params=pltpu.CompilerParams(
            collective_id=0, has_side_effects=True, vmem_limit_bytes=32 * 1024 * 1024
        ),
    )(
        pltpu.with_memory_space_constraint(states, pltpu.HBM),
        pltpu.with_memory_space_constraint(qkv_weight, pltpu.HBM),
        wanted,
        slot,
        global_ids,
    )


def layer_gathered(
    states,
    qkv_weight,
    out_weight,
    up_weight,
    down_weight,
    attn_gain,
    mlp_gain,
    global_ids,
    random_owner,
    random_local,
):
    tokens, width = states.shape
    inner = qkv_weight.shape[2]
    heads = inner // HD
    pairs = heads // 2
    blocks = tokens // BS
    g_count = global_ids.shape[0]
    n = lax.axis_size("seq")
    trees = len(TREES)
    piece = tokens // (2 * trees)
    chunk = 16 * BS
    chunks = CHUNKS
    rows = tokens // chunks
    bf = jnp.bfloat16
    dma = pltpu.SemaphoreType.DMA
    operands = (
        states.reshape(2 * trees, piece, width),
        qkv_weight,
        random_owner.transpose(0, 3, 1, 2),
        random_local.transpose(0, 3, 1, 2),
        global_ids,
        out_weight,
        up_weight,
        down_weight,
        attn_gain.reshape(1, width),
        mlp_gain.reshape(1, width),
    )
    return pl.pallas_call(
        functools.partial(gather_kernel, n, heads, blocks, g_count, chunks),
        out_shape=jax.ShapeDtypeStruct((tokens, width), bf),
        in_specs=[pl.BlockSpec(memory_space=pltpu.HBM)] * len(operands),
        out_specs=pl.BlockSpec(memory_space=pltpu.VMEM),
        scratch_shapes=[
            pltpu.VMEM((n * 2 * trees, piece, width), bf),
            pltpu.VMEM((width, inner), bf),
            pltpu.VMEM((width, 2 * inner), bf),
            pltpu.VMEM((n * blocks, BS, 2 * inner), bf),
            pltpu.VMEM((tokens, inner), bf),
            pltpu.VMEM((n * tokens // chunk, 2 * BS, chunk), jnp.float32),
            pltpu.VMEM((blocks * pairs, 2 * BS, (3 + R + g_count) * BS), jnp.float32),
            pltpu.VMEM((blocks * pairs, 2 * BS, (3 + R + g_count) * BS), bf),
            pltpu.VMEM((BS, LANES), bf),
            pltpu.VMEM((pairs * g_count, BS, LANES), bf),
            pltpu.SMEM((1, R, blocks, heads), jnp.int32),
            pltpu.SMEM((1, R, blocks, heads), jnp.int32),
            pltpu.SMEM(global_ids.shape, jnp.int32),
            pltpu.VMEM((pairs, tokens, LANES), bf),
            pltpu.VMEM(out_weight.shape, bf),
            pltpu.VMEM(up_weight.shape, bf),
            pltpu.VMEM(down_weight.shape, bf),
            pltpu.VMEM((1, width), jnp.float32),
            pltpu.VMEM((1, width), jnp.float32),
        ]
        + [pltpu.VMEM((chunks, rows, width), bf)] * 5
        + [dma((n * trees,))] * 4
        + [dma((n,)), dma((n * trees,)), dma((n,))]
        + [dma((4,)), dma((pairs * g_count,))]
        + [dma((chunks,))] * 4
        + [dma((len(operands) + 2,))],
        compiler_params=pltpu.CompilerParams(
            collective_id=0, has_side_effects=True, vmem_limit_bytes=48 * 1024 * 1024
        ),
    )(*[pltpu.with_memory_space_constraint(a, pltpu.HBM) for a in operands])


def gathers(states, qkv_weight, global_ids):
    tokens, width = states.shape
    n = lax.axis_size("seq")
    inner = qkv_weight.shape[2]
    held = n * tokens * (width + 2 * inner) * 2
    pairs = inner // LANES
    return (
        n % 4 == 0
        and global_ids.shape[0] == 2
        and pairs < 4
        and pairs < n // 4
        and lax.axis_size("mp") == 2
        and held <= 24 * 1024 * 1024
        and n * tokens % (16 * BS) == 0
        and tokens % (2 * len(TREES) * 16) == 0
        and 2 * inner % 256 == 0
    )


def shards(
    states,
    qkv_weight,
    out_weight,
    up_weight,
    down_weight,
    attn_gain,
    mlp_gain,
    global_ids,
    random_owner,
    random_local,
):
    tokens, width = states.shape
    if gathers(states, qkv_weight, global_ids):
        return layer_gathered(
            states,
            qkv_weight,
            out_weight,
            up_weight,
            down_weight,
            attn_gain,
            mlp_gain,
            global_ids,
            random_owner,
            random_local,
        )
    bf = jnp.bfloat16
    dma = pltpu.SemaphoreType.DMA
    att = attend_requested(states, qkv_weight, global_ids, random_owner, random_local)

    chunks = 4
    rows = tokens // chunks
    link = jnp.bfloat16
    return pl.pallas_call(
        functools.partial(tail_kernel, chunks),
        out_shape=jax.ShapeDtypeStruct((tokens, width), bf),
        in_specs=vmem_specs(7),
        out_specs=pl.BlockSpec(memory_space=pltpu.VMEM),
        scratch_shapes=[pltpu.VMEM((chunks, rows, width), link)] * 4
        + [dma((chunks,))] * 4
        + [pltpu.VMEM((chunks, rows, width), bf)],
        compiler_params=pltpu.CompilerParams(
            collective_id=1, has_side_effects=True, vmem_limit_bytes=32 * 1024 * 1024
        ),
    )(
        att,
        states,
        out_weight,
        up_weight,
        down_weight,
        attn_gain.reshape(1, width),
        mlp_gain.reshape(1, width),
    )


def solution(mesh):
    in_specs = (
        P("seq", None),
        P(None, None, "mp"),
        P("mp", None),
        P(None, "mp"),
        P("mp", None),
        P(),
        P(),
        P(),
        P("mp", "seq", None, None),
        P("mp", "seq", None, None),
    )
    out_specs = P("seq", None)
    return jax.shard_map(shards, mesh=mesh, in_specs=in_specs, out_specs=out_specs, check_vma=False)
```

```python
import functools

import jax
import jax.numpy as jnp
from jax import lax
from jax.experimental import pallas as pl
from jax.experimental.pallas import tpu as pltpu
from jax.sharding import PartitionSpec as P

HD = 64
BS = 64
R = 3
LANES = 128
MESH = pl.DeviceIdType.MESH

EPSILON = 1e-05
NEGATIVE = -1e30


def layer_norm(inputs, scales):
    center = jnp.mean(inputs, axis=-1, keepdims=True)
    shifted = inputs - center
    spread = jnp.mean(shifted * shifted, axis=-1, keepdims=True)
    return shifted * lax.rsqrt(spread + EPSILON) * scales


def dot_t(a, b):
    return lax.dot_general(a, b, (((1,), (1,)), ((), ())), preferred_element_type=jnp.float32)


def dot(a, b):
    return jnp.dot(a, b, preferred_element_type=jnp.float32)


def swap_halves(x):
    return pltpu.roll(x, HD, 1)


def attend_kernel(
    n,
    cap,
    heads,
    blocks,
    g_count,
    states_hbm,
    weight_hbm,
    wanted,
    slot,
    gids,
    att,
    states,
    weight,
    tab,
    tab_s,
    cand,
    cand_in,
    pick,
    gath,
    gstates,
    kvb,
    qpad,
    stage,
    rr,
    halo_l,
    halo_r,
    win,
    gq,
    gkv,
    part,
    part_in,
    gmine,
    gout,
    scores,
    s_tab,
    r_tab,
    s_cand,
    r_cand,
    s_gath,
    r_gath,
    s_rand,
    r_rand,
    s_halo,
    r_halo,
    s_part,
    r_part,
    s_gout,
    r_gout,
    s_mp,
    r_mp,
    l_sem,
    w_sem,
):
    me = lax.axis_index("seq")
    mine = lax.axis_index("mp")
    pairs = heads // 2
    width = states.shape[1]
    cols = width // LANES
    quarters = BS // 16
    half = gath.shape[0]
    gper = gath.shape[1] // (cols * quarters)
    units = gper * cols * quarters
    per = cand_in.shape[1]
    cand_parts = units // per
    rows_per = part_in.shape[2]
    part_parts = part.shape[0]
    left = lax.rem(me + n - 1, n)
    right = lax.rem(me + 1, n)

    def peer(k):
        return lax.rem(me + k, n)

    def each_peer(body):
        def step(k, carry):
            body(peer(k))
            return carry

        lax.fori_loop(1, n, step, 0)

    def guarded(limit, who, body):
        if limit < n:
            pl.when(who < limit)(body)
        else:
            body()

    def remote(src, dst, ssem, rsem, d):
        return pltpu.make_async_remote_copy(
            src_ref=src,
            dst_ref=dst,
            send_sem=ssem,
            recv_sem=rsem,
            device_id={"seq": d},
            device_id_type=MESH,
        )

    def tab_copy(d, owner):
        return remote(wanted.at[d], tab.at[owner], s_tab.at[d], r_tab.at[owner], d)

    def cand_copy(d, owner, at):
        return remote(
            cand.at[pl.ds(at * per, per)], cand_in.at[owner], s_cand.at[d], r_cand.at[owner], d
        )

    def gath_copy(d, owner):
        return remote(
            pick, gath.at[mine, pl.ds(owner * per, per)], s_gath.at[d], r_gath.at[owner], d
        )

    def rand_copy(d, owner):
        return remote(
            stage.at[pl.ds(d * cap, cap)],
            rr.at[pl.ds(owner * cap, cap)],
            s_rand.at[d],
            r_rand.at[owner],
            d,
        )

    def part_copy(d, owner, at):
        return remote(part.at[at], part_in.at[owner], s_part.at[d], r_part.at[owner], d)

    def gout_copy(d, owner):
        return remote(gmine, gout.at[owner], s_gout.at[d], r_gout.at[owner], d)

    def mp_copy(k, owner):
        other = lax.rem(mine + k, half)
        return pltpu.make_async_remote_copy(
            src_ref=gath.at[mine],
            dst_ref=gath.at[owner],
            send_sem=s_mp.at[k],
            recv_sem=r_mp.at[owner],
            device_id={"mp": other},
            device_id_type=MESH,
        )

    to_right = remote(
        kvb.at[pl.ds((blocks - 1) * heads, heads)], halo_l, s_halo.at[0], r_halo.at[0], right
    )
    to_left = remote(kvb.at[pl.ds(0, heads)], halo_r, s_halo.at[1], r_halo.at[1], left)

    loads = [pltpu.make_async_copy(states_hbm, states, w_sem.at[3])] + [
        pltpu.make_async_copy(weight_hbm.at[i], weight.at[i], w_sem.at[i]) for i in (1, 2, 0)
    ]
    for load in loads:
        load.start()

    barrier = pltpu.get_barrier_semaphore()
    each_peer(
        lambda d: pl.semaphore_signal(barrier, inc=1, device_id={"seq": d}, device_id_type=MESH)
    )
    for k in range(1, half):
        pl.semaphore_signal(
            barrier, inc=1, device_id={"mp": lax.rem(mine + k, half)}, device_id_type=MESH
        )

    loads[0].wait()
    for i in range(gper):
        local = lax.rem(gids[mine * gper + i], blocks)
        for j in range(cols):
            cut = slice(j * LANES, (j + 1) * LANES)
            piece = states[0:BS, cut]
            for b in range(1, blocks):
                piece = jnp.where(local == b, states[b * BS : (b + 1) * BS, cut], piece)
            for q in range(quarters):
                cand[(i * cols + j) * quarters + q] = piece[q * 16 : (q + 1) * 16]
    tab[me] = wanted[me]

    def own_cand():
        cand_in[me] = cand[pl.ds(me * per, per)]

    guarded(cand_parts, me, own_cand)
    loads[1].wait()
    loads[2].wait()

    lane = lax.broadcasted_iota(jnp.int32, (BS, LANES), 1)
    low = lane < HD
    x = states[...]
    for j in range(pairs):
        cut = slice(j * LANES, (j + 1) * LANES)
        k = dot(x, weight[1, :, cut])
        v = dot(x, weight[2, :, cut])
        for b in range(blocks):
            kb, vb = k[b * BS : (b + 1) * BS], v[b * BS : (b + 1) * BS]
            kvb[b * heads + 2 * j] = jnp.where(low, kb, swap_halves(vb)).astype(jnp.bfloat16)
            kvb[b * heads + 2 * j + 1] = jnp.where(low, swap_halves(kb), vb).astype(jnp.bfloat16)

    pl.semaphore_wait(barrier, n - 1 + half - 1)
    each_peer(lambda d: tab_copy(d, me).start())
    each_peer(lambda d: guarded(cand_parts, d, lambda: cand_copy(d, me, d).start()))
    to_right.start()
    to_left.start()

    loads[3].wait()
    scaling = HD ** (-0.5)
    for j in range(pairs):
        cut = slice(j * LANES, (j + 1) * LANES)
        q = dot(x, weight[0, :, cut]).astype(jnp.bfloat16).astype(jnp.float32) * scaling
        for b in range(blocks):
            qb = q[b * BS : (b + 1) * BS]
            qpad[b * heads + 2 * j] = jnp.where(low, qb, 0.0).astype(jnp.bfloat16)
            qpad[b * heads + 2 * j + 1] = jnp.where(low, swap_halves(qb), 0.0).astype(jnp.bfloat16)

    def relay():
        each_peer(lambda d: cand_copy(d, d, me).wait_recv())
        for u in range(per):
            g = (me * per + u) // (cols * quarters)
            wanted_id = gids[mine * gper + g]

            def choose(d, so_far):
                here = (wanted_id >= d * blocks) & (wanted_id < (d + 1) * blocks)
                return jnp.where(here, cand_in[d, u], so_far)

            pick[u] = lax.fori_loop(1, n, choose, cand_in[0, u])
        gath[mine, pl.ds(me * per, per)] = pick[...]
        each_peer(lambda d: gath_copy(d, me).start())

    guarded(cand_parts, me, relay)

    each_peer(lambda d: tab_copy(d, d).wait_recv())
    table = pltpu.make_async_copy(tab, tab_s, l_sem)
    table.start()
    table.wait()

    def serve(d):
        for c in range(cap):
            stage[d * cap + c] = kvb[tab_s[d, 0, c]]
        rand_copy(d, me).start()

    def serve_some(start, stop):
        def step(k, carry):
            serve(peer(k))
            return carry

        lax.fori_loop(start, stop, step, 0)

    for c in range(cap):
        rr[me * cap + c] = kvb[tab_s[me, 0, c]]

    each_peer(lambda d: guarded(cand_parts, d, lambda: gath_copy(d, d).wait_recv()))
    for k in range(1, half):
        mp_copy(k, mine).start()
    for k in range(1, half):
        mp_copy(k, lax.rem(mine + k, half)).wait_recv()
    for g in range(g_count):
        for j in range(cols):
            for q in range(quarters):
                gstates[g * BS + q * 16 : g * BS + (q + 1) * 16, j * LANES : (j + 1) * LANES] = (
                    gath[g // gper, ((g % gper) * cols + j) * quarters + q]
                )
    gx = gstates[...]
    rows = g_count * BS
    glane = lax.broadcasted_iota(jnp.int32, (rows, LANES), 1)
    glow = glane < HD
    for j in range(pairs):
        cut = slice(j * LANES, (j + 1) * LANES)
        q = dot(gx, weight[0, :, cut]).astype(jnp.bfloat16).astype(jnp.float32) * scaling
        k = dot(gx, weight[1, :, cut])
        v = dot(gx, weight[2, :, cut])
        gq[2 * j] = jnp.where(glow, q, 0.0).astype(jnp.bfloat16)
        gq[2 * j + 1] = jnp.where(glow, swap_halves(q), 0.0).astype(jnp.bfloat16)
        gkv[2 * j] = jnp.where(glow, k, swap_halves(v)).astype(jnp.bfloat16)
        gkv[2 * j + 1] = jnp.where(glow, swap_halves(k), v).astype(jnp.bfloat16)

    for h in range(heads):
        keys = jnp.concatenate([kvb[b * heads + h] for b in range(blocks)], axis=0)
        s = dot_t(gq[h], keys)
        high = jnp.max(s, axis=-1, keepdims=True)
        e = jnp.exp(s - high)
        total = jnp.sum(e, axis=-1, keepdims=True)
        e_high = e.astype(jnp.bfloat16)
        e_low = (e - e_high.astype(jnp.float32)).astype(jnp.bfloat16)
        acc = (dot(e_high, keys) + dot(e_low, keys)) * (1.0 / total)
        level = high + jnp.log(total)
        first = level.astype(jnp.bfloat16).astype(jnp.float32)
        second = (level - first).astype(jnp.bfloat16).astype(jnp.float32)
        third = level - first - second
        packed = jnp.where(
            glane < 16,
            first,
            jnp.where(glane < 32, second, jnp.where(glow, third, acc)),
        ).astype(jnp.bfloat16)
        cuts = rows // rows_per
        for c in range(cuts):
            part[(h // 2) * cuts + c, h % 2] = packed[c * rows_per : (c + 1) * rows_per]
    each_peer(lambda d: guarded(part_parts, d, lambda: part_copy(d, me, d).start()))
    serve_some(1, n)

    to_right.wait_recv()
    to_left.wait_recv()
    win[0:heads] = halo_l[...]
    win[heads : heads + blocks * heads] = kvb[...]
    win[heads + blocks * heads :] = halo_r[...]

    near = 3 + g_count
    slot_lane = lax.broadcasted_iota(jnp.int32, (BS, near * BS), 1)

    def near_keys(at, h):
        return jnp.concatenate([win[at + t * heads] for t in range(3)] + [gkv[h]], axis=0)

    def near_step(b, carry):
        first = me * blocks + b
        start = jnp.where(first == 0, BS, 0)
        stop = jnp.where(first == n * blocks - 1, 2 * BS, 3 * BS)
        outside = (slot_lane < start) | ((slot_lane >= stop) & (slot_lane < 3 * BS))
        for h in range(heads):
            at = b * heads + h
            scores[at] = jnp.where(outside, NEGATIVE, dot_t(qpad[at], near_keys(at, h)))
        return carry

    lax.fori_loop(0, blocks, near_step, 0)

    def combine():
        part_in[me] = part[me]
        each_peer(lambda d: part_copy(d, d, me).wait_recv())
        outs = []
        for parity in range(2):

            def level(d):
                piece = part_in[d, parity].astype(jnp.float32)
                return piece, piece[:, 0:1] + piece[:, 16:17] + piece[:, 32:33]

            def top(d, best):
                return jnp.maximum(best, level(d)[1])

            best = lax.fori_loop(1, n, top, level(0)[1])

            def add(d, so_far):
                piece, high = level(d)
                factor = jnp.exp(high - best)
                return so_far[0] + piece * factor, so_far[1] + factor

            zero = (jnp.zeros((rows_per, LANES), jnp.float32), jnp.zeros((rows_per, 1), jnp.float32))
            summed, total = lax.fori_loop(0, n, add, zero)
            outs.append(summed / total)
        plow = lax.broadcasted_iota(jnp.int32, (rows_per, LANES), 1) < HD
        done = jnp.where(plow, swap_halves(outs[0]), outs[1]).astype(jnp.bfloat16)
        gmine[...] = done
        gout[me] = done
        each_peer(lambda d: gout_copy(d, me).start())

    guarded(part_parts, me, combine)

    each_peer(lambda d: rand_copy(d, d).wait_recv())

    def block_step(b, carry):
        for j in range(pairs):
            halves = []
            for h in (2 * j, 2 * j + 1):
                at = b * heads + h
                early_keys = near_keys(at, h)
                keys = jnp.concatenate([rr[slot[at * R + r]] for r in range(R)], axis=0)
                s = dot_t(qpad[at], keys)
                early_s = scores[at]
                high = jnp.maximum(
                    jnp.max(s, axis=-1, keepdims=True), jnp.max(early_s, axis=-1, keepdims=True)
                )
                e = jnp.exp(s - high)
                early_e = jnp.exp(early_s - high)
                total = jnp.sum(e, axis=-1, keepdims=True) + jnp.sum(
                    early_e, axis=-1, keepdims=True
                )
                share = 1.0 / total
                w = (e * share).astype(jnp.bfloat16)
                early_w = (early_e * share).astype(jnp.bfloat16)
                halves.append(dot(w, keys) + dot(early_w, early_keys))
            att[j, pl.ds(pl.multiple_of(b * BS, BS), BS), :] = jnp.where(
                low, swap_halves(halves[0]), halves[1]
            ).astype(jnp.bfloat16)
        return carry

    lax.fori_loop(0, blocks, block_step, 0)

    each_peer(lambda d: guarded(part_parts, d, lambda: gout_copy(d, d).wait_recv()))
    for j in range(pairs):
        for g in range(g_count):
            cuts = BS // rows_per
            at = (j * g_count + g) * cuts
            row = jnp.concatenate([gout[at + c] for c in range(cuts)], axis=0).astype(jnp.float32)
            for b in range(blocks):
                here = gids[g] == me * blocks + b
                old = att[j, b * BS : (b + 1) * BS, :].astype(jnp.float32)
                att[j, b * BS : (b + 1) * BS, :] = jnp.where(here, row, old).astype(jnp.bfloat16)

    def drain(d):
        tab_copy(d, me).wait_send()
        guarded(cand_parts, d, lambda: cand_copy(d, me, d).wait_send())
        guarded(cand_parts, me, lambda: gath_copy(d, me).wait_send())
        rand_copy(d, me).wait_send()
        guarded(part_parts, d, lambda: part_copy(d, me, d).wait_send())
        guarded(part_parts, me, lambda: gout_copy(d, me).wait_send())

    each_peer(drain)
    for k in range(1, half):
        mp_copy(k, mine).wait_send()
    to_right.wait_send()
    to_left.wait_send()


TREES = ("zxy", "zyx", "yzx", "xzy")
PLACES = ((0, 0), (1, 0), (0, 1), (1, 1))
TURNS = (
    (-21.5, -8.5, -4.5, 11.5),
    (-15.0, 1.0, -2.5, 14.5),
    (-17.5, 0.0, -6.5, 11.5),
    (-13.0, -3.0, 2.5, 15.0),
)
PAUSES = (7.5, 9.5, 13.5, 18.0)
ROUND = 9.0
CHUNKS = 2


def arrivals(depth):
    steps = []
    for slot in range(depth):
        for p, (dx, dy) in enumerate(PLACES):
            if not slot and not p:
                continue
            place = (slot, dx, dy)
            turns = [ROUND * slot + row[p] for row in TURNS]
            steps += [(turn, 0, t, place) for t, turn in enumerate(turns)]
            steps.append((max(turns) + PAUSES[p], 1, 0, place))
    return [step[1:] for step in sorted(steps)]


def hops(tree, slot, dx, dy):
    moved = {"x": dx, "y": dy, "z": slot}
    last = max((i for i in range(3) if moved[tree[i]]), default=-1)
    onward = tree[last + 1 :]
    via = tree[last] if last >= 0 else ""
    return via, ("z" if via == "z" else "") + onward


def slots(z, depth):
    inward = 1 if 2 * z < depth else -1
    return sorted(range(depth), key=lambda q: (abs(q - z), (z - q) * inward))


def gather_kernel(
    n,
    heads,
    blocks,
    g_count,
    chunks,
    states_hbm,
    weight_hbm,
    owner_hbm,
    local_hbm,
    gids_hbm,
    out_hbm,
    up_hbm,
    down_hbm,
    gain1_hbm,
    gain2_hbm,
    out,
    xs,
    wq,
    wkv,
    kv,
    q_all,
    wide,
    scores,
    weights,
    gmine,
    gout,
    owner,
    local,
    gids,
    att,
    out_w,
    up_w,
    down_w,
    gain1,
    gain2,
    mine1,
    theirs1,
    mine2,
    theirs2,
    normed,
    s_x,
    s_y,
    s_up,
    s_down,
    s_mp,
    r_ici,
    r_mp,
    s_gout,
    r_gout,
    s1,
    r1,
    s2,
    r2,
    l_sem,
):
    me = lax.axis_index("seq")
    mine = lax.axis_index("mp")
    pairs = heads // 2
    inner = heads * HD
    trees = len(TREES)
    per = 2 * trees
    piece = xs.shape[1]
    width = xs.shape[2]
    tokens = per * piece
    depth = n // 4
    x_at, y_at, z_at = lax.rem(me, 2), lax.rem(me // 2, 2), me // 4

    def remote(src, dst, ssem, rsem, where):
        return pltpu.make_async_remote_copy(
            src_ref=src,
            dst_ref=dst,
            send_sem=ssem,
            recv_sem=rsem,
            device_id=where,
            device_id_type=MESH,
        )

    def plane(slot):
        if slot == 0:
            return z_at
        found = slots(0, depth)[slot]
        for z in range(1, depth):
            found = jnp.where(z_at == z, slots(z, depth)[slot], found)
        return found

    def shard_of(slot, dx, dy):
        x = 1 - x_at if dx else x_at
        y = 1 - y_at if dy else y_at
        return plane(slot) * 4 + y * 2 + x

    def ici(shard, t, ssem, d):
        at = xs.at[(shard * 2 + mine) * trees + t]
        return remote(at, at, ssem.at[shard * trees + t], r_ici.at[shard * trees + t], {"seq": d})

    def across(shard, core):
        at = xs.at[pl.ds((shard * 2 + core) * trees, trees)]
        return remote(at, at, s_mp.at[shard], r_mp.at[shard], {"mp": 1 - mine})

    x_peer = me + 1 - 2 * x_at
    y_peer = me + 2 - 4 * y_at
    up, down = lax.rem(me + 4, n), lax.rem(me + n - 4, n)

    def onward(t, slot, dx, dy, act):
        shard = shard_of(slot, dx, dy)
        via, axes = hops(TREES[t], slot, dx, dy)
        for axis in axes:
            if axis == "x":
                act(ici(shard, t, s_x, x_peer))
            elif axis == "y":
                act(ici(shard, t, s_y, y_peer))
            else:
                source = plane(slot)
                go_up = z_at < depth - 1
                go_down = z_at > 0
                if via == "z":
                    go_up = go_up & (source < z_at)
                    go_down = go_down & (source > z_at)
                pl.when(go_up)(lambda: act(ici(shard, t, s_up, up)))
                pl.when(go_down)(lambda: act(ici(shard, t, s_down, down)))

    order = arrivals(depth)

    pairs_of = [
        (states_hbm, xs.at[pl.ds(me * per, per)]),
        (weight_hbm.at[1], wkv.at[:, 0:inner]),
        (weight_hbm.at[2], wkv.at[:, inner : 2 * inner]),
        (weight_hbm.at[0], wq),
        (owner_hbm, owner),
        (local_hbm, local),
        (gids_hbm, gids),
        (gain1_hbm, gain1),
        (gain2_hbm, gain2),
        (out_hbm, out_w),
        (up_hbm, up_w),
        (down_hbm, down_w),
    ]
    loads = [pltpu.make_async_copy(a, b, l_sem.at[i]) for i, (a, b) in enumerate(pairs_of)]
    loads[0].start()
    barrier = pltpu.get_barrier_semaphore()
    for d in (x_peer, y_peer):
        pl.semaphore_signal(barrier, inc=1, device_id={"seq": d}, device_id_type=MESH)
    pl.semaphore_signal(barrier, inc=1, device_id={"mp": 1 - mine}, device_id_type=MESH)
    for there, d in ((z_at < depth - 1, up), (z_at > 0, down)):
        pl.when(there)(
            lambda d=d: pl.semaphore_signal(
                barrier, inc=1, device_id={"seq": d}, device_id_type=MESH
            )
        )
    for load in loads[1:]:
        load.start()
    column = jnp.where(z_at < depth - 1, 1, 0) + jnp.where(z_at > 0, 1, 0)
    loads[0].wait()
    pl.semaphore_wait(barrier, 3 + column)
    for t in range(trees):
        onward(t, 0, 0, 0, lambda copy: copy.start())
    for load in loads[1:4]:
        load.wait()

    def project(shard):
        x = xs[pl.ds(shard * per, per)].reshape(tokens, width)
        y = dot(x, wkv[...]).astype(jnp.bfloat16)
        kv[pl.ds(shard * blocks, blocks)] = y.reshape(blocks, BS, 2 * inner)

    x = xs[pl.ds(me * per, per)].reshape(tokens, width)
    scaling = HD ** (-0.5)
    q_all[...] = (
        dot(x, wq[...]).astype(jnp.bfloat16).astype(jnp.float32) * scaling
    ).astype(jnp.bfloat16)
    project(me)

    left = dict()
    for kind, t, place in order:
        shard = shard_of(*place)
        if kind:
            across(shard, 1 - mine).wait_recv()
            project(shard)
            continue
        ici(shard, t, s_x, x_peer).wait_recv()
        onward(t, *place, lambda copy: copy.start())
        left[place] = left.get(place, trees) - 1
        if left[place] == 0:
            across(shard, mine).start()
    for load in loads[4:]:
        load.wait()

    lane = lax.broadcasted_iota(jnp.int32, (BS, LANES), 1)
    low = lane < HD

    def split(q):
        zero = jnp.zeros_like(q)
        return jnp.concatenate([jnp.where(low, q, zero), jnp.where(low, zero, q)], axis=0)

    def together(out):
        return jnp.where(low, out[0:BS], out[BS : 2 * BS]).astype(jnp.bfloat16)

    spot = lax.rem(me, 4)
    final = n - 1
    steps, _, chunk = wide.shape
    per_chunk = chunk // BS

    def fold(best, s, join):
        for c in range(0, s.shape[1], LANES):
            best = join(best, s[:, c : c + LANES])
        return best

    def share():
        first_block = spot < pairs
        j = jnp.where(first_block, spot, z_at)
        block = jnp.where(first_block, gids[0], gids[1])
        k_cut = pl.ds(pl.multiple_of(j * LANES, LANES), LANES)
        v_cut = pl.ds(pl.multiple_of(inner + j * LANES, LANES), LANES)
        rows = BS // piece
        x = xs[pl.ds(block * rows, rows)].reshape(BS, width)
        q = dot(x, wq[:, k_cut]).astype(jnp.bfloat16).astype(jnp.float32) * scaling
        q2 = split(q.astype(jnp.bfloat16))

        def score(c, best):
            keys = kv[pl.ds(c * per_chunk, per_chunk), :, k_cut].reshape(chunk, LANES)
            s = dot_t(q2, keys)
            wide[c] = s
            return fold(best, s, jnp.maximum)

        best = jnp.full((2 * BS, LANES), NEGATIVE, jnp.float32)
        best = lax.fori_loop(0, steps, score, best, unroll=True)
        high = jnp.max(best, axis=-1, keepdims=True)

        def add(c, so_far):
            values = kv[pl.ds(c * per_chunk, per_chunk), :, v_cut].reshape(chunk, LANES)
            e = jnp.exp(wide[c] - high)
            e_high = e.astype(jnp.bfloat16)
            e_low = (e - e_high.astype(jnp.float32)).astype(jnp.bfloat16)
            return (
                so_far[0] + dot(e_high, values) + dot(e_low, values),
                fold(so_far[1], e, jnp.add),
            )

        zero = jnp.zeros((2 * BS, LANES), jnp.float32)
        summed, total = lax.fori_loop(0, steps, add, (zero, zero), unroll=True)
        gmine[...] = together(summed / jnp.sum(total, axis=-1, keepdims=True))

        def to_plane():
            for k in range(1, 4):
                gout_copy(spot, k).start()

        pl.when(first_block)(to_plane)
        pl.when(spot >= pairs)(lambda: last_copy(z_at).start())

    def gout_copy(unit, k):
        d = z_at * 4 + lax.rem(spot + k, 4)
        return remote(gmine, gout.at[unit], s_gout.at[k], r_gout.at[unit], {"seq": d})

    def last_copy(unit):
        at = pairs + unit
        return remote(gmine, gout.at[at], s_gout.at[0], r_gout.at[at], {"seq": final})

    shares = (spot < pairs) | ((spot == 3) & (z_at < pairs))
    pl.when(shares)(share)

    slot_lane = lax.broadcasted_iota(jnp.int32, (1, 3 * BS), 1)
    last = n * blocks - 1

    def rows_of(b, j, base):
        first = me * blocks + b
        near = [jnp.maximum(first - 1, 0), first, jnp.minimum(first + 1, last)]
        one = [owner[0, r, b, 2 * j] * blocks + local[0, r, b, 2 * j] for r in range(R)]
        two = [owner[0, r, b, 2 * j + 1] * blocks + local[0, r, b, 2 * j + 1] for r in range(R)]
        cut = slice(base + j * LANES, base + (j + 1) * LANES)
        return jnp.concatenate(
            [kv[at, :, cut] for at in near]
            + [jnp.where(low, kv[a, :, cut], kv[c, :, cut]) for a, c in zip(one, two)]
            + [kv[gids[g], :, cut] for g in range(g_count)],
            axis=0,
        )

    for b in range(blocks):
        first = me * blocks + b
        start = jnp.where(first == 0, BS, 0)
        stop = jnp.where(first == last, 2 * BS, 3 * BS)
        bias = jnp.where((slot_lane < start) | (slot_lane >= stop), NEGATIVE, 0.0)
        for j in range(pairs):
            q = q_all[b * BS : (b + 1) * BS, j * LANES : (j + 1) * LANES]
            s = dot_t(split(q), rows_of(b, j, 0))
            scores[b * pairs + j, :, 0 : 3 * BS] = s[:, 0 : 3 * BS] + bias
            scores[b * pairs + j, :, 3 * BS :] = s[:, 3 * BS :]

    def weigh(i, carry):
        for part in range(2):
            cut = slice(part * BS, (part + 1) * BS)
            s = scores[i, cut]
            e = jnp.exp(s - jnp.max(s, axis=-1, keepdims=True))
            share_of = 1.0 / jnp.sum(e, axis=-1, keepdims=True)
            weights[i, cut] = (e * share_of).astype(jnp.bfloat16)
        return carry

    lax.fori_loop(0, blocks * pairs, weigh, 0, unroll=6)

    for b in range(blocks):
        for j in range(pairs):
            mixed = dot(weights[b * pairs + j], rows_of(b, j, inner))
            att[j, b * BS : (b + 1) * BS, :] = together(mixed)

    for unit in range(pairs):
        pl.when(spot != unit)(lambda unit=unit: gout_copy(unit, 1).wait_recv())
    for j in range(pairs):
        row = jnp.where(spot == j, gmine[...], gout[j])
        for b in range(blocks):
            cut = slice(b * BS, (b + 1) * BS)
            here = gids[0] == me * blocks + b
            att[j, cut, :] = jnp.where(here, row, att[j, cut, :])

    def take_last():
        for unit in range(pairs):
            last_copy(unit).wait_recv()
            att[unit, (blocks - 1) * BS : blocks * BS, :] = gout[pairs + unit]

    pl.when(me == final)(take_last)

    rows = tokens // chunks

    def swap(sent, got, ssem, rsem, c):
        return remote(sent.at[c], got.at[c], ssem.at[c], rsem.at[c], {"mp": 1 - mine})

    for c in range(chunks):
        cut = slice(c * rows, (c + 1) * rows)
        acc = dot(att[0, cut, :], out_w[0:LANES, :])
        for j in range(1, pairs):
            acc = acc + dot(att[j, cut, :], out_w[j * LANES : (j + 1) * LANES, :])
        mine1[c] = acc.astype(mine1.dtype)
        swap(mine1, theirs1, s1, r1, c).start()
    x = xs[pl.ds(me * per, per)].reshape(chunks, rows, width)
    for c in range(chunks):
        swap(mine1, theirs1, s1, r1, c).wait_recv()
        summed = mine1[c].astype(jnp.float32) + theirs1[c].astype(jnp.float32)
        norm = layer_norm(x[c].astype(jnp.float32) + summed, gain1[...].reshape(1, width))
        norm = norm.astype(jnp.bfloat16)
        normed[c] = norm
        v = dot(norm, up_w[...])
        hidden = (v * (1.0 + lax.erf(v * (0.5**0.5))) * 0.5).astype(jnp.bfloat16)
        mine2[c] = dot(hidden, down_w[...]).astype(mine2.dtype)
        swap(mine2, theirs2, s2, r2, c).start()
    for c in range(chunks):
        cut = slice(c * rows, (c + 1) * rows)
        swap(mine2, theirs2, s2, r2, c).wait_recv()
        summed = mine2[c].astype(jnp.float32) + theirs2[c].astype(jnp.float32)
        out[cut, :] = layer_norm(normed[c].astype(jnp.float32) + summed, gain2[...].reshape(1, width)).astype(
            jnp.bfloat16
        )
    for c in range(chunks):
        swap(mine1, theirs1, s1, r1, c).wait_send()
        swap(mine2, theirs2, s2, r2, c).wait_send()
    for t in range(trees):
        onward(t, 0, 0, 0, lambda copy: copy.wait_send())
    for kind, t, place in order:
        if not kind:
            onward(t, *place, lambda copy: copy.wait_send())
    for place in left:
        across(shard_of(*place), mine).wait_send()

    def drain():
        for k in range(1, 4):
            gout_copy(spot, k).wait_send()

    pl.when(spot < pairs)(drain)
    pl.when((spot == 3) & (z_at < pairs))(lambda: last_copy(z_at).wait_send())


def tail_kernel(
    chunks,
    att,
    states,
    out_w,
    up_w,
    down_w,
    gain1,
    gain2,
    out,
    mine1,
    theirs1,
    mine2,
    theirs2,
    s1,
    r1,
    s2,
    r2,
    normed,
):
    other = 1 - lax.axis_index("mp")
    barrier = pltpu.get_barrier_semaphore()
    pl.semaphore_signal(barrier, inc=1, device_id={"mp": other}, device_id_type=MESH)
    pl.semaphore_wait(barrier, 1)
    rows = states.shape[0] // chunks

    def swap(mine, theirs, ssem, rsem, c):
        return pltpu.make_async_remote_copy(
            src_ref=mine.at[c],
            dst_ref=theirs.at[c],
            send_sem=ssem.at[c],
            recv_sem=rsem.at[c],
            device_id={"mp": other},
            device_id_type=MESH,
        )

    for c in range(chunks):
        cut = slice(c * rows, (c + 1) * rows)
        acc = dot(att[0, cut, :], out_w[0:LANES, :])
        for j in range(1, att.shape[0]):
            acc = acc + dot(att[j, cut, :], out_w[j * LANES : (j + 1) * LANES, :])
        mine1[c] = acc.astype(mine1.dtype)
        swap(mine1, theirs1, s1, r1, c).start()
    for c in range(chunks):
        cut = slice(c * rows, (c + 1) * rows)
        swap(mine1, theirs1, s1, r1, c).wait_recv()
        summed = mine1[c].astype(jnp.float32) + theirs1[c].astype(jnp.float32)
        norm = layer_norm(states[cut, :].astype(jnp.float32) + summed, gain1[...])
        norm = norm.astype(jnp.bfloat16)
        normed[c] = norm
        v = dot(norm, up_w[...])
        hidden = (v * (1.0 + lax.erf(v * (0.5**0.5))) * 0.5).astype(jnp.bfloat16)
        mine2[c] = dot(hidden, down_w[...]).astype(mine2.dtype)
        swap(mine2, theirs2, s2, r2, c).start()
    for c in range(chunks):
        cut = slice(c * rows, (c + 1) * rows)
        swap(mine2, theirs2, s2, r2, c).wait_recv()
        summed = mine2[c].astype(jnp.float32) + theirs2[c].astype(jnp.float32)
        out[cut, :] = layer_norm(normed[c].astype(jnp.float32) + summed, gain2[...]).astype(
            jnp.bfloat16
        )
    for c in range(chunks):
        swap(mine1, theirs1, s1, r1, c).wait_send()
        swap(mine2, theirs2, s2, r2, c).wait_send()


def vmem_specs(count):
    return [pl.BlockSpec(memory_space=pltpu.VMEM)] * count


def attend_requested(states, qkv_weight, global_ids, random_owner, random_local):
    tokens, width = states.shape
    heads = qkv_weight.shape[2] // HD
    pairs = heads // 2
    blocks = tokens // BS
    g_count = global_ids.shape[0]
    n = lax.axis_size("seq")

    owner = random_owner.reshape(-1)
    items = owner.shape[0]
    cap = max(2, items // n + 1)
    head_list = jnp.broadcast_to(
        jnp.arange(heads, dtype=jnp.int32)[None, :, None], (blocks, heads, R)
    ).reshape(-1)
    code = random_local.reshape(-1) * heads + head_list
    earlier = jnp.arange(items)[:, None] > jnp.arange(items)[None, :]
    rank = jnp.sum(((owner[:, None] == owner[None, :]) & earlier).astype(jnp.int32), axis=1)
    slot = owner * cap + rank
    place = owner * LANES + rank
    wanted = jnp.sum(
        jnp.where(
            place[None, None, :]
            == (jnp.arange(n)[:, None] * LANES + jnp.arange(LANES)[None, :])[:, :, None],
            code[None, None, :],
            0,
        ),
        axis=2,
    ).reshape(n, 1, LANES)

    half = lax.axis_size("mp")
    units = (g_count // half) * (width // LANES) * (BS // 16)
    per = -(-units // n)
    part_rows = pairs * g_count * BS
    rows_per = -(-part_rows // n // 16) * 16
    parts = part_rows // rows_per
    bf = jnp.bfloat16
    own = blocks * heads
    dma = pltpu.SemaphoreType.DMA
    return pl.pallas_call(
        functools.partial(attend_kernel, n, cap, heads, blocks, g_count),
        out_shape=jax.ShapeDtypeStruct((pairs, tokens, LANES), bf),
        in_specs=[pl.BlockSpec(memory_space=pltpu.HBM)] * 2
        + vmem_specs(1)
        + [pl.BlockSpec(memory_space=pltpu.SMEM)] * 2,
        out_specs=pl.BlockSpec(memory_space=pltpu.VMEM),
        scratch_shapes=[
            pltpu.VMEM((tokens, width), bf),
            pltpu.VMEM(qkv_weight.shape, bf),
            pltpu.VMEM((n, 1, LANES), jnp.int32),
            pltpu.SMEM((n, 1, LANES), jnp.int32),
            pltpu.VMEM((units, 16, LANES), bf),
            pltpu.VMEM((n, per, 16, LANES), bf),
            pltpu.VMEM((per, 16, LANES), bf),
            pltpu.VMEM((half, units, 16, LANES), bf),
            pltpu.VMEM((g_count * BS, width), bf),
            pltpu.VMEM((own, BS, LANES), bf),
            pltpu.VMEM((own, BS, LANES), bf),
            pltpu.VMEM((n * cap, BS, LANES), bf),
            pltpu.VMEM((n * cap, BS, LANES), bf),
            pltpu.VMEM((heads, BS, LANES), bf),
            pltpu.VMEM((heads, BS, LANES), bf),
            pltpu.VMEM((own + 2 * heads, BS, LANES), bf),
            pltpu.VMEM((heads, g_count * BS, LANES), bf),
            pltpu.VMEM((heads, g_count * BS, LANES), bf),
            pltpu.VMEM((parts, 2, rows_per, LANES), bf),
            pltpu.VMEM((n, 2, rows_per, LANES), bf),
            pltpu.VMEM((rows_per, LANES), bf),
            pltpu.VMEM((parts, rows_per, LANES), bf),
            pltpu.VMEM((own, BS, (3 + g_count) * BS), jnp.float32),
        ]
        + [dma((n,))] * 8
        + [dma((2,))] * 2
        + [dma((n,))] * 4
        + [dma((half,))] * 2
        + [dma(()), dma((4,))],
        cost_estimate=pl.CostEstimate(
            flops=30_000_000_000, bytes_accessed=20_000_000, transcendentals=0
        ),
        compiler_params=pltpu.CompilerParams(
            collective_id=0, has_side_effects=True, vmem_limit_bytes=32 * 1024 * 1024
        ),
    )(
        pltpu.with_memory_space_constraint(states, pltpu.HBM),
        pltpu.with_memory_space_constraint(qkv_weight, pltpu.HBM),
        wanted,
        slot,
        global_ids,
    )


def layer_gathered(
    states,
    qkv_weight,
    out_weight,
    up_weight,
    down_weight,
    attn_gain,
    mlp_gain,
    global_ids,
    random_owner,
    random_local,
):
    tokens, width = states.shape
    inner = qkv_weight.shape[2]
    heads = inner // HD
    pairs = heads // 2
    blocks = tokens // BS
    g_count = global_ids.shape[0]
    n = lax.axis_size("seq")
    trees = len(TREES)
    piece = tokens // (2 * trees)
    chunk = 16 * BS
    chunks = CHUNKS
    rows = tokens // chunks
    bf = jnp.bfloat16
    dma = pltpu.SemaphoreType.DMA
    operands = (
        states.reshape(2 * trees, piece, width),
        qkv_weight,
        random_owner.transpose(0, 3, 1, 2),
        random_local.transpose(0, 3, 1, 2),
        global_ids,
        out_weight,
        up_weight,
        down_weight,
        attn_gain,
        mlp_gain,
    )
    return pl.pallas_call(
        functools.partial(gather_kernel, n, heads, blocks, g_count, chunks),
        out_shape=jax.ShapeDtypeStruct((tokens, width), bf),
        in_specs=[pl.BlockSpec(memory_space=pltpu.HBM)] * len(operands),
        out_specs=pl.BlockSpec(memory_space=pltpu.VMEM),
        scratch_shapes=[
            pltpu.VMEM((n * 2 * trees, piece, width), bf),
            pltpu.VMEM((width, inner), bf),
            pltpu.VMEM((width, 2 * inner), bf),
            pltpu.VMEM((n * blocks, BS, 2 * inner), bf),
            pltpu.VMEM((tokens, inner), bf),
            pltpu.VMEM((n * tokens // chunk, 2 * BS, chunk), jnp.float32),
            pltpu.VMEM((blocks * pairs, 2 * BS, (3 + R + g_count) * BS), jnp.float32),
            pltpu.VMEM((blocks * pairs, 2 * BS, (3 + R + g_count) * BS), bf),
            pltpu.VMEM((BS, LANES), bf),
            pltpu.VMEM((pairs * g_count, BS, LANES), bf),
            pltpu.SMEM((1, R, blocks, heads), jnp.int32),
            pltpu.SMEM((1, R, blocks, heads), jnp.int32),
            pltpu.SMEM(global_ids.shape, jnp.int32),
            pltpu.VMEM((pairs, tokens, LANES), bf),
            pltpu.VMEM(out_weight.shape, bf),
            pltpu.VMEM(up_weight.shape, bf),
            pltpu.VMEM(down_weight.shape, bf),
            pltpu.VMEM((width,), jnp.float32),
            pltpu.VMEM((width,), jnp.float32),
        ]
        + [pltpu.VMEM((chunks, rows, width), bf)] * 5
        + [dma((n * trees,))] * 4
        + [dma((n,)), dma((n * trees,)), dma((n,))]
        + [dma((4,)), dma((pairs * g_count,))]
        + [dma((chunks,))] * 4
        + [dma((len(operands) + 2,))],
        compiler_params=pltpu.CompilerParams(
            collective_id=0, has_side_effects=True, vmem_limit_bytes=48 * 1024 * 1024
        ),
    )(*[pltpu.with_memory_space_constraint(a, pltpu.HBM) for a in operands])


def gathers(states, qkv_weight, global_ids):
    tokens, width = states.shape
    n = lax.axis_size("seq")
    inner = qkv_weight.shape[2]
    held = n * tokens * (width + 2 * inner) * 2
    pairs = inner // LANES
    return (
        n % 4 == 0
        and global_ids.shape[0] == 2
        and pairs < 4
        and pairs < n // 4
        and lax.axis_size("mp") == 2
        and held <= 24 * 1024 * 1024
        and n * tokens % (16 * BS) == 0
        and tokens % (2 * len(TREES) * 16) == 0
        and 2 * inner % 256 == 0
    )


def shards(
    states,
    qkv_weight,
    out_weight,
    up_weight,
    down_weight,
    attn_gain,
    mlp_gain,
    global_ids,
    random_owner,
    random_local,
):
    tokens, width = states.shape
    if gathers(states, qkv_weight, global_ids):
        return layer_gathered(
            states,
            qkv_weight,
            out_weight,
            up_weight,
            down_weight,
            attn_gain,
            mlp_gain,
            global_ids,
            random_owner,
            random_local,
        )
    bf = jnp.bfloat16
    dma = pltpu.SemaphoreType.DMA
    att = attend_requested(states, qkv_weight, global_ids, random_owner, random_local)

    chunks = 4
    rows = tokens // chunks
    link = jnp.bfloat16
    return pl.pallas_call(
        functools.partial(tail_kernel, chunks),
        out_shape=jax.ShapeDtypeStruct((tokens, width), bf),
        in_specs=vmem_specs(7),
        out_specs=pl.BlockSpec(memory_space=pltpu.VMEM),
        scratch_shapes=[pltpu.VMEM((chunks, rows, width), link)] * 4
        + [dma((chunks,))] * 4
        + [pltpu.VMEM((chunks, rows, width), bf)],
        compiler_params=pltpu.CompilerParams(
            collective_id=1, has_side_effects=True, vmem_limit_bytes=32 * 1024 * 1024
        ),
    )(
        att,
        states,
        out_weight,
        up_weight,
        down_weight,
        attn_gain.reshape(1, width),
        mlp_gain.reshape(1, width),
    )


def solution(mesh):
    in_specs = (
        P("seq", None),
        P(None, None, "mp"),
        P("mp", None),
        P(None, "mp"),
        P("mp", None),
        P(),
        P(),
        P(),
        P("mp", "seq", None, None),
        P("mp", "seq", None, None),
    )
    out_specs = P("seq", None)
    return jax.shard_map(shards, mesh=mesh, in_specs=in_specs, out_specs=out_specs, check_vma=False)
```

```python
import functools

import jax
import jax.numpy as jnp
from jax import lax
from jax.experimental import pallas as pl
from jax.experimental.pallas import tpu as pltpu
from jax.sharding import PartitionSpec as P

HD = 64
BS = 64
R = 3
LANES = 128
MESH = pl.DeviceIdType.MESH

EPSILON = 1e-05
NEGATIVE = -1e30


def layer_norm(inputs, scales):
    center = jnp.mean(inputs, axis=-1, keepdims=True)
    shifted = inputs - center
    spread = jnp.mean(shifted * shifted, axis=-1, keepdims=True)
    return shifted * lax.rsqrt(spread + EPSILON) * scales


def dot_t(a, b):
    return lax.dot_general(a, b, (((1,), (1,)), ((), ())), preferred_element_type=jnp.float32)


def dot(a, b):
    return jnp.dot(a, b, preferred_element_type=jnp.float32)


def swap_halves(x):
    return pltpu.roll(x, HD, 1)


def attend_kernel(
    n,
    cap,
    heads,
    blocks,
    g_count,
    states_hbm,
    weight_hbm,
    wanted,
    slot,
    gids,
    att,
    states,
    weight,
    tab,
    tab_s,
    cand,
    cand_in,
    pick,
    gath,
    gstates,
    kvb,
    qpad,
    stage,
    rr,
    halo_l,
    halo_r,
    win,
    gq,
    gkv,
    part,
    part_in,
    gmine,
    gout,
    scores,
    s_tab,
    r_tab,
    s_cand,
    r_cand,
    s_gath,
    r_gath,
    s_rand,
    r_rand,
    s_halo,
    r_halo,
    s_part,
    r_part,
    s_gout,
    r_gout,
    s_mp,
    r_mp,
    l_sem,
    w_sem,
):
    me = lax.axis_index("seq")
    mine = lax.axis_index("mp")
    pairs = heads // 2
    width = states.shape[1]
    cols = width // LANES
    quarters = BS // 16
    half = gath.shape[0]
    gper = gath.shape[1] // (cols * quarters)
    units = gper * cols * quarters
    per = cand_in.shape[1]
    cand_parts = units // per
    rows_per = part_in.shape[2]
    part_parts = part.shape[0]
    left = lax.rem(me + n - 1, n)
    right = lax.rem(me + 1, n)

    def peer(k):
        return lax.rem(me + k, n)

    def each_peer(body):
        def step(k, carry):
            body(peer(k))
            return carry

        lax.fori_loop(1, n, step, 0)

    def guarded(limit, who, body):
        if limit < n:
            pl.when(who < limit)(body)
        else:
            body()

    def remote(src, dst, ssem, rsem, d):
        return pltpu.make_async_remote_copy(
            src_ref=src,
            dst_ref=dst,
            send_sem=ssem,
            recv_sem=rsem,
            device_id={"seq": d},
            device_id_type=MESH,
        )

    def tab_copy(d, owner):
        return remote(wanted.at[d], tab.at[owner], s_tab.at[d], r_tab.at[owner], d)

    def cand_copy(d, owner, at):
        return remote(
            cand.at[pl.ds(at * per, per)], cand_in.at[owner], s_cand.at[d], r_cand.at[owner], d
        )

    def gath_copy(d, owner):
        return remote(
            pick, gath.at[mine, pl.ds(owner * per, per)], s_gath.at[d], r_gath.at[owner], d
        )

    def rand_copy(d, owner):
        return remote(
            stage.at[pl.ds(d * cap, cap)],
            rr.at[pl.ds(owner * cap, cap)],
            s_rand.at[d],
            r_rand.at[owner],
            d,
        )

    def part_copy(d, owner, at):
        return remote(part.at[at], part_in.at[owner], s_part.at[d], r_part.at[owner], d)

    def gout_copy(d, owner):
        return remote(gmine, gout.at[owner], s_gout.at[d], r_gout.at[owner], d)

    def mp_copy(k, owner):
        other = lax.rem(mine + k, half)
        return pltpu.make_async_remote_copy(
            src_ref=gath.at[mine],
            dst_ref=gath.at[owner],
            send_sem=s_mp.at[k],
            recv_sem=r_mp.at[owner],
            device_id={"mp": other},
            device_id_type=MESH,
        )

    to_right = remote(
        kvb.at[pl.ds((blocks - 1) * heads, heads)], halo_l, s_halo.at[0], r_halo.at[0], right
    )
    to_left = remote(kvb.at[pl.ds(0, heads)], halo_r, s_halo.at[1], r_halo.at[1], left)

    loads = [pltpu.make_async_copy(states_hbm, states, w_sem.at[3])] + [
        pltpu.make_async_copy(weight_hbm.at[i], weight.at[i], w_sem.at[i]) for i in (1, 2, 0)
    ]
    for load in loads:
        load.start()

    barrier = pltpu.get_barrier_semaphore()
    each_peer(
        lambda d: pl.semaphore_signal(barrier, inc=1, device_id={"seq": d}, device_id_type=MESH)
    )
    for k in range(1, half):
        pl.semaphore_signal(
            barrier, inc=1, device_id={"mp": lax.rem(mine + k, half)}, device_id_type=MESH
        )

    loads[0].wait()
    for i in range(gper):
        local = lax.rem(gids[mine * gper + i], blocks)
        for j in range(cols):
            cut = slice(j * LANES, (j + 1) * LANES)
            piece = states[0:BS, cut]
            for b in range(1, blocks):
                piece = jnp.where(local == b, states[b * BS : (b + 1) * BS, cut], piece)
            for q in range(quarters):
                cand[(i * cols + j) * quarters + q] = piece[q * 16 : (q + 1) * 16]
    tab[me] = wanted[me]

    def own_cand():
        cand_in[me] = cand[pl.ds(me * per, per)]

    guarded(cand_parts, me, own_cand)
    loads[1].wait()
    loads[2].wait()

    lane = lax.broadcasted_iota(jnp.int32, (BS, LANES), 1)
    low = lane < HD
    x = states[...]
    for j in range(pairs):
        cut = slice(j * LANES, (j + 1) * LANES)
        k = dot(x, weight[1, :, cut])
        v = dot(x, weight[2, :, cut])
        for b in range(blocks):
            kb, vb = k[b * BS : (b + 1) * BS], v[b * BS : (b + 1) * BS]
            kvb[b * heads + 2 * j] = jnp.where(low, kb, swap_halves(vb)).astype(jnp.bfloat16)
            kvb[b * heads + 2 * j + 1] = jnp.where(low, swap_halves(kb), vb).astype(jnp.bfloat16)

    pl.semaphore_wait(barrier, n - 1 + half - 1)
    each_peer(lambda d: tab_copy(d, me).start())
    each_peer(lambda d: guarded(cand_parts, d, lambda: cand_copy(d, me, d).start()))
    to_right.start()
    to_left.start()

    loads[3].wait()
    scaling = HD ** (-0.5)
    for j in range(pairs):
        cut = slice(j * LANES, (j + 1) * LANES)
        q = dot(x, weight[0, :, cut]).astype(jnp.bfloat16).astype(jnp.float32) * scaling
        for b in range(blocks):
            qb = q[b * BS : (b + 1) * BS]
            qpad[b * heads + 2 * j] = jnp.where(low, qb, 0.0).astype(jnp.bfloat16)
            qpad[b * heads + 2 * j + 1] = jnp.where(low, swap_halves(qb), 0.0).astype(jnp.bfloat16)

    def relay():
        each_peer(lambda d: cand_copy(d, d, me).wait_recv())
        for u in range(per):
            g = (me * per + u) // (cols * quarters)
            wanted_id = gids[mine * gper + g]

            def choose(d, so_far):
                here = (wanted_id >= d * blocks) & (wanted_id < (d + 1) * blocks)
                return jnp.where(here, cand_in[d, u], so_far)

            pick[u] = lax.fori_loop(1, n, choose, cand_in[0, u])
        gath[mine, pl.ds(me * per, per)] = pick[...]
        each_peer(lambda d: gath_copy(d, me).start())

    guarded(cand_parts, me, relay)

    each_peer(lambda d: tab_copy(d, d).wait_recv())
    table = pltpu.make_async_copy(tab, tab_s, l_sem)
    table.start()
    table.wait()

    def serve(d):
        for c in range(cap):
            stage[d * cap + c] = kvb[tab_s[d, 0, c]]
        rand_copy(d, me).start()

    def serve_some(start, stop):
        def step(k, carry):
            serve(peer(k))
            return carry

        lax.fori_loop(start, stop, step, 0)

    for c in range(cap):
        rr[me * cap + c] = kvb[tab_s[me, 0, c]]

    each_peer(lambda d: guarded(cand_parts, d, lambda: gath_copy(d, d).wait_recv()))
    for k in range(1, half):
        mp_copy(k, mine).start()
    for k in range(1, half):
        mp_copy(k, lax.rem(mine + k, half)).wait_recv()
    for g in range(g_count):
        for j in range(cols):
            for q in range(quarters):
                gstates[g * BS + q * 16 : g * BS + (q + 1) * 16, j * LANES : (j + 1) * LANES] = (
                    gath[g // gper, ((g % gper) * cols + j) * quarters + q]
                )
    gx = gstates[...]
    rows = g_count * BS
    glane = lax.broadcasted_iota(jnp.int32, (rows, LANES), 1)
    glow = glane < HD
    for j in range(pairs):
        cut = slice(j * LANES, (j + 1) * LANES)
        q = dot(gx, weight[0, :, cut]).astype(jnp.bfloat16).astype(jnp.float32) * scaling
        k = dot(gx, weight[1, :, cut])
        v = dot(gx, weight[2, :, cut])
        gq[2 * j] = jnp.where(glow, q, 0.0).astype(jnp.bfloat16)
        gq[2 * j + 1] = jnp.where(glow, swap_halves(q), 0.0).astype(jnp.bfloat16)
        gkv[2 * j] = jnp.where(glow, k, swap_halves(v)).astype(jnp.bfloat16)
        gkv[2 * j + 1] = jnp.where(glow, swap_halves(k), v).astype(jnp.bfloat16)

    for h in range(heads):
        keys = jnp.concatenate([kvb[b * heads + h] for b in range(blocks)], axis=0)
        s = dot_t(gq[h], keys)
        high = jnp.max(s, axis=-1, keepdims=True)
        e = jnp.exp(s - high)
        total = jnp.sum(e, axis=-1, keepdims=True)
        e_high = e.astype(jnp.bfloat16)
        e_low = (e - e_high.astype(jnp.float32)).astype(jnp.bfloat16)
        acc = (dot(e_high, keys) + dot(e_low, keys)) * (1.0 / total)
        level = high + jnp.log(total)
        first = level.astype(jnp.bfloat16).astype(jnp.float32)
        second = (level - first).astype(jnp.bfloat16).astype(jnp.float32)
        third = level - first - second
        packed = jnp.where(
            glane < 16,
            first,
            jnp.where(glane < 32, second, jnp.where(glow, third, acc)),
        ).astype(jnp.bfloat16)
        cuts = rows // rows_per
        for c in range(cuts):
            part[(h // 2) * cuts + c, h % 2] = packed[c * rows_per : (c + 1) * rows_per]
    each_peer(lambda d: guarded(part_parts, d, lambda: part_copy(d, me, d).start()))
    serve_some(1, n)

    to_right.wait_recv()
    to_left.wait_recv()
    win[0:heads] = halo_l[...]
    win[heads : heads + blocks * heads] = kvb[...]
    win[heads + blocks * heads :] = halo_r[...]

    near = 3 + g_count
    slot_lane = lax.broadcasted_iota(jnp.int32, (BS, near * BS), 1)

    def near_keys(at, h):
        return jnp.concatenate([win[at + t * heads] for t in range(3)] + [gkv[h]], axis=0)

    def near_step(b, carry):
        first = me * blocks + b
        start = jnp.where(first == 0, BS, 0)
        stop = jnp.where(first == n * blocks - 1, 2 * BS, 3 * BS)
        outside = (slot_lane < start) | ((slot_lane >= stop) & (slot_lane < 3 * BS))
        for h in range(heads):
            at = b * heads + h
            scores[at] = jnp.where(outside, NEGATIVE, dot_t(qpad[at], near_keys(at, h)))
        return carry

    lax.fori_loop(0, blocks, near_step, 0)

    def combine():
        part_in[me] = part[me]
        each_peer(lambda d: part_copy(d, d, me).wait_recv())
        outs = []
        for parity in range(2):

            def level(d):
                piece = part_in[d, parity].astype(jnp.float32)
                return piece, piece[:, 0:1] + piece[:, 16:17] + piece[:, 32:33]

            def top(d, best):
                return jnp.maximum(best, level(d)[1])

            best = lax.fori_loop(1, n, top, level(0)[1])

            def add(d, so_far):
                piece, high = level(d)
                factor = jnp.exp(high - best)
                return so_far[0] + piece * factor, so_far[1] + factor

            zero = (jnp.zeros((rows_per, LANES), jnp.float32), jnp.zeros((rows_per, 1), jnp.float32))
            summed, total = lax.fori_loop(0, n, add, zero)
            outs.append(summed / total)
        plow = lax.broadcasted_iota(jnp.int32, (rows_per, LANES), 1) < HD
        done = jnp.where(plow, swap_halves(outs[0]), outs[1]).astype(jnp.bfloat16)
        gmine[...] = done
        gout[me] = done
        each_peer(lambda d: gout_copy(d, me).start())

    guarded(part_parts, me, combine)

    each_peer(lambda d: rand_copy(d, d).wait_recv())

    def block_step(b, carry):
        for j in range(pairs):
            halves = []
            for h in (2 * j, 2 * j + 1):
                at = b * heads + h
                early_keys = near_keys(at, h)
                keys = jnp.concatenate([rr[slot[at * R + r]] for r in range(R)], axis=0)
                s = dot_t(qpad[at], keys)
                early_s = scores[at]
                high = jnp.maximum(
                    jnp.max(s, axis=-1, keepdims=True), jnp.max(early_s, axis=-1, keepdims=True)
                )
                e = jnp.exp(s - high)
                early_e = jnp.exp(early_s - high)
                total = jnp.sum(e, axis=-1, keepdims=True) + jnp.sum(
                    early_e, axis=-1, keepdims=True
                )
                share = 1.0 / total
                w = (e * share).astype(jnp.bfloat16)
                early_w = (early_e * share).astype(jnp.bfloat16)
                halves.append(dot(w, keys) + dot(early_w, early_keys))
            att[j, pl.ds(pl.multiple_of(b * BS, BS), BS), :] = jnp.where(
                low, swap_halves(halves[0]), halves[1]
            ).astype(jnp.bfloat16)
        return carry

    lax.fori_loop(0, blocks, block_step, 0)

    each_peer(lambda d: guarded(part_parts, d, lambda: gout_copy(d, d).wait_recv()))
    for j in range(pairs):
        for g in range(g_count):
            cuts = BS // rows_per
            at = (j * g_count + g) * cuts
            row = jnp.concatenate([gout[at + c] for c in range(cuts)], axis=0).astype(jnp.float32)
            for b in range(blocks):
                here = gids[g] == me * blocks + b
                old = att[j, b * BS : (b + 1) * BS, :].astype(jnp.float32)
                att[j, b * BS : (b + 1) * BS, :] = jnp.where(here, row, old).astype(jnp.bfloat16)

    def drain(d):
        tab_copy(d, me).wait_send()
        guarded(cand_parts, d, lambda: cand_copy(d, me, d).wait_send())
        guarded(cand_parts, me, lambda: gath_copy(d, me).wait_send())
        rand_copy(d, me).wait_send()
        guarded(part_parts, d, lambda: part_copy(d, me, d).wait_send())
        guarded(part_parts, me, lambda: gout_copy(d, me).wait_send())

    each_peer(drain)
    for k in range(1, half):
        mp_copy(k, mine).wait_send()
    to_right.wait_send()
    to_left.wait_send()


TREES = ("zxy", "zyx", "yzx", "xzy")
PLACES = ((0, 0), (1, 0), (0, 1), (1, 1))
TURNS = (
    (-21.5, -8.5, -4.5, 11.5),
    (-15.0, 1.0, -2.5, 14.5),
    (-17.5, 0.0, -6.5, 11.5),
    (-13.0, -3.0, 2.5, 15.0),
)
PAUSES = (7.5, 9.5, 13.5, 18.0)
ROUND = 9.0
CHUNKS = 2
OWN = 16


def arrivals(depth):
    steps = []
    for slot in range(depth):
        for p, (dx, dy) in enumerate(PLACES):
            if not slot and not p:
                continue
            place = (slot, dx, dy)
            turns = [ROUND * slot + row[p] for row in TURNS]
            steps += [(turn, 0, t, place) for t, turn in enumerate(turns)]
            steps.append((max(turns) + PAUSES[p], 1, 0, place))
    return [step[1:] for step in sorted(steps)]


def hops(tree, slot, dx, dy):
    moved = {"x": dx, "y": dy, "z": slot}
    last = max((i for i in range(3) if moved[tree[i]]), default=-1)
    onward = tree[last + 1 :]
    via = tree[last] if last >= 0 else ""
    return via, ("z" if via == "z" else "") + onward


def slots(z, depth):
    inward = 1 if 2 * z < depth else -1
    return sorted(range(depth), key=lambda q: (abs(q - z), (z - q) * inward))


def gather_kernel(
    n,
    heads,
    blocks,
    g_count,
    chunks,
    states_hbm,
    weight_hbm,
    owner_hbm,
    local_hbm,
    gids_hbm,
    out_hbm,
    up_hbm,
    down_hbm,
    gain1_hbm,
    gain2_hbm,
    out,
    xs,
    wq,
    wkv,
    kv,
    q_all,
    wide,
    scores,
    weights,
    gmine,
    gout,
    owner,
    local,
    gids,
    att,
    out_w,
    up_w,
    down_w,
    gain1,
    gain2,
    mine1,
    theirs1,
    mine2,
    theirs2,
    normed,
    s_x,
    s_y,
    s_up,
    s_down,
    s_mp,
    r_ici,
    r_mp,
    s_gout,
    r_gout,
    s1,
    r1,
    s2,
    r2,
    l_sem,
):
    me = lax.axis_index("seq")
    mine = lax.axis_index("mp")
    pairs = heads // 2
    inner = heads * HD
    trees = len(TREES)
    per = 2 * trees
    piece = xs.shape[1]
    width = xs.shape[2]
    tokens = per * piece
    depth = n // 4
    x_at, y_at, z_at = lax.rem(me, 2), lax.rem(me // 2, 2), me // 4

    def remote(src, dst, ssem, rsem, where):
        return pltpu.make_async_remote_copy(
            src_ref=src,
            dst_ref=dst,
            send_sem=ssem,
            recv_sem=rsem,
            device_id=where,
            device_id_type=MESH,
        )

    def plane(slot):
        if slot == 0:
            return z_at
        found = slots(0, depth)[slot]
        for z in range(1, depth):
            found = jnp.where(z_at == z, slots(z, depth)[slot], found)
        return found

    def shard_of(slot, dx, dy):
        x = 1 - x_at if dx else x_at
        y = 1 - y_at if dy else y_at
        return plane(slot) * 4 + y * 2 + x

    def ici(shard, t, ssem, d):
        at = xs.at[(shard * 2 + mine) * trees + t]
        return remote(at, at, ssem.at[0], r_ici.at[shard * trees + t], {"seq": d})

    def across(shard, core):
        at = xs.at[pl.ds((shard * 2 + core) * trees, trees)]
        return remote(at, at, s_mp.at[0], r_mp.at[shard], {"mp": 1 - mine})

    x_peer = me + 1 - 2 * x_at
    y_peer = me + 2 - 4 * y_at
    up, down = lax.rem(me + 4, n), lax.rem(me + n - 4, n)

    def onward(t, slot, dx, dy, act):
        shard = shard_of(slot, dx, dy)
        via, axes = hops(TREES[t], slot, dx, dy)
        for axis in axes:
            if axis == "x":
                act(ici(shard, t, s_x, x_peer))
            elif axis == "y":
                act(ici(shard, t, s_y, y_peer))
            else:
                source = plane(slot)
                go_up = z_at < depth - 1
                go_down = z_at > 0
                if via == "z":
                    go_up = go_up & (source < z_at)
                    go_down = go_down & (source > z_at)
                pl.when(go_up)(lambda: act(ici(shard, t, s_up, up)))
                pl.when(go_down)(lambda: act(ici(shard, t, s_down, down)))

    order = arrivals(depth)

    pairs_of = [
        (states_hbm, xs.at[pl.ds(me * per, per)]),
        (weight_hbm.at[1], wkv.at[:, 0:inner]),
        (weight_hbm.at[2], wkv.at[:, inner : 2 * inner]),
        (weight_hbm.at[0], wq),
        (owner_hbm, owner),
        (local_hbm, local),
        (gids_hbm, gids),
        (gain1_hbm, gain1),
        (gain2_hbm, gain2),
        (out_hbm, out_w),
        (up_hbm, up_w),
        (down_hbm, down_w),
    ]
    loads = [pltpu.make_async_copy(a, b, l_sem.at[i]) for i, (a, b) in enumerate(pairs_of)]
    loads[0].start()
    barrier = pltpu.get_barrier_semaphore()
    for d in (x_peer, y_peer):
        pl.semaphore_signal(barrier, inc=1, device_id={"seq": d}, device_id_type=MESH)
    pl.semaphore_signal(barrier, inc=1, device_id={"mp": 1 - mine}, device_id_type=MESH)
    for there, d in ((z_at < depth - 1, up), (z_at > 0, down)):
        pl.when(there)(
            lambda d=d: pl.semaphore_signal(
                barrier, inc=1, device_id={"seq": d}, device_id_type=MESH
            )
        )
    for load in loads[1:4]:
        load.start()
    column = jnp.where(z_at < depth - 1, 1, 0) + jnp.where(z_at > 0, 1, 0)
    loads[0].wait()
    pl.semaphore_wait(barrier, 3 + column)
    for t in range(trees):
        onward(t, 0, 0, 0, lambda copy: copy.start())
    for load in loads[4:]:
        load.start()

    def project(*shards):
        x = [xs[pl.ds(shard * per, per)].reshape(tokens, width) for shard in shards]
        y = dot(jnp.concatenate(x, axis=0), wkv[...]).astype(jnp.bfloat16)
        for i, shard in enumerate(shards):
            part = y[i * tokens : (i + 1) * tokens]
            kv[pl.ds(shard * blocks, blocks)] = part.reshape(blocks, BS, 2 * inner)

    scaling = HD ** (-0.5)

    def project_own():
        for load in loads[1:4]:
            load.wait()
        x = xs[pl.ds(me * per, per)].reshape(tokens, width)
        q = dot(x, wq[...]).astype(jnp.bfloat16).astype(jnp.float32) * scaling
        q_all[...] = q.astype(jnp.bfloat16)
        project(me)

    left = dict()
    ready = []
    for i, (kind, t, place) in enumerate(order):
        if i == OWN:
            project_own()
        shard = shard_of(*place)
        if kind:
            across(shard, 1 - mine).wait_recv()
            ready.append(shard)
            after = [step[0] for step in order[i + 1 : i + 3]]
            if after != [1, 1] or len(ready) == 2:
                project(*ready)
                ready = []
            continue
        ici(shard, t, s_x, x_peer).wait_recv()
        onward(t, *place, lambda copy: copy.start())
        left[place] = left.get(place, trees) - 1
        if left[place] == 0:
            across(shard, mine).start()
    for load in loads[4:]:
        load.wait()

    lane = lax.broadcasted_iota(jnp.int32, (BS, LANES), 1)
    low = lane < HD

    def split(q):
        zero = jnp.zeros_like(q)
        return jnp.concatenate([jnp.where(low, q, zero), jnp.where(low, zero, q)], axis=0)

    def together(out):
        return jnp.where(low, out[0:BS], out[BS : 2 * BS]).astype(jnp.bfloat16)

    spot = lax.rem(me, 4)
    final = n - 1
    steps, _, chunk = wide.shape
    per_chunk = chunk // BS

    def fold(best, s, join):
        for c in range(0, s.shape[1], LANES):
            best = join(best, s[:, c : c + LANES])
        return best

    def share():
        first_block = spot < pairs
        j = jnp.where(first_block, spot, z_at)
        block = jnp.where(first_block, gids[0], gids[1])
        k_cut = pl.ds(pl.multiple_of(j * LANES, LANES), LANES)
        v_cut = pl.ds(pl.multiple_of(inner + j * LANES, LANES), LANES)
        rows = BS // piece
        x = xs[pl.ds(block * rows, rows)].reshape(BS, width)
        q = dot(x, wq[:, k_cut]).astype(jnp.bfloat16).astype(jnp.float32) * scaling
        q2 = split(q.astype(jnp.bfloat16))

        def score(c, best):
            keys = kv[pl.ds(c * per_chunk, per_chunk), :, k_cut].reshape(chunk, LANES)
            s = dot_t(q2, keys)
            wide[c] = s
            return fold(best, s, jnp.maximum)

        best = jnp.full((2 * BS, LANES), NEGATIVE, jnp.float32)
        best = lax.fori_loop(0, steps, score, best, unroll=True)
        high = jnp.max(best, axis=-1, keepdims=True)

        def add(c, so_far):
            values = kv[pl.ds(c * per_chunk, per_chunk), :, v_cut].reshape(chunk, LANES)
            e = jnp.exp(wide[c] - high)
            e_high = e.astype(jnp.bfloat16)
            e_low = (e - e_high.astype(jnp.float32)).astype(jnp.bfloat16)
            return (
                so_far[0] + dot(e_high, values) + dot(e_low, values),
                fold(so_far[1], e, jnp.add),
            )

        zero = jnp.zeros((2 * BS, LANES), jnp.float32)
        summed, total = lax.fori_loop(0, steps, add, (zero, zero), unroll=True)
        gmine[...] = together(summed / jnp.sum(total, axis=-1, keepdims=True))

        def to_plane():
            for k in range(1, 4):
                gout_copy(spot, k).start()

        pl.when(first_block)(to_plane)
        pl.when(spot >= pairs)(lambda: last_copy(z_at).start())

    def gout_copy(unit, k):
        d = z_at * 4 + lax.rem(spot + k, 4)
        return remote(gmine, gout.at[unit], s_gout.at[k], r_gout.at[unit], {"seq": d})

    def last_copy(unit):
        at = pairs + unit
        return remote(gmine, gout.at[at], s_gout.at[0], r_gout.at[at], {"seq": final})

    shares = (spot < pairs) | ((spot == 3) & (z_at < pairs))
    pl.when(shares)(share)

    slot_lane = lax.broadcasted_iota(jnp.int32, (1, 3 * BS), 1)
    last = n * blocks - 1

    def rows_of(b, j, base):
        first = me * blocks + b
        near = [jnp.maximum(first - 1, 0), first, jnp.minimum(first + 1, last)]
        one = [owner[0, r, b, 2 * j] * blocks + local[0, r, b, 2 * j] for r in range(R)]
        two = [owner[0, r, b, 2 * j + 1] * blocks + local[0, r, b, 2 * j + 1] for r in range(R)]
        cut = slice(base + j * LANES, base + (j + 1) * LANES)
        return jnp.concatenate(
            [kv[at, :, cut] for at in near]
            + [jnp.where(low, kv[a, :, cut], kv[c, :, cut]) for a, c in zip(one, two)]
            + [kv[gids[g], :, cut] for g in range(g_count)],
            axis=0,
        )

    for b in range(blocks):
        first = me * blocks + b
        start = jnp.where(first == 0, BS, 0)
        stop = jnp.where(first == last, 2 * BS, 3 * BS)
        bias = jnp.where((slot_lane < start) | (slot_lane >= stop), NEGATIVE, 0.0)
        for j in range(pairs):
            q = q_all[b * BS : (b + 1) * BS, j * LANES : (j + 1) * LANES]
            s = dot_t(split(q), rows_of(b, j, 0))
            scores[b * pairs + j, :, 0 : 3 * BS] = s[:, 0 : 3 * BS] + bias
            scores[b * pairs + j, :, 3 * BS :] = s[:, 3 * BS :]

    def weigh(i, carry):
        for part in range(2):
            cut = slice(part * BS, (part + 1) * BS)
            s = scores[i, cut]
            e = jnp.exp(s - jnp.max(s, axis=-1, keepdims=True))
            share_of = 1.0 / jnp.sum(e, axis=-1, keepdims=True)
            weights[i, cut] = (e * share_of).astype(jnp.bfloat16)
        return carry

    lax.fori_loop(0, blocks * pairs, weigh, 0, unroll=6)

    for b in range(blocks):
        for j in range(pairs):
            mixed = dot(weights[b * pairs + j], rows_of(b, j, inner))
            att[j, b * BS : (b + 1) * BS, :] = together(mixed)

    for unit in range(pairs):
        pl.when(spot != unit)(lambda unit=unit: gout_copy(unit, 1).wait_recv())
    for j in range(pairs):
        row = jnp.where(spot == j, gmine[...], gout[j])
        for b in range(blocks):
            cut = slice(b * BS, (b + 1) * BS)
            here = gids[0] == me * blocks + b
            att[j, cut, :] = jnp.where(here, row, att[j, cut, :])

    def take_last():
        for unit in range(pairs):
            last_copy(unit).wait_recv()
            att[unit, (blocks - 1) * BS : blocks * BS, :] = gout[pairs + unit]

    pl.when(me == final)(take_last)

    rows = tokens // chunks

    def swap(sent, got, ssem, rsem, c):
        return remote(sent.at[c], got.at[c], ssem.at[c], rsem.at[c], {"mp": 1 - mine})

    for c in range(chunks):
        cut = slice(c * rows, (c + 1) * rows)
        acc = dot(att[0, cut, :], out_w[0:LANES, :])
        for j in range(1, pairs):
            acc = acc + dot(att[j, cut, :], out_w[j * LANES : (j + 1) * LANES, :])
        mine1[c] = acc.astype(mine1.dtype)
        swap(mine1, theirs1, s1, r1, c).start()
    x = xs[pl.ds(me * per, per)].reshape(chunks, rows, width)
    for c in range(chunks):
        swap(mine1, theirs1, s1, r1, c).wait_recv()
        summed = mine1[c].astype(jnp.float32) + theirs1[c].astype(jnp.float32)
        norm = layer_norm(x[c].astype(jnp.float32) + summed, gain1[...].reshape(1, width))
        norm = norm.astype(jnp.bfloat16)
        normed[c] = norm
        v = dot(norm, up_w[...])
        hidden = (v * (1.0 + lax.erf(v * (0.5**0.5))) * 0.5).astype(jnp.bfloat16)
        mine2[c] = dot(hidden, down_w[...]).astype(mine2.dtype)
        swap(mine2, theirs2, s2, r2, c).start()
    for c in range(chunks):
        cut = slice(c * rows, (c + 1) * rows)
        swap(mine2, theirs2, s2, r2, c).wait_recv()
        summed = mine2[c].astype(jnp.float32) + theirs2[c].astype(jnp.float32)
        out[cut, :] = layer_norm(normed[c].astype(jnp.float32) + summed, gain2[...].reshape(1, width)).astype(
            jnp.bfloat16
        )
    for c in range(chunks):
        swap(mine1, theirs1, s1, r1, c).wait_send()
        swap(mine2, theirs2, s2, r2, c).wait_send()
    def drain_all(ssem, count):
        at = xs.at[pl.ds(0, count)]
        remote(at, at, ssem.at[0], r_mp.at[0], {"mp": 1 - mine}).wait_send()

    taken = [(t, (0, 0, 0)) for t in range(trees)]
    taken += [(t, place) for kind, t, place in order if not kind]
    routes = [(hops(TREES[t], *place), place[0]) for t, place in taken]
    for axis, ssem in (("x", s_x), ("y", s_y)):
        drain_all(ssem, sum(axis in axes for (_, axes), _ in routes))
    drain_all(s_mp, trees * len(left))
    for z in range(depth):
        here = [(via, slots(z, depth)[slot]) for (via, axes), slot in routes if "z" in axes]
        rising = sum(via != "z" or source < z for via, source in here) if z < depth - 1 else 0
        falling = sum(via != "z" or source > z for via, source in here) if z > 0 else 0
        for count, ssem in ((rising, s_up), (falling, s_down)):
            if count:
                pl.when(z_at == z)(lambda ssem=ssem, count=count: drain_all(ssem, count))

    def drain():
        for k in range(1, 4):
            gout_copy(spot, k).wait_send()

    pl.when(spot < pairs)(drain)
    pl.when((spot == 3) & (z_at < pairs))(lambda: last_copy(z_at).wait_send())


def tail_kernel(
    chunks,
    att,
    states,
    out_w,
    up_w,
    down_w,
    gain1,
    gain2,
    out,
    mine1,
    theirs1,
    mine2,
    theirs2,
    s1,
    r1,
    s2,
    r2,
    normed,
):
    other = 1 - lax.axis_index("mp")
    barrier = pltpu.get_barrier_semaphore()
    pl.semaphore_signal(barrier, inc=1, device_id={"mp": other}, device_id_type=MESH)
    pl.semaphore_wait(barrier, 1)
    rows = states.shape[0] // chunks

    def swap(mine, theirs, ssem, rsem, c):
        return pltpu.make_async_remote_copy(
            src_ref=mine.at[c],
            dst_ref=theirs.at[c],
            send_sem=ssem.at[c],
            recv_sem=rsem.at[c],
            device_id={"mp": other},
            device_id_type=MESH,
        )

    for c in range(chunks):
        cut = slice(c * rows, (c + 1) * rows)
        acc = dot(att[0, cut, :], out_w[0:LANES, :])
        for j in range(1, att.shape[0]):
            acc = acc + dot(att[j, cut, :], out_w[j * LANES : (j + 1) * LANES, :])
        mine1[c] = acc.astype(mine1.dtype)
        swap(mine1, theirs1, s1, r1, c).start()
    for c in range(chunks):
        cut = slice(c * rows, (c + 1) * rows)
        swap(mine1, theirs1, s1, r1, c).wait_recv()
        summed = mine1[c].astype(jnp.float32) + theirs1[c].astype(jnp.float32)
        norm = layer_norm(states[cut, :].astype(jnp.float32) + summed, gain1[...])
        norm = norm.astype(jnp.bfloat16)
        normed[c] = norm
        v = dot(norm, up_w[...])
        hidden = (v * (1.0 + lax.erf(v * (0.5**0.5))) * 0.5).astype(jnp.bfloat16)
        mine2[c] = dot(hidden, down_w[...]).astype(mine2.dtype)
        swap(mine2, theirs2, s2, r2, c).start()
    for c in range(chunks):
        cut = slice(c * rows, (c + 1) * rows)
        swap(mine2, theirs2, s2, r2, c).wait_recv()
        summed = mine2[c].astype(jnp.float32) + theirs2[c].astype(jnp.float32)
        out[cut, :] = layer_norm(normed[c].astype(jnp.float32) + summed, gain2[...]).astype(
            jnp.bfloat16
        )
    for c in range(chunks):
        swap(mine1, theirs1, s1, r1, c).wait_send()
        swap(mine2, theirs2, s2, r2, c).wait_send()


def vmem_specs(count):
    return [pl.BlockSpec(memory_space=pltpu.VMEM)] * count


def attend_requested(states, qkv_weight, global_ids, random_owner, random_local):
    tokens, width = states.shape
    heads = qkv_weight.shape[2] // HD
    pairs = heads // 2
    blocks = tokens // BS
    g_count = global_ids.shape[0]
    n = lax.axis_size("seq")

    owner = random_owner.reshape(-1)
    items = owner.shape[0]
    cap = max(2, items // n + 1)
    head_list = jnp.broadcast_to(
        jnp.arange(heads, dtype=jnp.int32)[None, :, None], (blocks, heads, R)
    ).reshape(-1)
    code = random_local.reshape(-1) * heads + head_list
    earlier = jnp.arange(items)[:, None] > jnp.arange(items)[None, :]
    rank = jnp.sum(((owner[:, None] == owner[None, :]) & earlier).astype(jnp.int32), axis=1)
    slot = owner * cap + rank
    place = owner * LANES + rank
    wanted = jnp.sum(
        jnp.where(
            place[None, None, :]
            == (jnp.arange(n)[:, None] * LANES + jnp.arange(LANES)[None, :])[:, :, None],
            code[None, None, :],
            0,
        ),
        axis=2,
    ).reshape(n, 1, LANES)

    half = lax.axis_size("mp")
    units = (g_count // half) * (width // LANES) * (BS // 16)
    per = -(-units // n)
    part_rows = pairs * g_count * BS
    rows_per = -(-part_rows // n // 16) * 16
    parts = part_rows // rows_per
    bf = jnp.bfloat16
    own = blocks * heads
    dma = pltpu.SemaphoreType.DMA
    return pl.pallas_call(
        functools.partial(attend_kernel, n, cap, heads, blocks, g_count),
        out_shape=jax.ShapeDtypeStruct((pairs, tokens, LANES), bf),
        in_specs=[pl.BlockSpec(memory_space=pltpu.HBM)] * 2
        + vmem_specs(1)
        + [pl.BlockSpec(memory_space=pltpu.SMEM)] * 2,
        out_specs=pl.BlockSpec(memory_space=pltpu.VMEM),
        scratch_shapes=[
            pltpu.VMEM((tokens, width), bf),
            pltpu.VMEM(qkv_weight.shape, bf),
            pltpu.VMEM((n, 1, LANES), jnp.int32),
            pltpu.SMEM((n, 1, LANES), jnp.int32),
            pltpu.VMEM((units, 16, LANES), bf),
            pltpu.VMEM((n, per, 16, LANES), bf),
            pltpu.VMEM((per, 16, LANES), bf),
            pltpu.VMEM((half, units, 16, LANES), bf),
            pltpu.VMEM((g_count * BS, width), bf),
            pltpu.VMEM((own, BS, LANES), bf),
            pltpu.VMEM((own, BS, LANES), bf),
            pltpu.VMEM((n * cap, BS, LANES), bf),
            pltpu.VMEM((n * cap, BS, LANES), bf),
            pltpu.VMEM((heads, BS, LANES), bf),
            pltpu.VMEM((heads, BS, LANES), bf),
            pltpu.VMEM((own + 2 * heads, BS, LANES), bf),
            pltpu.VMEM((heads, g_count * BS, LANES), bf),
            pltpu.VMEM((heads, g_count * BS, LANES), bf),
            pltpu.VMEM((parts, 2, rows_per, LANES), bf),
            pltpu.VMEM((n, 2, rows_per, LANES), bf),
            pltpu.VMEM((rows_per, LANES), bf),
            pltpu.VMEM((parts, rows_per, LANES), bf),
            pltpu.VMEM((own, BS, (3 + g_count) * BS), jnp.float32),
        ]
        + [dma((n,))] * 8
        + [dma((2,))] * 2
        + [dma((n,))] * 4
        + [dma((half,))] * 2
        + [dma(()), dma((4,))],
        cost_estimate=pl.CostEstimate(
            flops=30_000_000_000, bytes_accessed=20_000_000, transcendentals=0
        ),
        compiler_params=pltpu.CompilerParams(
            collective_id=0, has_side_effects=True, vmem_limit_bytes=32 * 1024 * 1024
        ),
    )(
        pltpu.with_memory_space_constraint(states, pltpu.HBM),
        pltpu.with_memory_space_constraint(qkv_weight, pltpu.HBM),
        wanted,
        slot,
        global_ids,
    )


def layer_gathered(
    states,
    qkv_weight,
    out_weight,
    up_weight,
    down_weight,
    attn_gain,
    mlp_gain,
    global_ids,
    random_owner,
    random_local,
):
    tokens, width = states.shape
    inner = qkv_weight.shape[2]
    heads = inner // HD
    pairs = heads // 2
    blocks = tokens // BS
    g_count = global_ids.shape[0]
    n = lax.axis_size("seq")
    trees = len(TREES)
    piece = tokens // (2 * trees)
    chunk = 16 * BS
    chunks = CHUNKS
    rows = tokens // chunks
    bf = jnp.bfloat16
    dma = pltpu.SemaphoreType.DMA
    operands = (
        states.reshape(2 * trees, piece, width),
        qkv_weight,
        random_owner.transpose(0, 3, 1, 2),
        random_local.transpose(0, 3, 1, 2),
        global_ids,
        out_weight,
        up_weight,
        down_weight,
        attn_gain,
        mlp_gain,
    )
    return pl.pallas_call(
        functools.partial(gather_kernel, n, heads, blocks, g_count, chunks),
        out_shape=jax.ShapeDtypeStruct((tokens, width), bf),
        in_specs=[pl.BlockSpec(memory_space=pltpu.HBM)] * len(operands),
        out_specs=pl.BlockSpec(memory_space=pltpu.VMEM),
        scratch_shapes=[
            pltpu.VMEM((n * 2 * trees, piece, width), bf),
            pltpu.VMEM((width, inner), bf),
            pltpu.VMEM((width, 2 * inner), bf),
            pltpu.VMEM((n * blocks, BS, 2 * inner), bf),
            pltpu.VMEM((tokens, inner), bf),
            pltpu.VMEM((n * tokens // chunk, 2 * BS, chunk), jnp.float32),
            pltpu.VMEM((blocks * pairs, 2 * BS, (3 + R + g_count) * BS), jnp.float32),
            pltpu.VMEM((blocks * pairs, 2 * BS, (3 + R + g_count) * BS), bf),
            pltpu.VMEM((BS, LANES), bf),
            pltpu.VMEM((pairs * g_count, BS, LANES), bf),
            pltpu.SMEM((1, R, blocks, heads), jnp.int32),
            pltpu.SMEM((1, R, blocks, heads), jnp.int32),
            pltpu.SMEM(global_ids.shape, jnp.int32),
            pltpu.VMEM((pairs, tokens, LANES), bf),
            pltpu.VMEM(out_weight.shape, bf),
            pltpu.VMEM(up_weight.shape, bf),
            pltpu.VMEM(down_weight.shape, bf),
            pltpu.VMEM((width,), jnp.float32),
            pltpu.VMEM((width,), jnp.float32),
        ]
        + [pltpu.VMEM((chunks, rows, width), bf)] * 5
        + [dma((1,))] * 5
        + [dma((n * trees,)), dma((n,))]
        + [dma((4,)), dma((pairs * g_count,))]
        + [dma((chunks,))] * 4
        + [dma((len(operands) + 2,))],
        compiler_params=pltpu.CompilerParams(
            collective_id=0, has_side_effects=True, vmem_limit_bytes=48 * 1024 * 1024
        ),
    )(*[pltpu.with_memory_space_constraint(a, pltpu.HBM) for a in operands])


def gathers(states, qkv_weight, global_ids):
    tokens, width = states.shape
    n = lax.axis_size("seq")
    inner = qkv_weight.shape[2]
    held = n * tokens * (width + 2 * inner) * 2
    pairs = inner // LANES
    return (
        n % 4 == 0
        and global_ids.shape[0] == 2
        and pairs < 4
        and pairs < n // 4
        and lax.axis_size("mp") == 2
        and held <= 24 * 1024 * 1024
        and n * tokens % (16 * BS) == 0
        and tokens % (2 * len(TREES) * 16) == 0
        and 2 * inner % 256 == 0
    )


def shards(
    states,
    qkv_weight,
    out_weight,
    up_weight,
    down_weight,
    attn_gain,
    mlp_gain,
    global_ids,
    random_owner,
    random_local,
):
    tokens, width = states.shape
    if gathers(states, qkv_weight, global_ids):
        return layer_gathered(
            states,
            qkv_weight,
            out_weight,
            up_weight,
            down_weight,
            attn_gain,
            mlp_gain,
            global_ids,
            random_owner,
            random_local,
        )
    bf = jnp.bfloat16
    dma = pltpu.SemaphoreType.DMA
    att = attend_requested(states, qkv_weight, global_ids, random_owner, random_local)

    chunks = 4
    rows = tokens // chunks
    link = jnp.bfloat16
    return pl.pallas_call(
        functools.partial(tail_kernel, chunks),
        out_shape=jax.ShapeDtypeStruct((tokens, width), bf),
        in_specs=vmem_specs(7),
        out_specs=pl.BlockSpec(memory_space=pltpu.VMEM),
        scratch_shapes=[pltpu.VMEM((chunks, rows, width), link)] * 4
        + [dma((chunks,))] * 4
        + [pltpu.VMEM((chunks, rows, width), bf)],
        compiler_params=pltpu.CompilerParams(
            collective_id=1, has_side_effects=True, vmem_limit_bytes=32 * 1024 * 1024
        ),
    )(
        att,
        states,
        out_weight,
        up_weight,
        down_weight,
        attn_gain.reshape(1, width),
        mlp_gain.reshape(1, width),
    )


def solution(mesh):
    in_specs = (
        P("seq", None),
        P(None, None, "mp"),
        P("mp", None),
        P(None, "mp"),
        P("mp", None),
        P(),
        P(),
        P(),
        P("mp", "seq", None, None),
        P("mp", "seq", None, None),
    )
    out_specs = P("seq", None)
    return jax.shard_map(shards, mesh=mesh, in_specs=in_specs, out_specs=out_specs, check_vma=False)
```

```python
import functools

import jax
import jax.numpy as jnp
from jax import lax
from jax.experimental import pallas as pl
from jax.experimental.pallas import tpu as pltpu
from jax.sharding import PartitionSpec as P

HD = 64
BS = 64
R = 3
LANES = 128
MESH = pl.DeviceIdType.MESH

EPSILON = 1e-05
NEGATIVE = -1e30


def layer_norm(inputs, scales):
    center = jnp.mean(inputs, axis=-1, keepdims=True)
    shifted = inputs - center
    spread = jnp.mean(shifted * shifted, axis=-1, keepdims=True)
    return shifted * lax.rsqrt(spread + EPSILON) * scales


def dot_t(a, b):
    return lax.dot_general(a, b, (((1,), (1,)), ((), ())), preferred_element_type=jnp.float32)


def dot(a, b):
    return jnp.dot(a, b, preferred_element_type=jnp.float32)


def swap_halves(x):
    return pltpu.roll(x, HD, 1)


def attend_kernel(
    n,
    cap,
    heads,
    blocks,
    g_count,
    states_hbm,
    weight_hbm,
    wanted,
    slot,
    gids,
    att,
    states,
    weight,
    tab,
    tab_s,
    cand,
    cand_in,
    pick,
    gath,
    gstates,
    kvb,
    qpad,
    stage,
    rr,
    halo_l,
    halo_r,
    win,
    gq,
    gkv,
    part,
    part_in,
    gmine,
    gout,
    scores,
    s_tab,
    r_tab,
    s_cand,
    r_cand,
    s_gath,
    r_gath,
    s_rand,
    r_rand,
    s_halo,
    r_halo,
    s_part,
    r_part,
    s_gout,
    r_gout,
    s_mp,
    r_mp,
    l_sem,
    w_sem,
):
    me = lax.axis_index("seq")
    mine = lax.axis_index("mp")
    pairs = heads // 2
    width = states.shape[1]
    cols = width // LANES
    quarters = BS // 16
    half = gath.shape[0]
    gper = gath.shape[1] // (cols * quarters)
    units = gper * cols * quarters
    per = cand_in.shape[1]
    cand_parts = units // per
    rows_per = part_in.shape[2]
    part_parts = part.shape[0]
    left = lax.rem(me + n - 1, n)
    right = lax.rem(me + 1, n)

    def peer(k):
        return lax.rem(me + k, n)

    def each_peer(body):
        def step(k, carry):
            body(peer(k))
            return carry

        lax.fori_loop(1, n, step, 0)

    def guarded(limit, who, body):
        if limit < n:
            pl.when(who < limit)(body)
        else:
            body()

    def remote(src, dst, ssem, rsem, d):
        return pltpu.make_async_remote_copy(
            src_ref=src,
            dst_ref=dst,
            send_sem=ssem,
            recv_sem=rsem,
            device_id={"seq": d},
            device_id_type=MESH,
        )

    def tab_copy(d, owner):
        return remote(wanted.at[d], tab.at[owner], s_tab.at[d], r_tab.at[owner], d)

    def cand_copy(d, owner, at):
        return remote(
            cand.at[pl.ds(at * per, per)], cand_in.at[owner], s_cand.at[d], r_cand.at[owner], d
        )

    def gath_copy(d, owner):
        return remote(
            pick, gath.at[mine, pl.ds(owner * per, per)], s_gath.at[d], r_gath.at[owner], d
        )

    def rand_copy(d, owner):
        return remote(
            stage.at[pl.ds(d * cap, cap)],
            rr.at[pl.ds(owner * cap, cap)],
            s_rand.at[d],
            r_rand.at[owner],
            d,
        )

    def part_copy(d, owner, at):
        return remote(part.at[at], part_in.at[owner], s_part.at[d], r_part.at[owner], d)

    def gout_copy(d, owner):
        return remote(gmine, gout.at[owner], s_gout.at[d], r_gout.at[owner], d)

    def mp_copy(k, owner):
        other = lax.rem(mine + k, half)
        return pltpu.make_async_remote_copy(
            src_ref=gath.at[mine],
            dst_ref=gath.at[owner],
            send_sem=s_mp.at[k],
            recv_sem=r_mp.at[owner],
            device_id={"mp": other},
            device_id_type=MESH,
        )

    to_right = remote(
        kvb.at[pl.ds((blocks - 1) * heads, heads)], halo_l, s_halo.at[0], r_halo.at[0], right
    )
    to_left = remote(kvb.at[pl.ds(0, heads)], halo_r, s_halo.at[1], r_halo.at[1], left)

    loads = [pltpu.make_async_copy(states_hbm, states, w_sem.at[3])] + [
        pltpu.make_async_copy(weight_hbm.at[i], weight.at[i], w_sem.at[i]) for i in (1, 2, 0)
    ]
    for load in loads:
        load.start()

    barrier = pltpu.get_barrier_semaphore()
    each_peer(
        lambda d: pl.semaphore_signal(barrier, inc=1, device_id={"seq": d}, device_id_type=MESH)
    )
    for k in range(1, half):
        pl.semaphore_signal(
            barrier, inc=1, device_id={"mp": lax.rem(mine + k, half)}, device_id_type=MESH
        )

    loads[0].wait()
    for i in range(gper):
        local = lax.rem(gids[mine * gper + i], blocks)
        for j in range(cols):
            cut = slice(j * LANES, (j + 1) * LANES)
            piece = states[0:BS, cut]
            for b in range(1, blocks):
                piece = jnp.where(local == b, states[b * BS : (b + 1) * BS, cut], piece)
            for q in range(quarters):
                cand[(i * cols + j) * quarters + q] = piece[q * 16 : (q + 1) * 16]
    tab[me] = wanted[me]

    def own_cand():
        cand_in[me] = cand[pl.ds(me * per, per)]

    guarded(cand_parts, me, own_cand)
    loads[1].wait()
    loads[2].wait()

    lane = lax.broadcasted_iota(jnp.int32, (BS, LANES), 1)
    low = lane < HD
    x = states[...]
    for j in range(pairs):
        cut = slice(j * LANES, (j + 1) * LANES)
        k = dot(x, weight[1, :, cut])
        v = dot(x, weight[2, :, cut])
        for b in range(blocks):
            kb, vb = k[b * BS : (b + 1) * BS], v[b * BS : (b + 1) * BS]
            kvb[b * heads + 2 * j] = jnp.where(low, kb, swap_halves(vb)).astype(jnp.bfloat16)
            kvb[b * heads + 2 * j + 1] = jnp.where(low, swap_halves(kb), vb).astype(jnp.bfloat16)

    pl.semaphore_wait(barrier, n - 1 + half - 1)
    each_peer(lambda d: tab_copy(d, me).start())
    each_peer(lambda d: guarded(cand_parts, d, lambda: cand_copy(d, me, d).start()))
    to_right.start()
    to_left.start()

    loads[3].wait()
    scaling = HD ** (-0.5)
    for j in range(pairs):
        cut = slice(j * LANES, (j + 1) * LANES)
        q = dot(x, weight[0, :, cut]).astype(jnp.bfloat16).astype(jnp.float32) * scaling
        for b in range(blocks):
            qb = q[b * BS : (b + 1) * BS]
            qpad[b * heads + 2 * j] = jnp.where(low, qb, 0.0).astype(jnp.bfloat16)
            qpad[b * heads + 2 * j + 1] = jnp.where(low, swap_halves(qb), 0.0).astype(jnp.bfloat16)

    def relay():
        each_peer(lambda d: cand_copy(d, d, me).wait_recv())
        for u in range(per):
            g = (me * per + u) // (cols * quarters)
            wanted_id = gids[mine * gper + g]

            def choose(d, so_far):
                here = (wanted_id >= d * blocks) & (wanted_id < (d + 1) * blocks)
                return jnp.where(here, cand_in[d, u], so_far)

            pick[u] = lax.fori_loop(1, n, choose, cand_in[0, u])
        gath[mine, pl.ds(me * per, per)] = pick[...]
        each_peer(lambda d: gath_copy(d, me).start())

    guarded(cand_parts, me, relay)

    each_peer(lambda d: tab_copy(d, d).wait_recv())
    table = pltpu.make_async_copy(tab, tab_s, l_sem)
    table.start()
    table.wait()

    def serve(d):
        for c in range(cap):
            stage[d * cap + c] = kvb[tab_s[d, 0, c]]
        rand_copy(d, me).start()

    def serve_some(start, stop):
        def step(k, carry):
            serve(peer(k))
            return carry

        lax.fori_loop(start, stop, step, 0)

    for c in range(cap):
        rr[me * cap + c] = kvb[tab_s[me, 0, c]]

    each_peer(lambda d: guarded(cand_parts, d, lambda: gath_copy(d, d).wait_recv()))
    for k in range(1, half):
        mp_copy(k, mine).start()
    for k in range(1, half):
        mp_copy(k, lax.rem(mine + k, half)).wait_recv()
    for g in range(g_count):
        for j in range(cols):
            for q in range(quarters):
                gstates[g * BS + q * 16 : g * BS + (q + 1) * 16, j * LANES : (j + 1) * LANES] = (
                    gath[g // gper, ((g % gper) * cols + j) * quarters + q]
                )
    gx = gstates[...]
    rows = g_count * BS
    glane = lax.broadcasted_iota(jnp.int32, (rows, LANES), 1)
    glow = glane < HD
    for j in range(pairs):
        cut = slice(j * LANES, (j + 1) * LANES)
        q = dot(gx, weight[0, :, cut]).astype(jnp.bfloat16).astype(jnp.float32) * scaling
        k = dot(gx, weight[1, :, cut])
        v = dot(gx, weight[2, :, cut])
        gq[2 * j] = jnp.where(glow, q, 0.0).astype(jnp.bfloat16)
        gq[2 * j + 1] = jnp.where(glow, swap_halves(q), 0.0).astype(jnp.bfloat16)
        gkv[2 * j] = jnp.where(glow, k, swap_halves(v)).astype(jnp.bfloat16)
        gkv[2 * j + 1] = jnp.where(glow, swap_halves(k), v).astype(jnp.bfloat16)

    for h in range(heads):
        keys = jnp.concatenate([kvb[b * heads + h] for b in range(blocks)], axis=0)
        s = dot_t(gq[h], keys)
        high = jnp.max(s, axis=-1, keepdims=True)
        e = jnp.exp(s - high)
        total = jnp.sum(e, axis=-1, keepdims=True)
        e_high = e.astype(jnp.bfloat16)
        e_low = (e - e_high.astype(jnp.float32)).astype(jnp.bfloat16)
        acc = (dot(e_high, keys) + dot(e_low, keys)) * (1.0 / total)
        level = high + jnp.log(total)
        first = level.astype(jnp.bfloat16).astype(jnp.float32)
        second = (level - first).astype(jnp.bfloat16).astype(jnp.float32)
        third = level - first - second
        packed = jnp.where(
            glane < 16,
            first,
            jnp.where(glane < 32, second, jnp.where(glow, third, acc)),
        ).astype(jnp.bfloat16)
        cuts = rows // rows_per
        for c in range(cuts):
            part[(h // 2) * cuts + c, h % 2] = packed[c * rows_per : (c + 1) * rows_per]
    each_peer(lambda d: guarded(part_parts, d, lambda: part_copy(d, me, d).start()))
    serve_some(1, n)

    to_right.wait_recv()
    to_left.wait_recv()
    win[0:heads] = halo_l[...]
    win[heads : heads + blocks * heads] = kvb[...]
    win[heads + blocks * heads :] = halo_r[...]

    near = 3 + g_count
    slot_lane = lax.broadcasted_iota(jnp.int32, (BS, near * BS), 1)

    def near_keys(at, h):
        return jnp.concatenate([win[at + t * heads] for t in range(3)] + [gkv[h]], axis=0)

    def near_step(b, carry):
        first = me * blocks + b
        start = jnp.where(first == 0, BS, 0)
        stop = jnp.where(first == n * blocks - 1, 2 * BS, 3 * BS)
        outside = (slot_lane < start) | ((slot_lane >= stop) & (slot_lane < 3 * BS))
        for h in range(heads):
            at = b * heads + h
            scores[at] = jnp.where(outside, NEGATIVE, dot_t(qpad[at], near_keys(at, h)))
        return carry

    lax.fori_loop(0, blocks, near_step, 0)

    def combine():
        part_in[me] = part[me]
        each_peer(lambda d: part_copy(d, d, me).wait_recv())
        outs = []
        for parity in range(2):

            def level(d):
                piece = part_in[d, parity].astype(jnp.float32)
                return piece, piece[:, 0:1] + piece[:, 16:17] + piece[:, 32:33]

            def top(d, best):
                return jnp.maximum(best, level(d)[1])

            best = lax.fori_loop(1, n, top, level(0)[1])

            def add(d, so_far):
                piece, high = level(d)
                factor = jnp.exp(high - best)
                return so_far[0] + piece * factor, so_far[1] + factor

            zero = (jnp.zeros((rows_per, LANES), jnp.float32), jnp.zeros((rows_per, 1), jnp.float32))
            summed, total = lax.fori_loop(0, n, add, zero)
            outs.append(summed / total)
        plow = lax.broadcasted_iota(jnp.int32, (rows_per, LANES), 1) < HD
        done = jnp.where(plow, swap_halves(outs[0]), outs[1]).astype(jnp.bfloat16)
        gmine[...] = done
        gout[me] = done
        each_peer(lambda d: gout_copy(d, me).start())

    guarded(part_parts, me, combine)

    each_peer(lambda d: rand_copy(d, d).wait_recv())

    def block_step(b, carry):
        for j in range(pairs):
            halves = []
            for h in (2 * j, 2 * j + 1):
                at = b * heads + h
                early_keys = near_keys(at, h)
                keys = jnp.concatenate([rr[slot[at * R + r]] for r in range(R)], axis=0)
                s = dot_t(qpad[at], keys)
                early_s = scores[at]
                high = jnp.maximum(
                    jnp.max(s, axis=-1, keepdims=True), jnp.max(early_s, axis=-1, keepdims=True)
                )
                e = jnp.exp(s - high)
                early_e = jnp.exp(early_s - high)
                total = jnp.sum(e, axis=-1, keepdims=True) + jnp.sum(
                    early_e, axis=-1, keepdims=True
                )
                share = 1.0 / total
                w = (e * share).astype(jnp.bfloat16)
                early_w = (early_e * share).astype(jnp.bfloat16)
                halves.append(dot(w, keys) + dot(early_w, early_keys))
            att[j, pl.ds(pl.multiple_of(b * BS, BS), BS), :] = jnp.where(
                low, swap_halves(halves[0]), halves[1]
            ).astype(jnp.bfloat16)
        return carry

    lax.fori_loop(0, blocks, block_step, 0)

    each_peer(lambda d: guarded(part_parts, d, lambda: gout_copy(d, d).wait_recv()))
    for j in range(pairs):
        for g in range(g_count):
            cuts = BS // rows_per
            at = (j * g_count + g) * cuts
            row = jnp.concatenate([gout[at + c] for c in range(cuts)], axis=0).astype(jnp.float32)
            for b in range(blocks):
                here = gids[g] == me * blocks + b
                old = att[j, b * BS : (b + 1) * BS, :].astype(jnp.float32)
                att[j, b * BS : (b + 1) * BS, :] = jnp.where(here, row, old).astype(jnp.bfloat16)

    def drain(d):
        tab_copy(d, me).wait_send()
        guarded(cand_parts, d, lambda: cand_copy(d, me, d).wait_send())
        guarded(cand_parts, me, lambda: gath_copy(d, me).wait_send())
        rand_copy(d, me).wait_send()
        guarded(part_parts, d, lambda: part_copy(d, me, d).wait_send())
        guarded(part_parts, me, lambda: gout_copy(d, me).wait_send())

    each_peer(drain)
    for k in range(1, half):
        mp_copy(k, mine).wait_send()
    to_right.wait_send()
    to_left.wait_send()


TREES = ("zxy", "zyx", "yzx", "xzy")
PLACES = ((0, 0), (1, 0), (0, 1), (1, 1))
TURNS = (
    (-21.5, -8.5, -4.5, 11.5),
    (-15.0, 1.0, -2.5, 14.5),
    (-17.5, 0.0, -6.5, 11.5),
    (-13.0, -3.0, 2.5, 15.0),
)
PAUSES = (7.5, 9.5, 13.5, 18.0)
ROUND = 9.0
CHUNKS = 2
OWN = 16


def arrivals(depth):
    steps = []
    for slot in range(depth):
        for p, (dx, dy) in enumerate(PLACES):
            if not slot and not p:
                continue
            place = (slot, dx, dy)
            turns = [ROUND * slot + row[p] for row in TURNS]
            steps += [(turn, 0, t, place) for t, turn in enumerate(turns)]
            steps.append((max(turns) + PAUSES[p], 1, 0, place))
    return [step[1:] for step in sorted(steps)]


def hops(tree, slot, dx, dy):
    moved = {"x": dx, "y": dy, "z": slot}
    last = max((i for i in range(3) if moved[tree[i]]), default=-1)
    onward = tree[last + 1 :]
    via = tree[last] if last >= 0 else ""
    return via, ("z" if via == "z" else "") + onward


def slots(z, depth):
    inward = 1 if 2 * z < depth else -1
    return sorted(range(depth), key=lambda q: (abs(q - z), (z - q) * inward))


def gather_kernel(
    n,
    heads,
    blocks,
    g_count,
    chunks,
    states_hbm,
    weight_hbm,
    owner_hbm,
    local_hbm,
    gids_hbm,
    out_hbm,
    up_hbm,
    down_hbm,
    gain1_hbm,
    gain2_hbm,
    out,
    xs,
    wq,
    wkv,
    kv,
    q_all,
    wide,
    scores,
    weights,
    gmine,
    gout,
    owner,
    local,
    gids,
    att,
    out_w,
    up_w,
    down_w,
    gain1,
    gain2,
    mine1,
    theirs1,
    mine2,
    theirs2,
    normed,
    s_x,
    s_y,
    s_up,
    s_down,
    s_mp,
    r_ici,
    r_mp,
    s_gout,
    r_gout,
    s1,
    r1,
    s2,
    r2,
    l_sem,
):
    me = lax.axis_index("seq")
    mine = lax.axis_index("mp")
    pairs = heads // 2
    inner = heads * HD
    trees = len(TREES)
    per = 2 * trees
    piece = xs.shape[1]
    width = xs.shape[2]
    tokens = per * piece
    depth = n // 4
    x_at, y_at, z_at = lax.rem(me, 2), lax.rem(me // 2, 2), me // 4

    def remote(src, dst, ssem, rsem, where):
        return pltpu.make_async_remote_copy(
            src_ref=src,
            dst_ref=dst,
            send_sem=ssem,
            recv_sem=rsem,
            device_id=where,
            device_id_type=MESH,
        )

    def plane(slot):
        if slot == 0:
            return z_at
        found = slots(0, depth)[slot]
        for z in range(1, depth):
            found = jnp.where(z_at == z, slots(z, depth)[slot], found)
        return found

    def shard_of(slot, dx, dy):
        x = 1 - x_at if dx else x_at
        y = 1 - y_at if dy else y_at
        return plane(slot) * 4 + y * 2 + x

    def ici(shard, t, ssem, d):
        at = xs.at[(shard * 2 + mine) * trees + t]
        return remote(at, at, ssem.at[0], r_ici.at[shard * trees + t], {"seq": d})

    def across(shard, core):
        at = xs.at[pl.ds((shard * 2 + core) * trees, trees)]
        return remote(at, at, s_mp.at[0], r_mp.at[shard], {"mp": 1 - mine})

    x_peer = me + 1 - 2 * x_at
    y_peer = me + 2 - 4 * y_at
    up, down = lax.rem(me + 4, n), lax.rem(me + n - 4, n)

    def onward(t, slot, dx, dy, act):
        shard = shard_of(slot, dx, dy)
        via, axes = hops(TREES[t], slot, dx, dy)
        for axis in axes:
            if axis == "x":
                act(ici(shard, t, s_x, x_peer))
            elif axis == "y":
                act(ici(shard, t, s_y, y_peer))
            else:
                source = plane(slot)
                go_up = z_at < depth - 1
                go_down = z_at > 0
                if via == "z":
                    go_up = go_up & (source < z_at)
                    go_down = go_down & (source > z_at)
                pl.when(go_up)(lambda: act(ici(shard, t, s_up, up)))
                pl.when(go_down)(lambda: act(ici(shard, t, s_down, down)))

    order = arrivals(depth)

    pairs_of = [
        (states_hbm, xs.at[pl.ds(me * per, per)]),
        (weight_hbm.at[1], wkv.at[:, 0:inner]),
        (weight_hbm.at[2], wkv.at[:, inner : 2 * inner]),
        (weight_hbm.at[0], wq),
        (owner_hbm, owner),
        (local_hbm, local),
        (gids_hbm, gids),
        (gain1_hbm, gain1),
        (gain2_hbm, gain2),
        (out_hbm, out_w),
        (up_hbm, up_w),
        (down_hbm, down_w),
    ]
    loads = [pltpu.make_async_copy(a, b, l_sem.at[i]) for i, (a, b) in enumerate(pairs_of)]
    loads[0].start()
    barrier = pltpu.get_barrier_semaphore()
    for d in (x_peer, y_peer):
        pl.semaphore_signal(barrier, inc=1, device_id={"seq": d}, device_id_type=MESH)
    pl.semaphore_signal(barrier, inc=1, device_id={"mp": 1 - mine}, device_id_type=MESH)
    for there, d in ((z_at < depth - 1, up), (z_at > 0, down)):
        pl.when(there)(
            lambda d=d: pl.semaphore_signal(
                barrier, inc=1, device_id={"seq": d}, device_id_type=MESH
            )
        )
    for load in loads[1:4]:
        load.start()
    column = jnp.where(z_at < depth - 1, 1, 0) + jnp.where(z_at > 0, 1, 0)
    loads[0].wait()
    pl.semaphore_wait(barrier, 3 + column)
    for t in range(trees):
        onward(t, 0, 0, 0, lambda copy: copy.start())
    for load in loads[4:]:
        load.start()

    def project(*shards):
        x = [xs[pl.ds(shard * per, per)].reshape(tokens, width) for shard in shards]
        y = dot(jnp.concatenate(x, axis=0), wkv[...]).astype(jnp.bfloat16)
        for i, shard in enumerate(shards):
            part = y[i * tokens : (i + 1) * tokens]
            kv[pl.ds(shard * blocks, blocks)] = part.reshape(blocks, BS, 2 * inner)

    scaling = HD ** (-0.5)

    def project_own():
        for load in loads[1:4]:
            load.wait()
        x = xs[pl.ds(me * per, per)].reshape(tokens, width)
        q = dot(x, wq[...]).astype(jnp.bfloat16).astype(jnp.float32) * scaling
        q_all[...] = q.astype(jnp.bfloat16)
        project(me)

    left = dict()
    ready = []
    for i, (kind, t, place) in enumerate(order):
        if i == OWN:
            project_own()
        shard = shard_of(*place)
        if kind:
            across(shard, 1 - mine).wait_recv()
            ready.append(shard)
            after = [step[0] for step in order[i + 1 : i + 3]]
            if after != [1, 1] or len(ready) == 2:
                project(*ready)
                ready = []
            continue
        ici(shard, t, s_x, x_peer).wait_recv()
        onward(t, *place, lambda copy: copy.start())
        left[place] = left.get(place, trees) - 1
        if left[place] == 0:
            across(shard, mine).start()
    for load in loads[4:]:
        load.wait()

    lane = lax.broadcasted_iota(jnp.int32, (BS, LANES), 1)
    low = lane < HD

    def split(q):
        zero = jnp.zeros_like(q)
        return jnp.concatenate([jnp.where(low, q, zero), jnp.where(low, zero, q)], axis=0)

    def together(out):
        return jnp.where(low, out[0:BS], out[BS : 2 * BS]).astype(jnp.bfloat16)

    spot = lax.rem(me, 4)
    final = n - 1
    steps, _, chunk = wide.shape
    per_chunk = chunk // BS

    def fold(best, s, join):
        for c in range(0, s.shape[1], LANES):
            best = join(best, s[:, c : c + LANES])
        return best

    def share():
        first_block = spot < pairs
        j = jnp.where(first_block, spot, z_at)
        block = jnp.where(first_block, gids[0], gids[1])
        k_cut = pl.ds(pl.multiple_of(j * LANES, LANES), LANES)
        v_cut = pl.ds(pl.multiple_of(inner + j * LANES, LANES), LANES)
        rows = BS // piece
        x = xs[pl.ds(block * rows, rows)].reshape(BS, width)
        q = dot(x, wq[:, k_cut]).astype(jnp.bfloat16).astype(jnp.float32) * scaling
        q2 = split(q.astype(jnp.bfloat16))

        def score(c, best):
            keys = kv[pl.ds(c * per_chunk, per_chunk), :, k_cut].reshape(chunk, LANES)
            s = dot_t(q2, keys)
            wide[c] = s
            return fold(best, s, jnp.maximum)

        best = jnp.full((2 * BS, LANES), NEGATIVE, jnp.float32)
        best = lax.fori_loop(0, steps, score, best, unroll=True)
        high = jnp.max(best, axis=-1, keepdims=True)

        def add(c, so_far):
            values = kv[pl.ds(c * per_chunk, per_chunk), :, v_cut].reshape(chunk, LANES)
            e = jnp.exp(wide[c] - high)
            e_high = e.astype(jnp.bfloat16)
            e_low = (e - e_high.astype(jnp.float32)).astype(jnp.bfloat16)
            return (
                so_far[0] + dot(e_high, values) + dot(e_low, values),
                fold(so_far[1], e, jnp.add),
            )

        zero = jnp.zeros((2 * BS, LANES), jnp.float32)
        summed, total = lax.fori_loop(0, steps, add, (zero, zero), unroll=True)
        gmine[...] = together(summed / jnp.sum(total, axis=-1, keepdims=True))

        def to_plane():
            for k in range(1, 4):
                gout_copy(spot, k).start()

        pl.when(first_block)(to_plane)
        pl.when(spot >= pairs)(lambda: last_copy(z_at).start())

    def gout_copy(unit, k):
        d = z_at * 4 + lax.rem(spot + k, 4)
        return remote(gmine, gout.at[unit], s_gout.at[k], r_gout.at[unit], {"seq": d})

    def last_copy(unit):
        at = pairs + unit
        return remote(gmine, gout.at[at], s_gout.at[0], r_gout.at[at], {"seq": final})

    shares = (spot < pairs) | ((spot == 3) & (z_at < pairs))
    pl.when(shares)(share)

    slot_lane = lax.broadcasted_iota(jnp.int32, (1, 3 * BS), 1)
    last = n * blocks - 1

    def rows_of(b, j, base):
        first = me * blocks + b
        near = [jnp.maximum(first - 1, 0), first, jnp.minimum(first + 1, last)]
        one = [owner[0, r, b, 2 * j] * blocks + local[0, r, b, 2 * j] for r in range(R)]
        two = [owner[0, r, b, 2 * j + 1] * blocks + local[0, r, b, 2 * j + 1] for r in range(R)]
        cut = slice(base + j * LANES, base + (j + 1) * LANES)
        return jnp.concatenate(
            [kv[at, :, cut] for at in near]
            + [jnp.where(low, kv[a, :, cut], kv[c, :, cut]) for a, c in zip(one, two)]
            + [kv[gids[g], :, cut] for g in range(g_count)],
            axis=0,
        )

    for b in range(blocks):
        first = me * blocks + b
        start = jnp.where(first == 0, BS, 0)
        stop = jnp.where(first == last, 2 * BS, 3 * BS)
        bias = jnp.where((slot_lane < start) | (slot_lane >= stop), NEGATIVE, 0.0)
        for j in range(pairs):
            q = q_all[b * BS : (b + 1) * BS, j * LANES : (j + 1) * LANES]
            s = dot_t(split(q), rows_of(b, j, 0))
            scores[b * pairs + j, :, 0 : 3 * BS] = s[:, 0 : 3 * BS] + bias
            scores[b * pairs + j, :, 3 * BS :] = s[:, 3 * BS :]

    def weigh(i, carry):
        for part in range(2):
            cut = slice(part * BS, (part + 1) * BS)
            s = scores[i, cut]
            e = jnp.exp(s - jnp.max(s, axis=-1, keepdims=True))
            share_of = 1.0 / jnp.sum(e, axis=-1, keepdims=True)
            weights[i, cut] = (e * share_of).astype(jnp.bfloat16)
        return carry

    lax.fori_loop(0, blocks * pairs, weigh, 0, unroll=True)

    for b in range(blocks):
        for j in range(pairs):
            mixed = dot(weights[b * pairs + j], rows_of(b, j, inner))
            att[j, b * BS : (b + 1) * BS, :] = together(mixed)

    for unit in range(pairs):
        pl.when(spot != unit)(lambda unit=unit: gout_copy(unit, 1).wait_recv())
    for j in range(pairs):
        row = jnp.where(spot == j, gmine[...], gout[j])
        for b in range(blocks):
            cut = slice(b * BS, (b + 1) * BS)
            here = gids[0] == me * blocks + b
            att[j, cut, :] = jnp.where(here, row, att[j, cut, :])

    def take_last():
        for unit in range(pairs):
            last_copy(unit).wait_recv()
            att[unit, (blocks - 1) * BS : blocks * BS, :] = gout[pairs + unit]

    pl.when(me == final)(take_last)

    rows = tokens // chunks

    def swap(sent, got, ssem, rsem, c):
        return remote(sent.at[c], got.at[c], ssem.at[0], rsem.at[c], {"mp": 1 - mine})

    for c in range(chunks):
        cut = slice(c * rows, (c + 1) * rows)
        acc = dot(att[0, cut, :], out_w[0:LANES, :])
        for j in range(1, pairs):
            acc = acc + dot(att[j, cut, :], out_w[j * LANES : (j + 1) * LANES, :])
        mine1[c] = acc.astype(mine1.dtype)
        swap(mine1, theirs1, s1, r1, c).start()
    x = xs[pl.ds(me * per, per)].reshape(chunks, rows, width)
    for c in range(chunks):
        swap(mine1, theirs1, s1, r1, c).wait_recv()
        summed = mine1[c].astype(jnp.float32) + theirs1[c].astype(jnp.float32)
        norm = layer_norm(x[c].astype(jnp.float32) + summed, gain1[...].reshape(1, width))
        norm = norm.astype(jnp.bfloat16)
        normed[c] = norm
        v = dot(norm, up_w[...])
        hidden = (v * (1.0 + lax.erf(v * (0.5**0.5))) * 0.5).astype(jnp.bfloat16)
        mine2[c] = dot(hidden, down_w[...]).astype(mine2.dtype)
        swap(mine2, theirs2, s2, r2, c).start()
    for c in range(chunks):
        cut = slice(c * rows, (c + 1) * rows)
        swap(mine2, theirs2, s2, r2, c).wait_recv()
        summed = mine2[c].astype(jnp.float32) + theirs2[c].astype(jnp.float32)
        out[cut, :] = layer_norm(normed[c].astype(jnp.float32) + summed, gain2[...].reshape(1, width)).astype(
            jnp.bfloat16
        )
    remote(mine1, theirs1, s1.at[0], r1.at[0], {"mp": 1 - mine}).wait_send()
    remote(mine2, theirs2, s2.at[0], r2.at[0], {"mp": 1 - mine}).wait_send()
    def drain_all(ssem, count):
        at = xs.at[pl.ds(0, count)]
        remote(at, at, ssem.at[0], r_mp.at[0], {"mp": 1 - mine}).wait_send()

    taken = [(t, (0, 0, 0)) for t in range(trees)]
    taken += [(t, place) for kind, t, place in order if not kind]
    routes = [(hops(TREES[t], *place), place[0]) for t, place in taken]
    for axis, ssem in (("x", s_x), ("y", s_y)):
        drain_all(ssem, sum(axis in axes for (_, axes), _ in routes))
    drain_all(s_mp, trees * len(left))
    for z in range(depth):
        here = [(via, slots(z, depth)[slot]) for (via, axes), slot in routes if "z" in axes]
        rising = sum(via != "z" or source < z for via, source in here) if z < depth - 1 else 0
        falling = sum(via != "z" or source > z for via, source in here) if z > 0 else 0
        for count, ssem in ((rising, s_up), (falling, s_down)):
            if count:
                pl.when(z_at == z)(lambda ssem=ssem, count=count: drain_all(ssem, count))

    def drain():
        for k in range(1, 4):
            gout_copy(spot, k).wait_send()

    pl.when(spot < pairs)(drain)
    pl.when((spot == 3) & (z_at < pairs))(lambda: last_copy(z_at).wait_send())


def tail_kernel(
    chunks,
    att,
    states,
    out_w,
    up_w,
    down_w,
    gain1,
    gain2,
    out,
    mine1,
    theirs1,
    mine2,
    theirs2,
    s1,
    r1,
    s2,
    r2,
    normed,
):
    other = 1 - lax.axis_index("mp")
    barrier = pltpu.get_barrier_semaphore()
    pl.semaphore_signal(barrier, inc=1, device_id={"mp": other}, device_id_type=MESH)
    pl.semaphore_wait(barrier, 1)
    rows = states.shape[0] // chunks

    def swap(mine, theirs, ssem, rsem, c):
        return pltpu.make_async_remote_copy(
            src_ref=mine.at[c],
            dst_ref=theirs.at[c],
            send_sem=ssem.at[c],
            recv_sem=rsem.at[c],
            device_id={"mp": other},
            device_id_type=MESH,
        )

    for c in range(chunks):
        cut = slice(c * rows, (c + 1) * rows)
        acc = dot(att[0, cut, :], out_w[0:LANES, :])
        for j in range(1, att.shape[0]):
            acc = acc + dot(att[j, cut, :], out_w[j * LANES : (j + 1) * LANES, :])
        mine1[c] = acc.astype(mine1.dtype)
        swap(mine1, theirs1, s1, r1, c).start()
    for c in range(chunks):
        cut = slice(c * rows, (c + 1) * rows)
        swap(mine1, theirs1, s1, r1, c).wait_recv()
        summed = mine1[c].astype(jnp.float32) + theirs1[c].astype(jnp.float32)
        norm = layer_norm(states[cut, :].astype(jnp.float32) + summed, gain1[...])
        norm = norm.astype(jnp.bfloat16)
        normed[c] = norm
        v = dot(norm, up_w[...])
        hidden = (v * (1.0 + lax.erf(v * (0.5**0.5))) * 0.5).astype(jnp.bfloat16)
        mine2[c] = dot(hidden, down_w[...]).astype(mine2.dtype)
        swap(mine2, theirs2, s2, r2, c).start()
    for c in range(chunks):
        cut = slice(c * rows, (c + 1) * rows)
        swap(mine2, theirs2, s2, r2, c).wait_recv()
        summed = mine2[c].astype(jnp.float32) + theirs2[c].astype(jnp.float32)
        out[cut, :] = layer_norm(normed[c].astype(jnp.float32) + summed, gain2[...]).astype(
            jnp.bfloat16
        )
    for c in range(chunks):
        swap(mine1, theirs1, s1, r1, c).wait_send()
        swap(mine2, theirs2, s2, r2, c).wait_send()


def vmem_specs(count):
    return [pl.BlockSpec(memory_space=pltpu.VMEM)] * count


def attend_requested(states, qkv_weight, global_ids, random_owner, random_local):
    tokens, width = states.shape
    heads = qkv_weight.shape[2] // HD
    pairs = heads // 2
    blocks = tokens // BS
    g_count = global_ids.shape[0]
    n = lax.axis_size("seq")

    owner = random_owner.reshape(-1)
    items = owner.shape[0]
    cap = max(2, items // n + 1)
    head_list = jnp.broadcast_to(
        jnp.arange(heads, dtype=jnp.int32)[None, :, None], (blocks, heads, R)
    ).reshape(-1)
    code = random_local.reshape(-1) * heads + head_list
    earlier = jnp.arange(items)[:, None] > jnp.arange(items)[None, :]
    rank = jnp.sum(((owner[:, None] == owner[None, :]) & earlier).astype(jnp.int32), axis=1)
    slot = owner * cap + rank
    place = owner * LANES + rank
    wanted = jnp.sum(
        jnp.where(
            place[None, None, :]
            == (jnp.arange(n)[:, None] * LANES + jnp.arange(LANES)[None, :])[:, :, None],
            code[None, None, :],
            0,
        ),
        axis=2,
    ).reshape(n, 1, LANES)

    half = lax.axis_size("mp")
    units = (g_count // half) * (width // LANES) * (BS // 16)
    per = -(-units // n)
    part_rows = pairs * g_count * BS
    rows_per = -(-part_rows // n // 16) * 16
    parts = part_rows // rows_per
    bf = jnp.bfloat16
    own = blocks * heads
    dma = pltpu.SemaphoreType.DMA
    return pl.pallas_call(
        functools.partial(attend_kernel, n, cap, heads, blocks, g_count),
        out_shape=jax.ShapeDtypeStruct((pairs, tokens, LANES), bf),
        in_specs=[pl.BlockSpec(memory_space=pltpu.HBM)] * 2
        + vmem_specs(1)
        + [pl.BlockSpec(memory_space=pltpu.SMEM)] * 2,
        out_specs=pl.BlockSpec(memory_space=pltpu.VMEM),
        scratch_shapes=[
            pltpu.VMEM((tokens, width), bf),
            pltpu.VMEM(qkv_weight.shape, bf),
            pltpu.VMEM((n, 1, LANES), jnp.int32),
            pltpu.SMEM((n, 1, LANES), jnp.int32),
            pltpu.VMEM((units, 16, LANES), bf),
            pltpu.VMEM((n, per, 16, LANES), bf),
            pltpu.VMEM((per, 16, LANES), bf),
            pltpu.VMEM((half, units, 16, LANES), bf),
            pltpu.VMEM((g_count * BS, width), bf),
            pltpu.VMEM((own, BS, LANES), bf),
            pltpu.VMEM((own, BS, LANES), bf),
            pltpu.VMEM((n * cap, BS, LANES), bf),
            pltpu.VMEM((n * cap, BS, LANES), bf),
            pltpu.VMEM((heads, BS, LANES), bf),
            pltpu.VMEM((heads, BS, LANES), bf),
            pltpu.VMEM((own + 2 * heads, BS, LANES), bf),
            pltpu.VMEM((heads, g_count * BS, LANES), bf),
            pltpu.VMEM((heads, g_count * BS, LANES), bf),
            pltpu.VMEM((parts, 2, rows_per, LANES), bf),
            pltpu.VMEM((n, 2, rows_per, LANES), bf),
            pltpu.VMEM((rows_per, LANES), bf),
            pltpu.VMEM((parts, rows_per, LANES), bf),
            pltpu.VMEM((own, BS, (3 + g_count) * BS), jnp.float32),
        ]
        + [dma((n,))] * 8
        + [dma((2,))] * 2
        + [dma((n,))] * 4
        + [dma((half,))] * 2
        + [dma(()), dma((4,))],
        cost_estimate=pl.CostEstimate(
            flops=30_000_000_000, bytes_accessed=20_000_000, transcendentals=0
        ),
        compiler_params=pltpu.CompilerParams(
            collective_id=0, has_side_effects=True, vmem_limit_bytes=32 * 1024 * 1024
        ),
    )(
        pltpu.with_memory_space_constraint(states, pltpu.HBM),
        pltpu.with_memory_space_constraint(qkv_weight, pltpu.HBM),
        wanted,
        slot,
        global_ids,
    )


def layer_gathered(
    states,
    qkv_weight,
    out_weight,
    up_weight,
    down_weight,
    attn_gain,
    mlp_gain,
    global_ids,
    random_owner,
    random_local,
):
    tokens, width = states.shape
    inner = qkv_weight.shape[2]
    heads = inner // HD
    pairs = heads // 2
    blocks = tokens // BS
    g_count = global_ids.shape[0]
    n = lax.axis_size("seq")
    trees = len(TREES)
    piece = tokens // (2 * trees)
    chunk = 16 * BS
    chunks = CHUNKS
    rows = tokens // chunks
    bf = jnp.bfloat16
    dma = pltpu.SemaphoreType.DMA
    operands = (
        states.reshape(2 * trees, piece, width),
        qkv_weight,
        random_owner.transpose(0, 3, 1, 2),
        random_local.transpose(0, 3, 1, 2),
        global_ids,
        out_weight,
        up_weight,
        down_weight,
        attn_gain,
        mlp_gain,
    )
    return pl.pallas_call(
        functools.partial(gather_kernel, n, heads, blocks, g_count, chunks),
        out_shape=jax.ShapeDtypeStruct((tokens, width), bf),
        in_specs=[pl.BlockSpec(memory_space=pltpu.HBM)] * len(operands),
        out_specs=pl.BlockSpec(memory_space=pltpu.VMEM),
        scratch_shapes=[
            pltpu.VMEM((n * 2 * trees, piece, width), bf),
            pltpu.VMEM((width, inner), bf),
            pltpu.VMEM((width, 2 * inner), bf),
            pltpu.VMEM((n * blocks, BS, 2 * inner), bf),
            pltpu.VMEM((tokens, inner), bf),
            pltpu.VMEM((n * tokens // chunk, 2 * BS, chunk), jnp.float32),
            pltpu.VMEM((blocks * pairs, 2 * BS, (3 + R + g_count) * BS), jnp.float32),
            pltpu.VMEM((blocks * pairs, 2 * BS, (3 + R + g_count) * BS), bf),
            pltpu.VMEM((BS, LANES), bf),
            pltpu.VMEM((pairs * g_count, BS, LANES), bf),
            pltpu.SMEM((1, R, blocks, heads), jnp.int32),
            pltpu.SMEM((1, R, blocks, heads), jnp.int32),
            pltpu.SMEM(global_ids.shape, jnp.int32),
            pltpu.VMEM((pairs, tokens, LANES), bf),
            pltpu.VMEM(out_weight.shape, bf),
            pltpu.VMEM(up_weight.shape, bf),
            pltpu.VMEM(down_weight.shape, bf),
            pltpu.VMEM((width,), jnp.float32),
            pltpu.VMEM((width,), jnp.float32),
        ]
        + [pltpu.VMEM((chunks, rows, width), bf)] * 5
        + [dma((1,))] * 5
        + [dma((n * trees,)), dma((n,))]
        + [dma((4,)), dma((pairs * g_count,))]
        + [dma((1,)), dma((chunks,))] * 2
        + [dma((len(operands) + 2,))],
        compiler_params=pltpu.CompilerParams(
            collective_id=0, has_side_effects=True, vmem_limit_bytes=48 * 1024 * 1024
        ),
    )(*[pltpu.with_memory_space_constraint(a, pltpu.HBM) for a in operands])


def gathers(states, qkv_weight, global_ids):
    tokens, width = states.shape
    n = lax.axis_size("seq")
    inner = qkv_weight.shape[2]
    held = n * tokens * (width + 2 * inner) * 2
    pairs = inner // LANES
    return (
        n % 4 == 0
        and global_ids.shape[0] == 2
        and pairs < 4
        and pairs < n // 4
        and lax.axis_size("mp") == 2
        and held <= 24 * 1024 * 1024
        and n * tokens % (16 * BS) == 0
        and tokens % (2 * len(TREES) * 16) == 0
        and 2 * inner % 256 == 0
    )


def shards(
    states,
    qkv_weight,
    out_weight,
    up_weight,
    down_weight,
    attn_gain,
    mlp_gain,
    global_ids,
    random_owner,
    random_local,
):
    tokens, width = states.shape
    if gathers(states, qkv_weight, global_ids):
        return layer_gathered(
            states,
            qkv_weight,
            out_weight,
            up_weight,
            down_weight,
            attn_gain,
            mlp_gain,
            global_ids,
            random_owner,
            random_local,
        )
    bf = jnp.bfloat16
    dma = pltpu.SemaphoreType.DMA
    att = attend_requested(states, qkv_weight, global_ids, random_owner, random_local)

    chunks = 4
    rows = tokens // chunks
    link = jnp.bfloat16
    return pl.pallas_call(
        functools.partial(tail_kernel, chunks),
        out_shape=jax.ShapeDtypeStruct((tokens, width), bf),
        in_specs=vmem_specs(7),
        out_specs=pl.BlockSpec(memory_space=pltpu.VMEM),
        scratch_shapes=[pltpu.VMEM((chunks, rows, width), link)] * 4
        + [dma((chunks,))] * 4
        + [pltpu.VMEM((chunks, rows, width), bf)],
        compiler_params=pltpu.CompilerParams(
            collective_id=1, has_side_effects=True, vmem_limit_bytes=32 * 1024 * 1024
        ),
    )(
        att,
        states,
        out_weight,
        up_weight,
        down_weight,
        attn_gain.reshape(1, width),
        mlp_gain.reshape(1, width),
    )


def solution(mesh):
    in_specs = (
        P("seq", None),
        P(None, None, "mp"),
        P("mp", None),
        P(None, "mp"),
        P("mp", None),
        P(),
        P(),
        P(),
        P("mp", "seq", None, None),
        P("mp", "seq", None, None),
    )
    out_specs = P("seq", None)
    return jax.shard_map(shards, mesh=mesh, in_specs=in_specs, out_specs=out_specs, check_vma=False)
```
